256 devices in a mesh: beam: 2 (over z), tm: 16 (over x, core), dm: 8 (over y).
Axes of the slice: x: 8, y: 8, z: 2, core: 2. Of those that a mesh axis runs over, the one named last changes fastest.
The devices are a block of a 8x8x16 slice.
Arguments:
- series: float32 [32, 524288], P(('beam', 'dm'), 'tm'), parts along dimension 0, may hold values from -16 to 16
- cand_start: int32 [32, 8, 8, 16], P(('beam', 'tm'), 'dm'), parts along dimension 0, may hold values from 0 to 1920
- cand_count: int32 [32, 8, 8], P(('beam', 'tm'), 'dm'), parts along dimension 0, may hold values from 0 to 16, as said below
Outputs:
- harmonic_sum: float32 [32, 32768], P(('beam', 'dm'), 'tm'), parts along dimension 0
- sifted: float32 [32, 8, 8, 16, 128], P(('beam', 'tm'), 'dm'), parts along dimension 0
The draws below stay inside these ranges and needn't reach their ends.
There are 2 independent parts, one for each index of `beam`. The reference program is written for one: setup_inputs(seed, part) draws one part's arguments, and reference() takes and returns one part's arrays. A program takes and returns all parts, laid end to end along the dimension named above; each array names one. Nothing has to cross between parts.
Inputs may be any that keep to these rules, and one draw needn't show every extreme that they name: `cand_count`: in every draw some destination band receives 16 live slots from every source band and frequency shard.
All inputs are finite; a program needn't handle non-finite values.
Results may differ from the reference program's by a relative error of at most 0.00015.
Values sent between devices are 32-bit elements; how exact they have to be, the bound alone decides.
No kernel may reach another device: no remote copies, remote signals or barrier semaphores. Data moves between devices by JAX's collectives and lax.ppermute only.
A program may use at most 128 MiB of HBM per device.

```python
import jax
import jax.numpy as jnp
from jax import lax

DM_DEV = 2
NT = 524288
N1 = 512
HARM = 8
BW = 128
CAP = 16
NDM = 16
TSHARDS = 16
BANDS = 8
NH = 32768
FL = 2048


def draw_series(key, part):
    noise_key, echo_key, gain_key = jax.random.split(jax.random.fold_in(key, 11), 3)
    echo_lag = NT // N1
    noise = jax.random.truncated_normal(noise_key, -4.0, 4.0, (NDM, NT + echo_lag), jnp.float32)
    echo_level = jax.random.uniform(echo_key, (NDM, 1), jnp.float32, 0.4, 0.8)
    time_ramp = jnp.ones((1, NT), jnp.float32)
    row_gain = jax.random.uniform(gain_key, (NDM, 1), jnp.float32, 0.5, 2.0)
    return (row_gain * time_ramp * (noise[:, echo_lag:] + echo_level * noise[:, :NT])).astype(jnp.float32)


def draw_cand_count(key, part):
    base_key, light_key, chosen_key = jax.random.split(jax.random.fold_in(key, 23), 3)
    counts = jax.random.randint(base_key, (TSHARDS, BANDS, BANDS), 0, CAP + 1)
    lighter = jax.random.randint(light_key, (BANDS,), 0, 2)
    chosen = jax.random.randint(chosen_key, (), 0, BANDS)
    targets = jnp.arange(BANDS, dtype=jnp.int32)
    counts = jnp.where(lighter[None, None, :] == 1, counts // 2, counts)
    counts = jnp.where(targets[None, None, :] == chosen, CAP, counts)
    return counts.astype(jnp.int32)


def place_ends(result, key, least, top_value):
    extent = result.shape
    index_at = [jax.random.randint(jax.random.fold_in(key, axis), (), 0, extent[axis]) for axis in range(len(extent))]
    result = result.at[tuple(index_at)].set(least)
    longest = extent.index(max(extent))
    index_at[longest] = (index_at[longest] + 1) % extent[longest]
    return result.at[tuple(index_at)].set(top_value)


def setup_inputs(seed: int = 0, part: int = 0) -> dict:
    key_of = jax.random.split(jax.random.key(seed), 4)
    own_keys = jax.random.split(jax.random.fold_in(key_of[3], part), 4)
    return {
        "series": draw_series(jax.random.fold_in(jax.random.fold_in(key_of[3], part), 71), part),
        "cand_start": place_ends(jax.random.randint(own_keys[1], (TSHARDS, BANDS, BANDS, CAP), 0, FL - BW + 1), jax.random.fold_in(own_keys[1], 1), 0, FL - BW).astype(jnp.int32),
        "cand_count": draw_cand_count(jax.random.fold_in(jax.random.fold_in(key_of[3], part), 71), part),
    }


EPSILON = 1e-06

def reference(series, cand_start, cand_count):
    spectrum = jnp.fft.rfft(series, axis=-1)[:, :NT // 2]
    power_bins = ((jnp.real(spectrum) ** 2 + jnp.imag(spectrum) ** 2) / NT).astype(jnp.float32)
    row_mean = lax.optimization_barrier(jnp.mean(power_bins, axis=1, keepdims=True))
    deviation = power_bins - row_mean
    spread = lax.optimization_barrier(jnp.mean(deviation * deviation, axis=1, keepdims=True))
    scores = deviation / jnp.sqrt(spread + EPSILON)
    summed = scores[:, :NH]
    for harmonic in range(2, HARM + 1):
        summed = summed + scores[:, 0:harmonic * NH:harmonic]
    banded = summed.reshape(BANDS, DM_DEV, TSHARDS, FL)
    peak_rows = lax.optimization_barrier(jnp.max(banded, axis=1))
    band_level = lax.optimization_barrier(jnp.sum(banded, axis=1)) / DM_DEV
    bin_span = cand_start[..., None] + jnp.arange(BW, dtype=jnp.int32)
    shard_ids = jnp.arange(TSHARDS, dtype=jnp.int32)[:, None, None, None, None]
    source_ids = jnp.arange(BANDS, dtype=jnp.int32)[None, :, None, None, None]
    target_ids = jnp.arange(BANDS, dtype=jnp.int32)[None, None, :, None, None]
    top_values = peak_rows[source_ids, shard_ids, bin_span]
    low_values = band_level[target_ids, shard_ids, bin_span]
    slot_ids = jnp.arange(CAP, dtype=jnp.int32)[None, None, None, :, None]
    live_slots = slot_ids < cand_count[..., None, None]
    sifted = jnp.where(live_slots, top_values - low_values, jnp.float32(0.0))
    sifted = jnp.transpose(sifted, (0, 2, 1, 3, 4))
    return (summed, sifted)
```

```python
import functools
import math

import jax
import jax.numpy as jnp
import numpy as np
from jax import lax
from jax.experimental import pallas as pl
from jax.experimental.pallas import tpu as pltpu
from jax.sharding import PartitionSpec as P

HARM = 8
BW = 128
EPSILON = 1e-06

LANES = 128
SUB = 8
COARSE = 256
SLOTS = 8
PIECE = 32
PIECES = [(h, c) for h in range(1, HARM + 1) for c in range(h)]
CHUNKS = len(PIECES) // 4

F32 = jnp.float32
BF16 = jnp.bfloat16


def halves(value):
    top = value.astype(BF16)
    return top, (value - top.astype(F32)).astype(BF16)


def np_halves(value):
    top = value.astype(np.float32).astype(BF16)
    rest = (value - top.astype(np.float64)).astype(np.float32).astype(BF16)
    return top, rest


def unit(turns, period):
    angle = -2.0 * math.pi * (turns % period) / period
    return np.cos(angle), np.sin(angle)


@functools.cache
def tables(shards, samples):
    inner = samples // COARSE
    a = np.arange(COARSE)
    r = np.arange(COARSE // 2)
    c1, s1 = unit(r[:, None] * a[None, :], COARSE)
    s1[0] = np.where(a % 2 == 0, 1.0, -1.0)
    first = np_halves(np.concatenate([c1, s1], axis=0))
    b = np.arange(LANES)
    j = np.arange(LANES // 2)
    rows = []
    for q2 in (j, LANES - 1 - j):
        c2, s2 = unit(q2[:, None] * b[None, :], LANES)
        rows += [np.concatenate([c2, -s2], axis=1), np.concatenate([s2, c2], axis=1)]
    second = np_halves(np.concatenate(rows, axis=0))
    s = np.arange(shards)
    pos = LANES * s[:, None] + b[None, :]
    slot = np.arange(SLOTS)
    by_slot = np.stack(unit(pos[:, None, :] * slot[None, :, None], samples))
    by_shard = np.stack(unit(SLOTS * s[:, None, None] * pos[None], samples), axis=1)
    by_extra = np.stack(unit((COARSE // 2) * pos, samples))
    between = np.stack(unit(s[:, None] * b[None, :], inner))
    small = [t.astype(np.float32) for t in (by_slot, by_shard, by_extra, between)]
    return first, second, small


def pack_kernel(x_ref, o_ref):
    shards = o_ref.shape[0] // 32
    chunks = x_ref.shape[1] // (LANES * shards)
    for d in range(shards):
        for a in range(chunks):
            piece = x_ref[:, pl.ds((a * shards + d) * LANES, LANES)]
            o_ref[pl.ds(d * 2 * chunks + a, 2, stride=chunks), :] = piece


def first_kernel(x_ref, th_ref, tl_ref, o_ref):
    shards = x_ref.shape[0]
    part = x_ref.shape[1] // 2
    tops, rests = [], []
    for row in range(2):
        top, rest = halves(x_ref[:, row * part : (row + 1) * part, :].reshape(COARSE, LANES))
        tops.append(top)
        rests.append(rest)
    top = jnp.concatenate(tops, axis=1)
    rest = jnp.concatenate(rests, axis=1)
    dot = functools.partial(jnp.dot, preferred_element_type=F32)
    y = dot(th_ref[...], top) + dot(th_ref[...], rest) + dot(tl_ref[...], top)
    half = COARSE // 2
    for part_id in range(2):
        for row in range(2):
            block = y[part_id * half : (part_id + 1) * half, row * LANES : (row + 1) * LANES]
            at = (part_id * 2 + row) * SUB
            o_ref[:, at : at + SUB, :] = block.reshape(shards, SUB, LANES)


def cmul(x, y):
    return x[0] * y[0] - x[1] * y[1], x[0] * y[1] + x[1] * y[0]


def cadd(x, y):
    return x[0] + y[0], x[1] + y[1]


def csub(x, y):
    return x[0] - y[0], x[1] - y[1]


def turn_back(x):
    return x[1], -x[0]


def four(x0, x1, x2, x3):
    s, d = cadd(x0, x2), csub(x0, x2)
    t, u = cadd(x1, x3), turn_back(csub(x1, x3))
    return cadd(s, t), cadd(d, u), csub(s, t), csub(d, u)


def sixteen(values):
    columns = [four(*values[low::4]) for low in range(4)]
    out = [None] * 16
    for k1 in range(4):
        terms = []
        for low in range(4):
            term = columns[low][k1]
            if low * k1:
                c, s = unit(np.float64(low * k1), 16)
                if abs(s + 1.0) < 1e-12:
                    term = turn_back(term)
                else:
                    term = cmul(term, (F32(c), F32(s)))
            terms.append(term)
        for k2, value in enumerate(four(*terms)):
            out[k1 + 4 * k2] = value
    return out


def second_kernel(d_ref, x_ref, ws_ref, wd_ref, wx_ref, a_ref, th_ref, tl_ref, o_ref, t_scr, dh_scr, dl_scr, r_scr, l_scr, s_scr, h_scr):
    shards = x_ref.shape[0]
    me = d_ref[0]
    is_first = me == 0
    sub = lax.broadcasted_iota(jnp.int32, (SUB, LANES), 0)
    lead = jnp.logical_and(sub == 0, is_first)

    for row in range(2):
        main, extra = [], []
        for s in range(shards):
            re = x_ref[s, row * SUB : (row + 1) * SUB, :]
            im = x_ref[s, (2 + row) * SUB : (3 + row) * SUB, :]
            own = wd_ref[0, 0, s : s + 1, :], wd_ref[0, 1, s : s + 1, :]
            twiddle = cmul((ws_ref[0, s], ws_ref[1, s]), own)
            main.append(cmul((re, jnp.where(lead, 0.0, im)), twiddle))
            extra.append((im * wx_ref[0, s : s + 1, :], im * wx_ref[1, s : s + 1, :]))
        for kind, values in enumerate((main, extra)):
            for rho, value in enumerate(sixteen(values)):
                value = cmul(value, (a_ref[0, rho : rho + 1, :], a_ref[1, rho : rho + 1, :]))
                t_scr[kind * 2 + row, rho, 0] = value[0]
                t_scr[kind * 2 + row, rho, 1] = value[1]

    for rho in range(shards):
        for part in range(2):
            low = jnp.concatenate([t_scr[0, rho, part], t_scr[1, rho, part]], axis=0)
            high = jnp.concatenate(
                [jnp.where(lead, t_scr[2 + row, rho, part], t_scr[row, shards - 1 - rho, part]) for row in range(2)],
                axis=0,
            )
            for k, tile in enumerate((low, high)):
                top, rest = halves(tile)
                rows = pl.ds(rho * PIECE + k * 16, 16)
                cols = pl.ds(part * LANES, LANES)
                dh_scr[rows, cols] = top
                dl_scr[rows, cols] = rest
    dims = (((1,), (1,)), ((), ()))
    dot_t = functools.partial(lax.dot_general, dimension_numbers=dims, preferred_element_type=F32)
    half = LANES // 2
    lane = lax.broadcasted_iota(jnp.int32, (half, 2 * LANES), 1)
    within = lane % PIECE
    from_low = jnp.logical_or(within < 16, jnp.logical_and(within % SUB == 0, is_first))
    scale = 1.0 / (shards * LANES * COARSE)
    powers = []
    for part in range(2):
        top = dh_scr[part * 256 : (part + 1) * 256, :]
        rest = dl_scr[part * 256 : (part + 1) * 256, :]
        z = dot_t(th_ref[...], top) + dot_t(th_ref[...], rest) + dot_t(tl_ref[...], top)
        z = z * z
        low = z[0:half] + z[half : 2 * half]
        high = z[2 * half : 3 * half] + z[3 * half :]
        powers.append(jnp.where(from_low, low, high) * scale)

    count = 2 * SLOTS * LANES * shards // 2
    one_row = (lane // SUB) % 2 == 1
    column = jnp.sum(powers[0] + powers[1], axis=0, keepdims=True)
    row_lane = one_row[0:1, :]
    mean0 = jnp.sum(jnp.where(row_lane, 0.0, column), axis=1, keepdims=True) / count
    mean1 = jnp.sum(jnp.where(row_lane, column, 0.0), axis=1, keepdims=True) / count
    centre = jnp.where(row_lane, mean1, mean0)
    off0 = powers[0] - centre
    off1 = powers[1] - centre
    column = jnp.sum(off0 * off0 + off1 * off1, axis=0, keepdims=True)
    dev0 = jnp.sum(jnp.where(row_lane, 0.0, column), axis=1, keepdims=True)
    dev1 = jnp.sum(jnp.where(row_lane, column, 0.0), axis=1, keepdims=True)
    stats = jnp.where(sub == 0, mean0, jnp.where(sub == 1, mean1, jnp.where(sub == 2, dev0, dev1)))
    for t in range(shards):
        o_ref[t, 4 * SUB : 5 * SUB, :] = stats

    for group in range(4):
        value = powers[group // 2][:, (group % 2) * LANES : (group % 2 + 1) * LANES]
        for shift in range(4):
            at = (group * 4 + shift) * half
            r_scr[at : at + half, :] = pltpu.roll(value, shift * PIECE, 1) if shift else value
    lane8 = lax.broadcasted_iota(jnp.int32, (SUB, LANES), 1) // PIECE
    for chunk in range(CHUNKS):
        for g_pair in range(shards // 2):
            tiles = []
            for g0 in (2 * g_pair, 2 * g_pair + 1):
                tile = None
                for place in range(4):
                    h, c = PIECES[chunk * 4 + place]
                    rho, e = (h * g0 + c) % shards, (h * g0 + c) // shards
                    shift = (place - rho % 4) % 4
                    rows = pl.ds((rho // 4 * 4 + shift) * half + e, SUB, stride=h)
                    got = r_scr[rows, :]
                    tile = got if tile is None else jnp.where(lane8 == place, got, tile)
                tiles.append(tile)
            top, rest = halves(jnp.concatenate(tiles, axis=0))
            cols = pl.ds(chunk * LANES, LANES)
            l_scr[pl.ds(g_pair * 16, 16), cols] = top
            l_scr[pl.ds(LANES + g_pair * 16, 16), cols] = rest
    phi = lax.broadcasted_iota(jnp.int32, (SUB, COARSE), 1)
    slot = lax.broadcasted_iota(jnp.int32, (SUB, COARSE), 0)
    mine = me * SLOTS + slot
    mirror = jnp.where(mine == 0, COARSE // 2, COARSE - mine)
    none = jnp.zeros((SUB, COARSE), F32)
    for index, (h, c) in enumerate(PIECES):
        for k, residue in enumerate((mine, mirror)):
            hit = jnp.where(h * phi - COARSE * c == residue, 1.0, 0.0)
            rows = pl.ds(index * PIECE + k * 16, 16)
            s_scr[rows, 0:COARSE] = jnp.concatenate([hit, none], axis=0).astype(BF16)
            s_scr[rows, COARSE : 2 * COARSE] = jnp.concatenate([none, hit], axis=0).astype(BF16)
    both = jnp.dot(l_scr[...], s_scr[...], preferred_element_type=F32)
    for tile in range(4):
        cols = slice(tile * LANES, (tile + 1) * LANES)
        h_scr[tile * LANES : (tile + 1) * LANES, :] = both[:LANES, cols] + both[LANES:, cols]
    for t in range(shards):
        for tile in range(4):
            rows = pl.ds(tile * LANES + (t % 2) * 64 + t // 2, SUB, stride=SUB)
            o_ref[t, tile * SUB : (tile + 1) * SUB, :] = h_scr[rows, :]


def third_kernel(x_ref, m_ref, hs_ref, msg_ref, level_ref):
    shards = x_ref.shape[0]
    total = x_ref[0]
    for s in range(1, shards):
        total = total + x_ref[s]
    mean = total[4 * SUB : 5 * SUB] / shards
    count = 2 * SLOTS * LANES * shards // 2
    between = jnp.zeros((SUB, LANES), F32)
    for s in range(shards):
        off = x_ref[s, 4 * SUB : 5 * SUB, :] - mean
        between = between + off * off
    tiles = []
    for row in range(2):
        deviation = total[4 * SUB + 2 + row : 4 * SUB + 3 + row] + count * between[row : row + 1]
        scale = 1.0 / jnp.sqrt(deviation / (count * shards) + EPSILON)
        shift = HARM * mean[row : row + 1]
        tiles.append([(total[(2 * row + k) * SUB : (2 * row + k + 1) * SUB] - shift) * scale for k in range(2)])
    for row in range(2):
        for k in range(2):
            for g in range(SUB):
                hs_ref[row : row + 1, pl.ds(g * COARSE + k * LANES, LANES)] = tiles[row][k][g : g + 1]
    for k in range(2):
        level_ref[k * SUB : (k + 1) * SUB, :] = (tiles[0][k] + tiles[1][k]) / 2
        peak = jnp.maximum(tiles[0][k], tiles[1][k])
        for e in range(msg_ref.shape[0]):
            msg_ref[e, k * SUB : (k + 1) * SUB, :] = peak
    for e in range(msg_ref.shape[0]):
        msg_ref[e, 2 * SUB : 3 * SUB, :] = m_ref[e]


def sift_kernel(x_ref, level_ref, o_ref):
    bands = x_ref.shape[0]
    level = level_ref[...]
    diff = jnp.concatenate([x_ref[d, 0:16, :] - level for d in range(bands)], axis=0)
    columns = []
    for d in range(bands):
        tile = x_ref[d, 16:24, :]
        for k in range(2):
            at = k * (LANES // 2)
            columns.append(jnp.broadcast_to(tile[:, at : at + 1], (SUB, LANES)))
    start = jnp.concatenate(columns, axis=0).astype(jnp.int32)
    rows = bands * 16
    lane = lax.broadcasted_iota(jnp.int32, (rows, LANES), 1)
    owner = lax.broadcasted_iota(jnp.int32, (rows, LANES), 0) // 16
    block = jnp.maximum(start, 0)
    tile_id, offset = block // LANES, block % LANES

    def pick(which):
        place = (which % 2) * SUB + which // 2
        hit = jnp.logical_and(jnp.logical_and(lane // 16 == owner, lane % 16 == place), which < 16)
        return jnp.where(hit, 1.0, 0.0).astype(BF16)

    top, rest = halves(diff)
    last = (diff - top.astype(F32) - rest.astype(F32)).astype(BF16)
    dot = functools.partial(jnp.dot, preferred_element_type=F32)
    here, after = pick(tile_id), pick(tile_id + 1)
    first = dot(here, top) + dot(here, rest) + dot(here, last)
    second = dot(after, top) + dot(after, rest) + dot(after, last)
    joined = jnp.where(lane >= offset, first, second)
    index = (lane + offset) % LANES
    moved = jnp.take_along_axis(joined, index, axis=1)
    moved = jnp.where(start >= 0, moved, 0.0)
    o_ref[...] = moved.reshape(bands, 16, LANES)


def call(kernel, out, inputs, scratch=()):
    vmem = pl.BlockSpec(memory_space=pltpu.VMEM)
    many = isinstance(out, (tuple, list))
    return pl.pallas_call(
        kernel,
        out_shape=out,
        in_specs=[vmem] * len(inputs),
        out_specs=[vmem] * len(out) if many else vmem,
        scratch_shapes=list(scratch),
    )(*inputs)


def shape(*dims):
    return jax.ShapeDtypeStruct(dims, F32)


def run_pack(series, shards):
    return call(pack_kernel, shape(shards * 32, LANES), [series]).reshape(shards, 32, LANES)


def run_first(received, first):
    return call(first_kernel, shape(*received.shape), [received, *map(jnp.asarray, first)])


def run_second(me, received, second, small):
    shards = received.shape[0]
    by_slot, by_shard, by_extra, between = map(jnp.asarray, small)
    inputs = [received, by_slot, by_shard, by_extra, between, *map(jnp.asarray, second)]

    def whole(array):
        return pl.BlockSpec(array.shape, lambda i, d: (0,) * array.ndim)

    specs = [whole(x) for x in inputs]
    specs[2] = pl.BlockSpec((1, *by_shard.shape[1:]), lambda i, d: (d[0], 0, 0, 0))
    out = shape(shards, 5 * SUB, LANES)
    return pl.pallas_call(
        second_kernel,
        out_shape=out,
        grid_spec=pltpu.PrefetchScalarGridSpec(
            num_scalar_prefetch=1,
            grid=(1,),
            in_specs=specs,
            out_specs=whole(out),
            scratch_shapes=[
                pltpu.VMEM((4, shards, 2, SUB, LANES), F32),
                pltpu.VMEM((shards * PIECE, 2 * LANES), BF16),
                pltpu.VMEM((shards * PIECE, 2 * LANES), BF16),
                pltpu.VMEM((16 * LANES // 2, LANES), F32),
                pltpu.VMEM((2 * LANES, CHUNKS * LANES), BF16),
                pltpu.VMEM((CHUNKS * LANES, 2 * COARSE), BF16),
                pltpu.VMEM((4 * LANES, LANES), F32),
            ],
        ),
    )(me, *inputs)


def run_third(received, markers):
    bands = markers.shape[0]
    out = (shape(2, SUB * COARSE), shape(bands, 3 * SUB, LANES), shape(2 * SUB, LANES))
    return call(third_kernel, out, [received, markers])


def run_sift(received, level):
    return call(sift_kernel, shape(received.shape[0], 16, LANES), [received, level])


def make_markers(cand_start, cand_count):
    starts = cand_start[0, 0]
    counts = cand_count[0, 0]
    bands, slot_total = starts.shape
    live = jnp.arange(slot_total, dtype=jnp.int32)[None, :] < counts[:, None]
    markers = jnp.where(live, starts, -1).astype(F32)
    tiles = jnp.swapaxes(markers.reshape(bands, 2, SUB), 1, 2)[..., None]
    return jnp.broadcast_to(tiles, (bands, SUB, 2, LANES // 2)).reshape(bands, SUB, LANES)


def per_device(series, cand_start, cand_count):
    shards = lax.axis_size("tm")
    first, second, small = tables(shards, shards * series.shape[1])
    me = lax.axis_index("tm").astype(jnp.int32).reshape(1)
    markers = make_markers(cand_start, cand_count)
    swap = functools.partial(lax.all_to_all, split_axis=0, concat_axis=0, tiled=True)
    samples = swap(run_pack(series, shards), "tm")
    partial = swap(run_first(samples, first), "tm")
    sums = swap(run_second(me, partial, second, small), "tm")
    harmonic_sum, message, level = run_third(sums, markers)
    sifted = run_sift(swap(message, "dm"), level)
    return harmonic_sum, sifted[None, None]


def solution(mesh):
    return jax.shard_map(
        per_device,
        mesh=mesh,
        in_specs=(
            P(("beam", "dm"), "tm"),
            P(("beam", "tm"), "dm", None, None),
            P(("beam", "tm"), "dm", None),
        ),
        out_specs=(P(("beam", "dm"), "tm"), P(("beam", "tm"), "dm", None, None, None)),
        check_vma=False,
    )
```

```python
import functools
import math

import jax
import jax.numpy as jnp
import numpy as np
from jax import lax
from jax.experimental import pallas as pl
from jax.experimental.pallas import tpu as pltpu
from jax.sharding import PartitionSpec as P

HARM = 8
BW = 128
EPSILON = 1e-06

LANES = 128
SUB = 8
COARSE = 256
SLOTS = 8
PIECE = 32
PIECES = [(h, c) for h in range(1, HARM + 1) for c in range(h)]
CHUNKS = len(PIECES) // 4

F32 = jnp.float32
BF16 = jnp.bfloat16


def halves(value):
    top = value.astype(BF16)
    return top, (value - top.astype(F32)).astype(BF16)


def np_halves(value):
    top = value.astype(np.float32).astype(BF16)
    rest = (value - top.astype(np.float64)).astype(np.float32).astype(BF16)
    return top, rest


def unit(turns, period):
    angle = -2.0 * math.pi * (turns % period) / period
    return np.cos(angle), np.sin(angle)


@functools.cache
def tables(shards, samples):
    inner = samples // COARSE
    a = np.arange(COARSE)
    r = np.arange(COARSE // 2)
    c1, s1 = unit(r[:, None] * a[None, :], COARSE)
    s1[0] = np.where(a % 2 == 0, 1.0, -1.0)
    first = np_halves(np.concatenate([c1, s1], axis=0))
    b = np.arange(LANES)
    j = np.arange(LANES // 2)
    rows = []
    for q2 in (j, LANES - 1 - j):
        c2, s2 = unit(q2[:, None] * b[None, :], LANES)
        rows += [np.concatenate([c2, -s2], axis=1), np.concatenate([s2, c2], axis=1)]
    second = np_halves(np.concatenate(rows, axis=0))
    s = np.arange(shards)
    pos = LANES * s[:, None] + b[None, :]
    slot = np.arange(SLOTS)
    by_slot = np.stack(unit(pos[:, None, :] * slot[None, :, None], samples))
    by_shard = np.stack(unit(SLOTS * s[:, None, None] * pos[None], samples), axis=1)
    by_extra = np.stack(unit((COARSE // 2) * pos, samples))
    between = np.stack(unit(s[:, None] * b[None, :], inner))
    small = [t.astype(np.float32) for t in (by_slot, by_shard, by_extra, between)]
    return first, second, small


def pack_kernel(start_ref, count_ref, x_ref, o_ref, m_ref):
    shards = o_ref.shape[0] // 32
    chunks = x_ref.shape[1] // (LANES * shards)
    for d in range(shards):
        for a in range(chunks):
            piece = x_ref[:, pl.ds((a * shards + d) * LANES, LANES)]
            o_ref[pl.ds(d * 2 * chunks + a, 2, stride=chunks), :] = piece
    sub = lax.broadcasted_iota(jnp.int32, (SUB, LANES), 0)
    half = lax.broadcasted_iota(jnp.int32, (SUB, LANES), 1) // (LANES // 2)
    place = half * SUB + sub
    for e in range(m_ref.shape[0]):
        tile = jnp.zeros((SUB, LANES), jnp.int32)
        for c in range(2 * SUB):
            tile = jnp.where(place == c, start_ref[e, c], tile)
        m_ref[e] = jnp.where(place < count_ref[e], tile, -1).astype(F32)


def first_kernel(x_ref, th_ref, tl_ref, o_ref):
    shards = x_ref.shape[0]
    part = x_ref.shape[1] // 2
    tops, rests = [], []
    for row in range(2):
        top, rest = halves(x_ref[:, row * part : (row + 1) * part, :].reshape(COARSE, LANES))
        tops.append(top)
        rests.append(rest)
    top = jnp.concatenate(tops, axis=1)
    rest = jnp.concatenate(rests, axis=1)
    dot = functools.partial(jnp.dot, preferred_element_type=F32)
    y = dot(th_ref[...], top) + dot(th_ref[...], rest) + dot(tl_ref[...], top)
    half = COARSE // 2
    for part_id in range(2):
        for row in range(2):
            block = y[part_id * half : (part_id + 1) * half, row * LANES : (row + 1) * LANES]
            at = (part_id * 2 + row) * SUB
            o_ref[:, at : at + SUB, :] = block.reshape(shards, SUB, LANES)


def cmul(x, y):
    return x[0] * y[0] - x[1] * y[1], x[0] * y[1] + x[1] * y[0]


def cadd(x, y):
    return x[0] + y[0], x[1] + y[1]


def csub(x, y):
    return x[0] - y[0], x[1] - y[1]


def turn_back(x):
    return x[1], -x[0]


def four(x0, x1, x2, x3):
    s, d = cadd(x0, x2), csub(x0, x2)
    t, u = cadd(x1, x3), turn_back(csub(x1, x3))
    return cadd(s, t), cadd(d, u), csub(s, t), csub(d, u)


def sixteen(values):
    columns = [four(*values[low::4]) for low in range(4)]
    out = [None] * 16
    for k1 in range(4):
        terms = []
        for low in range(4):
            term = columns[low][k1]
            if low * k1:
                c, s = unit(np.float64(low * k1), 16)
                if abs(s + 1.0) < 1e-12:
                    term = turn_back(term)
                else:
                    term = cmul(term, (F32(c), F32(s)))
            terms.append(term)
        for k2, value in enumerate(four(*terms)):
            out[k1 + 4 * k2] = value
    return out


def second_kernel(d_ref, x_ref, ws_ref, wd_ref, wx_ref, a_ref, th_ref, tl_ref, o_ref, t_scr, dh_scr, dl_scr, r_scr, l_scr, s_scr, h_scr):
    shards = x_ref.shape[0]
    me = d_ref[0]
    is_first = me == 0
    sub = lax.broadcasted_iota(jnp.int32, (SUB, LANES), 0)
    lead = jnp.logical_and(sub == 0, is_first)

    for row in range(2):
        main, extra = [], []
        for s in range(shards):
            re = x_ref[s, row * SUB : (row + 1) * SUB, :]
            im = x_ref[s, (2 + row) * SUB : (3 + row) * SUB, :]
            own = wd_ref[me, 0, s : s + 1, :], wd_ref[me, 1, s : s + 1, :]
            twiddle = cmul((ws_ref[0, s], ws_ref[1, s]), own)
            main.append(cmul((re, jnp.where(lead, 0.0, im)), twiddle))
            extra.append((im * wx_ref[0, s : s + 1, :], im * wx_ref[1, s : s + 1, :]))
        for kind, values in enumerate((main, extra)):
            for rho, value in enumerate(sixteen(values)):
                value = cmul(value, (a_ref[0, rho : rho + 1, :], a_ref[1, rho : rho + 1, :]))
                t_scr[kind * 2 + row, rho, 0] = value[0]
                t_scr[kind * 2 + row, rho, 1] = value[1]

    for rho in range(shards):
        for part in range(2):
            low = jnp.concatenate([t_scr[0, rho, part], t_scr[1, rho, part]], axis=0)
            high = jnp.concatenate(
                [jnp.where(lead, t_scr[2 + row, rho, part], t_scr[row, shards - 1 - rho, part]) for row in range(2)],
                axis=0,
            )
            for k, tile in enumerate((low, high)):
                top, rest = halves(tile)
                rows = pl.ds(rho * PIECE + k * 16, 16)
                cols = pl.ds(part * LANES, LANES)
                dh_scr[rows, cols] = top
                dl_scr[rows, cols] = rest
    dims = (((1,), (1,)), ((), ()))
    dot_t = functools.partial(lax.dot_general, dimension_numbers=dims, preferred_element_type=F32)
    half = LANES // 2
    lane = lax.broadcasted_iota(jnp.int32, (half, 2 * LANES), 1)
    within = lane % PIECE
    from_low = jnp.logical_or(within < 16, jnp.logical_and(within % SUB == 0, is_first))
    scale = 1.0 / (shards * LANES * COARSE)
    powers = []
    for part in range(2):
        top = dh_scr[part * 256 : (part + 1) * 256, :]
        rest = dl_scr[part * 256 : (part + 1) * 256, :]
        z = dot_t(th_ref[...], top) + dot_t(th_ref[...], rest) + dot_t(tl_ref[...], top)
        z = z * z
        low = z[0:half] + z[half : 2 * half]
        high = z[2 * half : 3 * half] + z[3 * half :]
        powers.append(jnp.where(from_low, low, high) * scale)

    count = 2 * SLOTS * LANES * shards // 2
    one_row = (lane // SUB) % 2 == 1
    column = jnp.sum(powers[0] + powers[1], axis=0, keepdims=True)
    row_lane = one_row[0:1, :]
    mean0 = jnp.sum(jnp.where(row_lane, 0.0, column), axis=1, keepdims=True) / count
    mean1 = jnp.sum(jnp.where(row_lane, column, 0.0), axis=1, keepdims=True) / count
    centre = jnp.where(row_lane, mean1, mean0)
    off0 = powers[0] - centre
    off1 = powers[1] - centre
    column = jnp.sum(off0 * off0 + off1 * off1, axis=0, keepdims=True)
    dev0 = jnp.sum(jnp.where(row_lane, 0.0, column), axis=1, keepdims=True)
    dev1 = jnp.sum(jnp.where(row_lane, column, 0.0), axis=1, keepdims=True)
    stats = jnp.where(sub == 0, mean0, jnp.where(sub == 1, mean1, jnp.where(sub == 2, dev0, dev1)))
    for t in range(shards):
        o_ref[t, 4 * SUB : 5 * SUB, :] = stats

    for group in range(4):
        value = powers[group // 2][:, (group % 2) * LANES : (group % 2 + 1) * LANES]
        for shift in range(4):
            at = (group * 4 + shift) * half
            r_scr[at : at + half, :] = pltpu.roll(value, shift * PIECE, 1) if shift else value
    lane8 = lax.broadcasted_iota(jnp.int32, (SUB, LANES), 1) // PIECE
    for chunk in range(CHUNKS):
        for g_pair in range(shards // 2):
            tiles = []
            for g0 in (2 * g_pair, 2 * g_pair + 1):
                tile = None
                for place in range(4):
                    h, c = PIECES[chunk * 4 + place]
                    rho, e = (h * g0 + c) % shards, (h * g0 + c) // shards
                    shift = (place - rho % 4) % 4
                    rows = pl.ds((rho // 4 * 4 + shift) * half + e, SUB, stride=h)
                    got = r_scr[rows, :]
                    tile = got if tile is None else jnp.where(lane8 == place, got, tile)
                tiles.append(tile)
            top, rest = halves(jnp.concatenate(tiles, axis=0))
            cols = pl.ds(chunk * LANES, LANES)
            l_scr[pl.ds(g_pair * 16, 16), cols] = top
            l_scr[pl.ds(LANES + g_pair * 16, 16), cols] = rest
    phi = lax.broadcasted_iota(jnp.int32, (SUB, COARSE), 1)
    slot = lax.broadcasted_iota(jnp.int32, (SUB, COARSE), 0)
    mine = me * SLOTS + slot
    mirror = jnp.where(mine == 0, COARSE // 2, COARSE - mine)
    none = jnp.zeros((SUB, COARSE), F32)
    for index, (h, c) in enumerate(PIECES):
        for k, residue in enumerate((mine, mirror)):
            hit = jnp.where(h * phi - COARSE * c == residue, 1.0, 0.0)
            rows = pl.ds(index * PIECE + k * 16, 16)
            s_scr[rows, 0:COARSE] = jnp.concatenate([hit, none], axis=0).astype(BF16)
            s_scr[rows, COARSE : 2 * COARSE] = jnp.concatenate([none, hit], axis=0).astype(BF16)
    both = jnp.dot(l_scr[...], s_scr[...], preferred_element_type=F32)
    for tile in range(4):
        cols = slice(tile * LANES, (tile + 1) * LANES)
        h_scr[tile * LANES : (tile + 1) * LANES, :] = both[:LANES, cols] + both[LANES:, cols]
    for t in range(shards):
        for tile in range(4):
            rows = pl.ds(tile * LANES + (t % 2) * 64 + t // 2, SUB, stride=SUB)
            o_ref[t, tile * SUB : (tile + 1) * SUB, :] = h_scr[rows, :]


def third_kernel(x_ref, m_ref, hs_ref, msg_ref, level_ref):
    shards = x_ref.shape[0]
    total = x_ref[0]
    for s in range(1, shards):
        total = total + x_ref[s]
    mean = total[4 * SUB : 5 * SUB] / shards
    count = 2 * SLOTS * LANES * shards // 2
    between = jnp.zeros((SUB, LANES), F32)
    for s in range(shards):
        off = x_ref[s, 4 * SUB : 5 * SUB, :] - mean
        between = between + off * off
    tiles = []
    for row in range(2):
        deviation = total[4 * SUB + 2 + row : 4 * SUB + 3 + row] + count * between[row : row + 1]
        scale = 1.0 / jnp.sqrt(deviation / (count * shards) + EPSILON)
        shift = HARM * mean[row : row + 1]
        tiles.append([(total[(2 * row + k) * SUB : (2 * row + k + 1) * SUB] - shift) * scale for k in range(2)])
    for row in range(2):
        for k in range(2):
            for g in range(SUB):
                hs_ref[row : row + 1, pl.ds(g * COARSE + k * LANES, LANES)] = tiles[row][k][g : g + 1]
    for k in range(2):
        level_ref[k * SUB : (k + 1) * SUB, :] = (tiles[0][k] + tiles[1][k]) / 2
        peak = jnp.maximum(tiles[0][k], tiles[1][k])
        for e in range(msg_ref.shape[0]):
            msg_ref[e, k * SUB : (k + 1) * SUB, :] = peak
    for e in range(msg_ref.shape[0]):
        msg_ref[e, 2 * SUB : 3 * SUB, :] = m_ref[e]


def sift_kernel(x_ref, level_ref, o_ref):
    bands = x_ref.shape[0]
    level = level_ref[...]
    diff = jnp.concatenate([x_ref[d, 0:16, :] - level for d in range(bands)], axis=0)
    columns = []
    for d in range(bands):
        tile = x_ref[d, 16:24, :]
        for k in range(2):
            at = k * (LANES // 2)
            columns.append(jnp.broadcast_to(tile[:, at : at + 1], (SUB, LANES)))
    start = jnp.concatenate(columns, axis=0).astype(jnp.int32)
    rows = bands * 16
    lane = lax.broadcasted_iota(jnp.int32, (rows, LANES), 1)
    owner = lax.broadcasted_iota(jnp.int32, (rows, LANES), 0) // 16
    block = jnp.maximum(start, 0)
    tile_id, offset = block // LANES, block % LANES

    def pick(which):
        place = (which % 2) * SUB + which // 2
        hit = jnp.logical_and(jnp.logical_and(lane // 16 == owner, lane % 16 == place), which < 16)
        return jnp.where(hit, 1.0, 0.0).astype(BF16)

    top, rest = halves(diff)
    last = (diff - top.astype(F32) - rest.astype(F32)).astype(BF16)
    dot = functools.partial(jnp.dot, preferred_element_type=F32)
    here, after = pick(tile_id), pick(tile_id + 1)
    first = dot(here, top) + dot(here, rest) + dot(here, last)
    second = dot(after, top) + dot(after, rest) + dot(after, last)
    joined = jnp.where(lane >= offset, first, second)
    index = (lane + offset) % LANES
    moved = jnp.take_along_axis(joined, index, axis=1)
    moved = jnp.where(start >= 0, moved, 0.0)
    o_ref[...] = moved.reshape(bands, 16, LANES)


PARAMS = pltpu.CompilerParams(vmem_limit_bytes=16 * 2**20)


def near(array):
    return pltpu.with_memory_space_constraint(array, pltpu.VMEM)


def call(kernel, out, inputs):
    vmem = pl.BlockSpec(memory_space=pltpu.VMEM)
    many = isinstance(out, (tuple, list))
    return pl.pallas_call(
        kernel,
        out_shape=out,
        in_specs=[vmem] * len(inputs),
        out_specs=[vmem] * len(out) if many else vmem,
        compiler_params=PARAMS,
    )(*inputs)


def shape(*dims):
    return pltpu.VMEM(dims, F32)


def run_pack(series, starts, counts, shards):
    vmem = pl.BlockSpec(memory_space=pltpu.VMEM)
    smem = pl.BlockSpec(memory_space=pltpu.SMEM)
    packed, markers = pl.pallas_call(
        pack_kernel,
        out_shape=(shape(shards * 32, LANES), shape(counts.shape[0], SUB, LANES)),
        in_specs=[smem, smem, vmem],
        out_specs=[vmem, vmem],
        compiler_params=PARAMS,
    )(starts, counts, series)
    return packed.reshape(shards, 32, LANES), markers


def run_first(received, first):
    return call(first_kernel, shape(*received.shape), [near(x) for x in (received, *map(jnp.asarray, first))])


def run_second(me, received, second, small):
    shards = received.shape[0]
    by_slot, by_shard, by_extra, between = map(jnp.asarray, small)
    inputs = [near(x) for x in (received, by_slot, by_shard, by_extra, between, *map(jnp.asarray, second))]
    vmem = pl.BlockSpec(memory_space=pltpu.VMEM)
    return pl.pallas_call(
        second_kernel,
        out_shape=shape(shards, 5 * SUB, LANES),
        in_specs=[pl.BlockSpec(memory_space=pltpu.SMEM)] + [vmem] * len(inputs),
        out_specs=vmem,
        scratch_shapes=[
            pltpu.VMEM((4, shards, 2, SUB, LANES), F32),
            pltpu.VMEM((shards * PIECE, 2 * LANES), BF16),
            pltpu.VMEM((shards * PIECE, 2 * LANES), BF16),
            pltpu.VMEM((16 * LANES // 2, LANES), F32),
            pltpu.VMEM((2 * LANES, CHUNKS * LANES), BF16),
            pltpu.VMEM((CHUNKS * LANES, 2 * COARSE), BF16),
            pltpu.VMEM((4 * LANES, LANES), F32),
        ],
        compiler_params=PARAMS,
    )(me, *inputs)


def run_third(received, markers):
    bands = markers.shape[0]
    out = (jax.ShapeDtypeStruct((2, SUB * COARSE), F32), shape(bands, 3 * SUB, LANES), shape(2 * SUB, LANES))
    return call(third_kernel, out, [near(received), near(markers)])


def run_sift(received, level):
    return call(sift_kernel, jax.ShapeDtypeStruct((received.shape[0], 16, LANES), F32), [near(received), near(level)])


def per_device(series, cand_start, cand_count):
    shards = lax.axis_size("tm")
    first, second, small = tables(shards, shards * series.shape[1])
    me, series = lax.optimization_barrier((lax.axis_index("tm").astype(jnp.int32).reshape(1), series))
    swap = functools.partial(lax.all_to_all, split_axis=0, concat_axis=0, tiled=True)
    packed, markers = run_pack(series, cand_start[0, 0], cand_count[0, 0], shards)
    samples = swap(packed, "tm")
    partial = swap(run_first(samples, first), "tm")
    sums = swap(run_second(me, partial, second, small), "tm")
    harmonic_sum, message, level = run_third(sums, markers)
    sifted = run_sift(swap(message, "dm"), level)
    return harmonic_sum, sifted[None, None]


def solution(mesh):
    return jax.shard_map(
        per_device,
        mesh=mesh,
        in_specs=(
            P(("beam", "dm"), "tm"),
            P(("beam", "tm"), "dm", None, None),
            P(("beam", "tm"), "dm", None),
        ),
        out_specs=(P(("beam", "dm"), "tm"), P(("beam", "tm"), "dm", None, None, None)),
        check_vma=False,
    )
```

```python
import functools
import math

import jax
import jax.numpy as jnp
import numpy as np
from jax import lax
from jax.experimental import pallas as pl
from jax.experimental.pallas import tpu as pltpu
from jax.sharding import PartitionSpec as P

HARM = 8
BW = 128
EPSILON = 1e-06

LANES = 128
SUB = 8
COARSE = 256
SLOTS = 16
PIECE = 32
PIECES = [(h, c) for h in range(1, HARM + 1) for c in range(h)]
CHUNKS = len(PIECES) // 4

F32 = jnp.float32
BF16 = jnp.bfloat16


def halves(value):
    top = value.astype(BF16)
    return top, (value - top.astype(F32)).astype(BF16)


def np_halves(value):
    top = value.astype(np.float32).astype(BF16)
    rest = (value - top.astype(np.float64)).astype(np.float32).astype(BF16)
    return top, rest


def unit(turns, period):
    angle = -2.0 * math.pi * (turns % period) / period
    return np.cos(angle), np.sin(angle)


@functools.cache
def tables(shards, samples):
    part = samples // (shards * shards)
    tiles = part // LANES
    m = np.arange(part)
    v = np.arange(LANES)
    s = np.arange(shards)
    half = shards // 2
    r = np.arange(half)
    within = np.stack(unit(r[:, None] * m[None, :], samples)).reshape(2, half, tiles, LANES)
    shift = np.stack(unit(s[:, None] * r[None, :], shards * shards), axis=1)
    shift = np.broadcast_to(shift[..., None], (shards, 2, half, LANES))
    after = np.stack(unit(s[:, None] * m[None, :], samples // shards)).reshape(2, shards, tiles, LANES)
    middle = (half + shards * r)[:, None] * m[None, :]
    middle = np.stack(unit(middle, samples)).reshape(2, half, tiles, LANES)
    between = np.stack(unit(s[:, None] * v[None, :], part))
    j = np.arange(LANES // 2)
    rows = []
    for q2 in (j, LANES - 1 - j):
        c2, s2 = unit(q2[:, None] * v[None, :], LANES)
        rows += [np.concatenate([c2, -s2], axis=1), np.concatenate([s2, c2], axis=1)]
    last = np_halves(np.concatenate(rows, axis=0))
    first = [x.astype(np.float32) for x in (within, shift)]
    second = [x.astype(np.float32) for x in (after, middle, between)] + list(last)
    return first, second


def cmul(x, y):
    if x[1] is None:
        return x[0] * y[0], x[0] * y[1]
    return x[0] * y[0] - x[1] * y[1], x[0] * y[1] + x[1] * y[0]


def plus(a, b):
    return b if a is None else a if b is None else a + b


def minus(a, b):
    return a if b is None else -b if a is None else a - b


def cadd(x, y):
    return plus(x[0], y[0]), plus(x[1], y[1])


def csub(x, y):
    return minus(x[0], y[0]), minus(x[1], y[1])


def turn_back(x):
    return x[1], minus(None, x[0])


def four(x0, x1, x2, x3):
    s, d = cadd(x0, x2), csub(x0, x2)
    t, u = cadd(x1, x3), turn_back(csub(x1, x3))
    return cadd(s, t), cadd(d, u), csub(s, t), csub(d, u)


def sixteen(values):
    columns = [four(*values[low::4]) for low in range(4)]
    out = [None] * 16
    for k1 in range(4):
        terms = []
        for low in range(4):
            term = columns[low][k1]
            if low * k1 == 4:
                term = turn_back(term)
            elif low * k1:
                c, s = unit(np.float64(low * k1), 16)
                term = cmul(term, (F32(c), F32(s)))
            terms.append(term)
        for k2, value in enumerate(four(*terms)):
            out[k1 + 4 * k2] = value
    return out


def first_kernel(d_ref, x_ref, within_ref, shift_ref, o_ref, w_scr):
    shards = x_ref.shape[0]
    me = d_ref[0]
    tiles = x_ref.shape[2] // LANES
    half = shards // 2
    for r in range(1, half):
        own = [shift_ref[me, part, r : r + 1, :] for part in range(2)]
        twiddle = cmul((within_ref[0, r], within_ref[1, r]), own)
        for part in range(2):
            w_scr[part, r] = twiddle[part]
    for u in range(tiles):
        values = [(x_ref[t, :, u * LANES : (u + 1) * LANES], None) for t in range(shards)]
        classes = sixteen(values)
        for r in range(half):
            if r:
                value = cmul(classes[r], [w_scr[part, r, u : u + 1, :] for part in range(2)])
            else:
                value = classes[0][0], classes[half][0]
            for part in range(2):
                at = r * 4 * tiles + part * tiles + u
                o_ref[pl.ds(at, 2, stride=2 * tiles), :] = value[part]


def second_kernel(d_ref, x_ref, after_ref, middle_ref, between_ref, th_ref, tl_ref, o_ref, v_scr, x_scr, t_scr, dh_scr, dl_scr, r_scr, l_scr, s_scr, h_scr):
    shards = x_ref.shape[0]
    tiles = x_ref.shape[1] // 2
    half = LANES // 2
    own_class = d_ref[0] // 2
    is_first = own_class == 0
    sub = lax.broadcasted_iota(jnp.int32, (SUB, LANES), 0)
    lead = jnp.logical_and(sub == 0, is_first)

    for k in range(tiles // SUB):
        rows = slice(k * SUB, (k + 1) * SUB)
        main, middle = [], []
        for s in range(shards):
            re = x_ref[s, k * SUB : (k + 1) * SUB, :]
            im = x_ref[s, tiles + k * SUB : tiles + (k + 1) * SUB, :]
            main.append((re, jnp.where(is_first, 0.0, im)))
            c, sn = unit(np.float64(s), 2 * shards)
            middle.append((im * F32(c), im * F32(sn) if s else None))
        for slot, value in enumerate(sixteen(main)):
            value = cmul(value, (after_ref[0, slot, rows, :], after_ref[1, slot, rows, :]))
            for part in range(2):
                v_scr[pl.ds(part * tiles * shards + k * SUB * shards + slot, SUB, stride=shards), :] = value[part]
        for slot, value in enumerate(sixteen(middle)[: shards // 2]):
            value = cmul(value, (middle_ref[0, slot, rows, :], middle_ref[1, slot, rows, :]))
            for part in range(2):
                at = part * tiles * SUB + k * SUB * SUB + slot
                x_scr[pl.ds(at, SUB, stride=SUB), :] = value[part]

    groups = [[], [], []]
    for u in range(tiles):
        low, high, mid = [], [], []
        for part in range(2):
            at = part * tiles * shards + u * shards
            low.append(v_scr[at : at + SUB, :])
            high.append(v_scr[at + SUB : at + 2 * SUB, :])
            at = part * tiles * SUB + u * SUB
            mid.append(x_scr[at : at + SUB, :])
        groups[0].append(tuple(low))
        groups[1].append(tuple(jnp.where(is_first, mid[part], high[part]) for part in range(2)))
        groups[2].append(tuple(high))
    for group, values in enumerate(groups):
        for rho, value in enumerate(sixteen(values)):
            value = cmul(value, (between_ref[0, rho : rho + 1, :], between_ref[1, rho : rho + 1, :]))
            for part in range(2):
                t_scr[group, rho, part] = value[part]

    for rho in range(tiles):
        for part in range(2):
            back = tiles - 1 - rho
            low = jnp.concatenate([t_scr[0, rho, part], t_scr[1, rho, part]], axis=0)
            turned = jnp.where(lead, t_scr[2, rho, part], t_scr[0, back, part])
            high = jnp.concatenate([turned, t_scr[1, back, part]], axis=0)
            for k, tile in enumerate((low, high)):
                top, rest = halves(tile)
                rows = pl.ds(rho * PIECE + k * SLOTS, SLOTS)
                cols = pl.ds(part * LANES, LANES)
                dh_scr[rows, cols] = top
                dl_scr[rows, cols] = rest
    dims = (((1,), (1,)), ((), ()))
    dot_t = functools.partial(lax.dot_general, dimension_numbers=dims, preferred_element_type=F32)
    lane = lax.broadcasted_iota(jnp.int32, (half, 2 * LANES), 1)
    within = lane % PIECE
    from_low = jnp.logical_or(within < SLOTS, jnp.logical_and(within == SLOTS, is_first))
    scale = 1.0 / (shards * shards * tiles * LANES)
    powers = []
    for part in range(2):
        top = dh_scr[part * 256 : (part + 1) * 256, :]
        rest = dl_scr[part * 256 : (part + 1) * 256, :]
        z = dot_t(th_ref[...], top) + dot_t(th_ref[...], rest) + dot_t(tl_ref[...], top)
        z = z * z
        low = z[0:half] + z[half : 2 * half]
        high = z[2 * half : 3 * half] + z[3 * half :]
        powers.append(jnp.where(from_low, low, high) * scale)

    count = 2 * SLOTS * half * tiles

    def over_all(value):
        column = jnp.sum(value, axis=0, keepdims=True)
        return jnp.sum(column, axis=1, keepdims=True)

    mean = over_all(powers[0] + powers[1]) / count
    off0, off1 = powers[0] - mean, powers[1] - mean
    deviation = over_all(off0 * off0 + off1 * off1)
    stats = jnp.where(sub == 0, mean, deviation)
    for t in range(shards):
        o_ref[t, 2 * SUB : 3 * SUB, :] = stats

    for group in range(4):
        value = powers[group // 2][:, (group % 2) * LANES : (group % 2 + 1) * LANES]
        for shift in range(4):
            at = (group * 4 + shift) * half
            r_scr[at : at + half, :] = pltpu.roll(value, shift * PIECE, 1) if shift else value
    lane8 = lax.broadcasted_iota(jnp.int32, (SUB, LANES), 1) // PIECE
    for chunk in range(CHUNKS):
        for g_pair in range(tiles // 2):
            parts = []
            for g0 in (2 * g_pair, 2 * g_pair + 1):
                tile = None
                for place in range(4):
                    h, c = PIECES[chunk * 4 + place]
                    rho, e = (h * g0 + c) % tiles, (h * g0 + c) // tiles
                    shift = (place - rho % 4) % 4
                    rows = pl.ds((rho // 4 * 4 + shift) * half + e, SUB, stride=h)
                    got = r_scr[rows, :]
                    tile = got if tile is None else jnp.where(lane8 == place, got, tile)
                parts.append(tile)
            top, rest = halves(jnp.concatenate(parts, axis=0))
            cols = pl.ds(chunk * LANES, LANES)
            l_scr[pl.ds(g_pair * 16, 16), cols] = top
            l_scr[pl.ds(LANES + g_pair * 16, 16), cols] = rest
    phi = lax.broadcasted_iota(jnp.int32, (SLOTS, COARSE), 1)
    slot = lax.broadcasted_iota(jnp.int32, (SLOTS, COARSE), 0)
    pairs = slot * SLOTS - jnp.where(slot < SUB, 0, SUB * SLOTS - SUB)
    mine = jnp.where(is_first, pairs, own_class + SLOTS * slot)
    mirror = jnp.where(mine == 0, COARSE // 2, COARSE - mine)
    for index, (h, c) in enumerate(PIECES):
        for k, residue in enumerate((mine, mirror)):
            hit = jnp.where(h * phi - COARSE * c == residue, 1.0, 0.0)
            s_scr[pl.ds(index * PIECE + k * SLOTS, SLOTS), :] = hit.astype(BF16)
    both = jnp.dot(l_scr[...], s_scr[...], preferred_element_type=F32)
    for tile in range(2):
        cols = slice(tile * LANES, (tile + 1) * LANES)
        h_scr[tile * LANES : (tile + 1) * LANES, :] = both[:LANES, cols] + both[LANES:, cols]
    for t in range(shards):
        for tile in range(2):
            rows = pl.ds(tile * LANES + (t % 2) * half + t // 2, SUB, stride=SUB)
            o_ref[t, tile * SUB : (tile + 1) * SUB, :] = h_scr[rows, :]


def third_kernel(start_ref, count_ref, x_ref, hs_ref, msg_ref, level_ref):
    shards = x_ref.shape[0]
    holders = shards // 2
    count = 2 * SLOTS * (LANES // 2) * SLOTS
    tiles = []
    for row in range(2):
        total = x_ref[row]
        for r in range(1, holders):
            total = total + x_ref[2 * r + row]
        mean = total[2 * SUB : 2 * SUB + 1] / holders
        spread = total[2 * SUB + 1 : 2 * SUB + 2]
        for r in range(holders):
            off = x_ref[2 * r + row, 2 * SUB : 2 * SUB + 1, :] - mean
            spread = spread + count * (off * off)
        scale = 1.0 / jnp.sqrt(spread / (count * holders) + EPSILON)
        tiles.append([(total[k * SUB : (k + 1) * SUB] - HARM * mean) * scale for k in range(2)])
    for row in range(2):
        for k in range(2):
            for g in range(SUB):
                hs_ref[row : row + 1, pl.ds(g * COARSE + k * LANES, LANES)] = tiles[row][k][g : g + 1]
    for k in range(2):
        level_ref[k * SUB : (k + 1) * SUB, :] = (tiles[0][k] + tiles[1][k]) / 2
        peak = jnp.maximum(tiles[0][k], tiles[1][k])
        for e in range(msg_ref.shape[0]):
            msg_ref[e, k * SUB : (k + 1) * SUB, :] = peak
    sub = lax.broadcasted_iota(jnp.int32, (SUB, LANES), 0)
    place = lax.broadcasted_iota(jnp.int32, (SUB, LANES), 1) // (LANES // 2) * SUB + sub
    for e in range(msg_ref.shape[0]):
        tile = jnp.zeros((SUB, LANES), jnp.int32)
        for c in range(2 * SUB):
            tile = jnp.where(place == c, start_ref[e, c], tile)
        msg_ref[e, 2 * SUB : 3 * SUB, :] = jnp.where(place < count_ref[e], tile, -1).astype(F32)


def sift_kernel(x_ref, level_ref, o_ref):
    bands = x_ref.shape[0]
    level = level_ref[...]
    diff = jnp.concatenate([x_ref[d, 0:16, :] - level for d in range(bands)], axis=0)
    columns = []
    for d in range(bands):
        tile = x_ref[d, 16:24, :]
        for k in range(2):
            at = k * (LANES // 2)
            columns.append(jnp.broadcast_to(tile[:, at : at + 1], (SUB, LANES)))
    start = jnp.concatenate(columns, axis=0).astype(jnp.int32)
    rows = bands * 16
    lane = lax.broadcasted_iota(jnp.int32, (rows, LANES), 1)
    owner = lax.broadcasted_iota(jnp.int32, (rows, LANES), 0) // 16
    block = jnp.maximum(start, 0)
    tile_id, offset = block // LANES, block % LANES

    def pick(which):
        place = (which % 2) * SUB + which // 2
        hit = jnp.logical_and(jnp.logical_and(lane // 16 == owner, lane % 16 == place), which < 16)
        return jnp.where(hit, 1.0, 0.0).astype(BF16)

    top, rest = halves(diff)
    last = (diff - top.astype(F32) - rest.astype(F32)).astype(BF16)
    dot = functools.partial(jnp.dot, preferred_element_type=F32)
    here, after = pick(tile_id), pick(tile_id + 1)
    first = dot(here, top) + dot(here, rest) + dot(here, last)
    second = dot(after, top) + dot(after, rest) + dot(after, last)
    joined = jnp.where(lane >= offset, first, second)
    index = (lane + offset) % LANES
    moved = jnp.take_along_axis(joined, index, axis=1)
    moved = jnp.where(start >= 0, moved, 0.0)
    o_ref[...] = moved.reshape(bands, 16, LANES)


PARAMS = pltpu.CompilerParams(vmem_limit_bytes=16 * 2**20)


def near(array):
    return pltpu.with_memory_space_constraint(array, pltpu.VMEM)


def shape(*dims):
    return pltpu.VMEM(dims, F32)


def spaces(*kinds):
    return [pl.BlockSpec(memory_space=pltpu.SMEM if kind == "s" else pltpu.VMEM) for kind in kinds]


def run_first(me, received, first):
    shards = received.shape[0]
    inputs = [near(x) for x in (received, *map(jnp.asarray, first))]
    sent = pl.pallas_call(
        first_kernel,
        out_shape=shape(shards * 32, LANES),
        in_specs=spaces(*"svvv"),
        out_specs=spaces("v")[0],
        scratch_shapes=[pltpu.VMEM((2, SUB, SLOTS, LANES), F32)],
        compiler_params=PARAMS,
    )(me, *inputs)
    return sent.reshape(shards, 32, LANES)


def run_second(me, received, second):
    shards = received.shape[0]
    inputs = [near(x) for x in (received, *map(jnp.asarray, second))]
    return pl.pallas_call(
        second_kernel,
        out_shape=shape(shards, 3 * SUB, LANES),
        in_specs=spaces("s", *"vvvvvv"),
        out_specs=spaces("v")[0],
        scratch_shapes=[
            pltpu.VMEM((2 * SLOTS * SLOTS, LANES), F32),
            pltpu.VMEM((2 * SLOTS * SUB, LANES), F32),
            pltpu.VMEM((3, SLOTS, 2, SUB, LANES), F32),
            pltpu.VMEM((SLOTS * PIECE, 2 * LANES), BF16),
            pltpu.VMEM((SLOTS * PIECE, 2 * LANES), BF16),
            pltpu.VMEM((16 * LANES // 2, LANES), F32),
            pltpu.VMEM((2 * LANES, CHUNKS * LANES), BF16),
            pltpu.VMEM((CHUNKS * LANES, COARSE), BF16),
            pltpu.VMEM((2 * LANES, LANES), F32),
        ],
        compiler_params=PARAMS,
    )(me, *inputs)


def run_third(received, starts, counts):
    bands = counts.shape[0]
    return pl.pallas_call(
        third_kernel,
        out_shape=(
            jax.ShapeDtypeStruct((2, SUB * COARSE), F32),
            shape(bands, 3 * SUB, LANES),
            shape(2 * SUB, LANES),
        ),
        in_specs=spaces(*"ssv"),
        out_specs=spaces(*"vvv"),
        compiler_params=PARAMS,
    )(starts, counts, near(received))


def run_sift(received, level):
    return pl.pallas_call(
        sift_kernel,
        out_shape=jax.ShapeDtypeStruct((received.shape[0], 16, LANES), F32),
        in_specs=spaces(*"vv"),
        out_specs=spaces("v")[0],
        compiler_params=PARAMS,
    )(near(received), near(level))


def per_device(series, cand_start, cand_count):
    shards = lax.axis_size("tm")
    first, second = tables(shards, shards * series.shape[1])
    me, series = lax.optimization_barrier((lax.axis_index("tm").astype(jnp.int32).reshape(1), series))
    swap = functools.partial(lax.all_to_all, split_axis=0, concat_axis=0, tiled=True)
    samples = swap(jnp.swapaxes(series.reshape(2, shards, -1), 0, 1), "tm")
    classes = swap(run_first(me, samples, first), "tm")
    sums = swap(run_second(me, classes, second), "tm")
    harmonic_sum, message, level = run_third(sums, cand_start[0, 0], cand_count[0, 0])
    sifted = run_sift(swap(message, "dm"), level)
    return harmonic_sum, sifted[None, None]


def solution(mesh):
    return jax.shard_map(
        per_device,
        mesh=mesh,
        in_specs=(
            P(("beam", "dm"), "tm"),
            P(("beam", "tm"), "dm", None, None),
            P(("beam", "tm"), "dm", None),
        ),
        out_specs=(P(("beam", "dm"), "tm"), P(("beam", "tm"), "dm", None, None, None)),
        check_vma=False,
    )
```

```python
import functools
import math

import jax
import jax.numpy as jnp
import numpy as np
from jax import lax
from jax.experimental import pallas as pl
from jax.experimental.pallas import tpu as pltpu
from jax.sharding import PartitionSpec as P

HARM = 8
BW = 128
EPSILON = 1e-06

LANES = 128
SUB = 8
COARSE = 256
SLOTS = 16
PIECE = 32
PIECES = [(h, c) for h in range(1, HARM + 1) for c in range(h)]
CHUNKS = len(PIECES) // 4
ROWS = 2 * SUB + 1

F32 = jnp.float32
BF16 = jnp.bfloat16


def halves(value):
    top = value.astype(BF16)
    return top, (value - top.astype(F32)).astype(BF16)


def np_halves(value):
    top = value.astype(np.float32).astype(BF16)
    rest = (value - top.astype(np.float64)).astype(np.float32).astype(BF16)
    return top, rest


def unit(turns, period):
    angle = -2.0 * math.pi * (turns % period) / period
    return np.cos(angle), np.sin(angle)


@functools.cache
def tables(shards, samples):
    part = samples // (shards * shards)
    tiles = part // LANES
    m = np.arange(part)
    v = np.arange(LANES)
    s = np.arange(shards)
    half = shards // 2
    r = np.arange(half)
    within = np.stack(unit(r[:, None] * m[None, :], samples)).reshape(2, half, tiles, LANES)
    shift = np.stack(unit(s[:, None] * r[None, :], shards * shards), axis=1)
    shift = np.broadcast_to(shift[..., None], (shards, 2, half, LANES))
    after = np.stack(unit(s[:, None] * m[None, :], samples // shards)).reshape(2, shards, tiles, LANES)
    middle = (half + shards * r)[:, None] * m[None, :]
    middle = np.stack(unit(middle, samples)).reshape(2, half, tiles, LANES)
    between = np.stack(unit(s[:, None] * v[None, :], part))
    j = np.arange(LANES // 2)
    rows = []
    for q2 in (j, LANES - 1 - j):
        c2, s2 = unit(q2[:, None] * v[None, :], LANES)
        rows += [np.concatenate([c2, -s2], axis=1), np.concatenate([s2, c2], axis=1)]
    last = np_halves(np.concatenate(rows, axis=0))
    first = [x.astype(np.float32) for x in (within, shift)]
    second = [x.astype(np.float32) for x in (after, middle, between)] + list(last)
    return first, second


def cmul(x, y):
    if x[1] is None:
        return x[0] * y[0], x[0] * y[1]
    return x[0] * y[0] - x[1] * y[1], x[0] * y[1] + x[1] * y[0]


def plus(a, b):
    return b if a is None else a if b is None else a + b


def minus(a, b):
    return a if b is None else -b if a is None else a - b


def cadd(x, y):
    return plus(x[0], y[0]), plus(x[1], y[1])


def csub(x, y):
    return minus(x[0], y[0]), minus(x[1], y[1])


def turn_back(x):
    return x[1], minus(None, x[0])


def four(x0, x1, x2, x3):
    s, d = cadd(x0, x2), csub(x0, x2)
    t, u = cadd(x1, x3), turn_back(csub(x1, x3))
    return cadd(s, t), cadd(d, u), csub(s, t), csub(d, u)


def sixteen(values):
    columns = [four(*values[low::4]) for low in range(4)]
    out = [None] * 16
    for k1 in range(4):
        terms = []
        for low in range(4):
            term = columns[low][k1]
            if low * k1 == 4:
                term = turn_back(term)
            elif low * k1:
                c, s = unit(np.float64(low * k1), 16)
                term = cmul(term, (F32(c), F32(s)))
            terms.append(term)
        for k2, value in enumerate(four(*terms)):
            out[k1 + 4 * k2] = value
    return out


def first_kernel(d_ref, x_ref, within_ref, shift_ref, start_ref, count_ref, o_ref, m_ref, w_scr):
    bands, slots = start_ref.shape
    cell = [lax.broadcasted_iota(jnp.int32, (bands, bands), axis) for axis in range(2)]
    counts = jnp.where(cell[0] == cell[1], count_ref[...].astype(F32), 0.0)
    live = jnp.sum(counts, axis=1, keepdims=True).astype(jnp.int32)
    slot = lax.broadcasted_iota(jnp.int32, (bands, slots), 1)
    starts = jnp.where(slot < live, start_ref[...], -1).astype(F32)
    m_ref[...] = jnp.concatenate([starts] * (LANES // slots), axis=1)

    shards = x_ref.shape[0]
    me = d_ref[0]
    tiles = x_ref.shape[2] // LANES
    half = shards // 2
    for r in range(1, half):
        own = [shift_ref[me, part, r : r + 1, :] for part in range(2)]
        twiddle = cmul((within_ref[0, r], within_ref[1, r]), own)
        for part in range(2):
            w_scr[part, r] = twiddle[part]
    for u in range(tiles):
        values = [(x_ref[t, :, u * LANES : (u + 1) * LANES], None) for t in range(shards)]
        classes = sixteen(values)
        for r in range(half):
            if r:
                value = cmul(classes[r], [w_scr[part, r, u : u + 1, :] for part in range(2)])
            else:
                value = classes[0][0], classes[half][0]
            for part in range(2):
                at = r * 4 * tiles + part * tiles + u
                o_ref[pl.ds(at, 2, stride=2 * tiles), :] = value[part]


def second_kernel(d_ref, x_ref, after_ref, middle_ref, between_ref, th_ref, tl_ref, o_ref, v_scr, x_scr, t_scr, dh_scr, dl_scr, r_scr, l_scr, s_scr, h_scr):
    shards = x_ref.shape[0]
    tiles = x_ref.shape[1] // 2
    half = LANES // 2
    own_class = d_ref[0] // 2
    is_first = own_class == 0
    sub = lax.broadcasted_iota(jnp.int32, (SUB, LANES), 0)
    lead = jnp.logical_and(sub == 0, is_first)

    for k in range(tiles // SUB):
        rows = slice(k * SUB, (k + 1) * SUB)
        main, middle = [], []
        for s in range(shards):
            re = x_ref[s, k * SUB : (k + 1) * SUB, :]
            im = x_ref[s, tiles + k * SUB : tiles + (k + 1) * SUB, :]
            main.append((re, jnp.where(is_first, 0.0, im)))
            c, sn = unit(np.float64(s), 2 * shards)
            middle.append((im * F32(c), im * F32(sn) if s else None))
        for slot, value in enumerate(sixteen(main)):
            value = cmul(value, (after_ref[0, slot, rows, :], after_ref[1, slot, rows, :]))
            for part in range(2):
                v_scr[pl.ds(part * tiles * shards + k * SUB * shards + slot, SUB, stride=shards), :] = value[part]
        for slot, value in enumerate(sixteen(middle)[: shards // 2]):
            value = cmul(value, (middle_ref[0, slot, rows, :], middle_ref[1, slot, rows, :]))
            for part in range(2):
                at = part * tiles * SUB + k * SUB * SUB + slot
                x_scr[pl.ds(at, SUB, stride=SUB), :] = value[part]

    groups = [[], [], []]
    for u in range(tiles):
        low, high, mid = [], [], []
        for part in range(2):
            at = part * tiles * shards + u * shards
            low.append(v_scr[at : at + SUB, :])
            high.append(v_scr[at + SUB : at + 2 * SUB, :])
            at = part * tiles * SUB + u * SUB
            mid.append(x_scr[at : at + SUB, :])
        groups[0].append(tuple(low))
        groups[1].append(tuple(jnp.where(is_first, mid[part], high[part]) for part in range(2)))
        groups[2].append(tuple(high))
    for group, values in enumerate(groups):
        for rho, value in enumerate(sixteen(values)):
            value = cmul(value, (between_ref[0, rho : rho + 1, :], between_ref[1, rho : rho + 1, :]))
            for part in range(2):
                t_scr[group, rho, part] = value[part]

    for rho in range(tiles):
        for part in range(2):
            back = tiles - 1 - rho
            low = jnp.concatenate([t_scr[0, rho, part], t_scr[1, rho, part]], axis=0)
            turned = jnp.where(lead, t_scr[2, rho, part], t_scr[0, back, part])
            high = jnp.concatenate([turned, t_scr[1, back, part]], axis=0)
            for k, tile in enumerate((low, high)):
                top, rest = halves(tile)
                rows = pl.ds(rho * PIECE + k * SLOTS, SLOTS)
                cols = pl.ds(part * LANES, LANES)
                dh_scr[rows, cols] = top
                dl_scr[rows, cols] = rest
    dims = (((1,), (1,)), ((), ()))
    dot_t = functools.partial(lax.dot_general, dimension_numbers=dims, preferred_element_type=F32)
    lane = lax.broadcasted_iota(jnp.int32, (half, 2 * LANES), 1)
    within = lane % PIECE
    from_low = jnp.logical_or(within < SLOTS, jnp.logical_and(within == SLOTS, is_first))
    scale = 1.0 / (shards * shards * tiles * LANES)
    powers = []
    for part in range(2):
        top = dh_scr[part * 256 : (part + 1) * 256, :]
        rest = dl_scr[part * 256 : (part + 1) * 256, :]
        z = dot_t(th_ref[...], top) + dot_t(th_ref[...], rest) + dot_t(tl_ref[...], top)
        z = z * z
        low = z[0:half] + z[half : 2 * half]
        high = z[2 * half : 3 * half] + z[3 * half :]
        powers.append(jnp.where(from_low, low, high) * scale)

    count = 2 * SLOTS * half * tiles

    def over_all(value):
        column = jnp.sum(value, axis=0, keepdims=True)
        return jnp.sum(column, axis=1, keepdims=True)

    mean = over_all(powers[0] + powers[1]) / count
    off0, off1 = powers[0] - mean, powers[1] - mean
    deviation = over_all(off0 * off0 + off1 * off1)
    stats = jnp.where(sub[0:1] + lax.broadcasted_iota(jnp.int32, (1, LANES), 1) < half, mean, deviation)
    for t in range(shards):
        o_ref[t * ROWS + 2 * SUB : (t + 1) * ROWS, :] = stats

    for group in range(4):
        value = powers[group // 2][:, (group % 2) * LANES : (group % 2 + 1) * LANES]
        for shift in range(4):
            at = (group * 4 + shift) * half
            r_scr[at : at + half, :] = pltpu.roll(value, shift * PIECE, 1) if shift else value
    lane8 = lax.broadcasted_iota(jnp.int32, (SUB, LANES), 1) // PIECE
    for chunk in range(CHUNKS):
        for g_pair in range(tiles // 2):
            parts = []
            for g0 in (2 * g_pair, 2 * g_pair + 1):
                tile = None
                for place in range(4):
                    h, c = PIECES[chunk * 4 + place]
                    rho, e = (h * g0 + c) % tiles, (h * g0 + c) // tiles
                    shift = (place - rho % 4) % 4
                    rows = pl.ds((rho // 4 * 4 + shift) * half + e, SUB, stride=h)
                    got = r_scr[rows, :]
                    tile = got if tile is None else jnp.where(lane8 == place, got, tile)
                parts.append(tile)
            top, rest = halves(jnp.concatenate(parts, axis=0))
            cols = pl.ds(chunk * LANES, LANES)
            l_scr[pl.ds(g_pair * 16, 16), cols] = top
            l_scr[pl.ds(LANES + g_pair * 16, 16), cols] = rest
    phi = lax.broadcasted_iota(jnp.int32, (SLOTS, COARSE), 1)
    slot = lax.broadcasted_iota(jnp.int32, (SLOTS, COARSE), 0)
    pairs = slot * SLOTS - jnp.where(slot < SUB, 0, SUB * SLOTS - SUB)
    mine = jnp.where(is_first, pairs, own_class + SLOTS * slot)
    mirror = jnp.where(mine == 0, COARSE // 2, COARSE - mine)
    for index, (h, c) in enumerate(PIECES):
        for k, residue in enumerate((mine, mirror)):
            hit = jnp.where(h * phi - COARSE * c == residue, 1.0, 0.0)
            s_scr[pl.ds(index * PIECE + k * SLOTS, SLOTS), :] = hit.astype(BF16)
    both = jnp.dot(l_scr[...], s_scr[...], preferred_element_type=F32)
    for tile in range(2):
        cols = slice(tile * LANES, (tile + 1) * LANES)
        h_scr[tile * LANES : (tile + 1) * LANES, :] = both[:LANES, cols] + both[LANES:, cols]
    for t in range(shards):
        for tile in range(2):
            rows = pl.ds(tile * LANES + (t % 2) * half + t // 2, SUB, stride=SUB)
            o_ref[t * ROWS + tile * SUB : t * ROWS + (tile + 1) * SUB, :] = h_scr[rows, :]


def third_kernel(m_ref, x_ref, hs_ref, msg_ref, level_ref):
    shards = x_ref.shape[0] // ROWS
    holders = shards // 2
    count = 2 * SLOTS * (LANES // 2) * SLOTS
    tiles = []
    for row in range(2):
        blocks = [(2 * r + row) * ROWS for r in range(holders)]
        sums = [x_ref[at : at + 2 * SUB, :] for at in blocks]
        stats = [x_ref[at + 2 * SUB : at + ROWS, :] for at in blocks]
        total, both = sums[0], stats[0]
        for r in range(1, holders):
            total, both = total + sums[r], both + stats[r]
        mean = both[:, 0:1] / holders
        spread = both[:, LANES // 2 : LANES // 2 + 1]
        for r in range(holders):
            off = stats[r][:, 0:1] - mean
            spread = spread + count * (off * off)
        scale = 1.0 / jnp.sqrt(spread / (count * holders) + EPSILON)
        tiles.append([(total[k * SUB : (k + 1) * SUB] - HARM * mean) * scale for k in range(2)])
    for row in range(2):
        for k in range(2):
            for g in range(SUB):
                hs_ref[row : row + 1, pl.ds(g * COARSE + k * LANES, LANES)] = tiles[row][k][g : g + 1]
    for k in range(2):
        level_ref[k * SUB : (k + 1) * SUB, :] = (tiles[0][k] + tiles[1][k]) / 2
    peak = jnp.concatenate([jnp.maximum(tiles[0][k], tiles[1][k]) for k in range(2)], axis=0)
    for e in range(m_ref.shape[0]):
        msg_ref[e * ROWS : e * ROWS + 2 * SUB, :] = peak
        msg_ref[e * ROWS + 2 * SUB : (e + 1) * ROWS, :] = m_ref[e : e + 1, :]


def sift_kernel(x_ref, level_ref, bins_ref, o_ref, hs_ref):
    hs_ref[...] = bins_ref[...]
    bands, slots = o_ref.shape[:2]
    level = level_ref[...]
    rows = bands * slots
    diff = jnp.concatenate([x_ref[d * ROWS : d * ROWS + 2 * SUB, :] - level for d in range(bands)], axis=0)
    lane = lax.broadcasted_iota(jnp.int32, (rows, LANES), 1)
    line = lax.broadcasted_iota(jnp.int32, (rows, LANES), 0)
    listed = [x_ref[d * ROWS + 2 * SUB : (d + 1) * ROWS, :] for d in range(bands)]
    listed = jnp.concatenate([jnp.broadcast_to(x, (slots, LANES)) for x in listed], axis=0)
    start = jnp.sum(jnp.where(lane == line % slots, listed, 0.0), axis=1, keepdims=True).astype(jnp.int32)
    block = jnp.maximum(start, 0)
    tile_id, offset = block // LANES, block % LANES

    def pick(which):
        place = (line // slots) * (2 * SUB) + (which % 2) * SUB + which // 2
        hit = jnp.logical_and(lane == place, which < 2 * SUB)
        return jnp.where(hit, 1.0, 0.0).astype(BF16)

    both = jnp.concatenate([pick(tile_id), pick(tile_id + 1)], axis=0)
    parts = jnp.dot(both, jnp.concatenate(halves(diff), axis=1), preferred_element_type=F32)
    parts = parts[:, :LANES] + parts[:, LANES:]
    joined = jnp.where(lane >= offset, parts[:rows], parts[rows:])
    moved = jnp.take_along_axis(joined, (lane + offset) % LANES, axis=1)
    moved = jnp.where(start >= 0, moved, 0.0)
    o_ref[...] = moved.reshape(bands, slots, LANES)


PARAMS = pltpu.CompilerParams(vmem_limit_bytes=16 * 2**20)


def near(array):
    return pltpu.with_memory_space_constraint(array, pltpu.VMEM)


def shape(*dims):
    return pltpu.VMEM(dims, F32)


def spaces(*kinds):
    return [pl.BlockSpec(memory_space=pltpu.SMEM if kind == "s" else pltpu.VMEM) for kind in kinds]


def run_first(me, received, first, starts, counts):
    shards = received.shape[0]
    inputs = [near(x) for x in (received, *map(jnp.asarray, first), starts, counts)]
    sent, markers = pl.pallas_call(
        first_kernel,
        out_shape=(shape(shards * 32, LANES), shape(starts.shape[0], LANES)),
        in_specs=spaces("s", *"vvvvv"),
        out_specs=spaces(*"vv"),
        scratch_shapes=[pltpu.VMEM((2, SUB, SLOTS, LANES), F32)],
        compiler_params=PARAMS,
    )(me, *inputs)
    return sent.reshape(shards, 32, LANES), markers


def run_second(me, received, second):
    shards = received.shape[0]
    inputs = [near(x) for x in (received, *map(jnp.asarray, second))]
    sent = pl.pallas_call(
        second_kernel,
        out_shape=shape(shards * ROWS, LANES),
        in_specs=spaces("s", *"vvvvvv"),
        out_specs=spaces("v")[0],
        scratch_shapes=[
            pltpu.VMEM((2 * SLOTS * SLOTS, LANES), F32),
            pltpu.VMEM((2 * SLOTS * SUB, LANES), F32),
            pltpu.VMEM((3, SLOTS, 2, SUB, LANES), F32),
            pltpu.VMEM((SLOTS * PIECE, 2 * LANES), BF16),
            pltpu.VMEM((SLOTS * PIECE, 2 * LANES), BF16),
            pltpu.VMEM((16 * LANES // 2, LANES), F32),
            pltpu.VMEM((2 * LANES, CHUNKS * LANES), BF16),
            pltpu.VMEM((CHUNKS * LANES, COARSE), BF16),
            pltpu.VMEM((2 * LANES, LANES), F32),
        ],
        compiler_params=PARAMS,
    )(me, *inputs)
    return sent.reshape(shards, 1, ROWS * LANES)


def run_third(received, markers):
    bands = markers.shape[0]
    bins, message, level = pl.pallas_call(
        third_kernel,
        out_shape=(shape(2, SUB * COARSE), shape(bands * ROWS, LANES), shape(2 * SUB, LANES)),
        in_specs=spaces(*"vv"),
        out_specs=spaces(*"vvv"),
        compiler_params=PARAMS,
    )(near(markers), near(received.reshape(-1, LANES)))
    return bins, message.reshape(bands, 1, ROWS * LANES), level


def run_sift(received, level, bins):
    bands = received.shape[0]
    return pl.pallas_call(
        sift_kernel,
        out_shape=(
            jax.ShapeDtypeStruct((bands, 2 * SUB, LANES), F32),
            jax.ShapeDtypeStruct(bins.shape, F32),
        ),
        in_specs=spaces(*"vvv"),
        out_specs=spaces(*"vv"),
        compiler_params=PARAMS,
    )(near(received.reshape(-1, LANES)), near(level), near(bins))


def per_device(series, cand_start, cand_count):
    shards = lax.axis_size("tm")
    first, second = tables(shards, shards * series.shape[1])
    me, series = lax.optimization_barrier((lax.axis_index("tm").astype(jnp.int32).reshape(1), series))
    swap = functools.partial(lax.all_to_all, split_axis=0, concat_axis=0, tiled=True)
    samples = swap(jnp.swapaxes(series.reshape(2, shards, -1), 0, 1), "tm")
    sent, markers = run_first(me, samples, first, cand_start[0, 0], cand_count[0])
    sums = swap(run_second(me, swap(sent, "tm"), second), "tm")
    bins, message, level = run_third(sums, markers)
    sifted, harmonic_sum = run_sift(swap(message, "dm"), level, bins)
    return harmonic_sum, sifted[None, None]


def solution(mesh):
    return jax.shard_map(
        per_device,
        mesh=mesh,
        in_specs=(
            P(("beam", "dm"), "tm"),
            P(("beam", "tm"), "dm", None, None),
            P(("beam", "tm"), "dm", None),
        ),
        out_specs=(P(("beam", "dm"), "tm"), P(("beam", "tm"), "dm", None, None, None)),
        check_vma=False,
    )
```

```python
import functools
import math

import jax
import jax.numpy as jnp
import numpy as np
from jax import lax
from jax.experimental import pallas as pl
from jax.experimental.pallas import tpu as pltpu
from jax.sharding import PartitionSpec as P

HARM = 8
BW = 128
EPSILON = 1e-06

LANES = 128
SUB = 8
COARSE = 256
SLOTS = 16
PIECE = 32
PIECES = [(h, c) for h in range(1, HARM + 1) for c in range(h)]
CHUNKS = len(PIECES) // 4
ROWS = 2 * SUB + 1

F32 = jnp.float32
BF16 = jnp.bfloat16


def halves(value):
    top = value.astype(BF16)
    return top, (value - top.astype(F32)).astype(BF16)


def np_halves(value):
    top = value.astype(np.float32).astype(BF16)
    rest = (value - top.astype(np.float64)).astype(np.float32).astype(BF16)
    return top, rest


def unit(turns, period):
    angle = -2.0 * math.pi * (turns % period) / period
    return np.cos(angle), np.sin(angle)


@functools.cache
def tables(shards, samples):
    part = samples // (shards * shards)
    tiles = part // LANES
    m = np.arange(part)
    v = np.arange(LANES)
    s = np.arange(shards)
    half = shards // 2
    r = np.arange(half)
    within = np.stack(unit(r[:, None] * m[None, :], samples)).reshape(2, half, tiles, LANES)
    shift = np.stack(unit(s[:, None] * r[None, :], shards * shards), axis=1)
    shift = np.broadcast_to(shift[..., None], (shards, 2, half, LANES))
    after = np.stack(unit(s[:, None] * m[None, :], samples // shards)).reshape(2, shards, tiles, LANES)
    middle = (half + shards * r)[:, None] * m[None, :]
    middle = np.stack(unit(middle, samples)).reshape(2, half, tiles, LANES)
    between = np.stack(unit(s[:, None] * v[None, :], part))
    j = np.arange(LANES // 2)
    rows = []
    for q2 in (j, LANES - 1 - j):
        c2, s2 = unit(q2[:, None] * v[None, :], LANES)
        rows += [np.concatenate([c2, -s2], axis=1), np.concatenate([s2, c2], axis=1)]
    last = np_halves(np.concatenate(rows, axis=0))
    first = [x.astype(np.float32) for x in (within, shift)]
    second = [x.astype(np.float32) for x in (after, middle, between)] + list(last)
    return first, second


def cmul(x, y):
    if x[1] is None:
        return x[0] * y[0], x[0] * y[1]
    return x[0] * y[0] - x[1] * y[1], x[0] * y[1] + x[1] * y[0]


def plus(a, b):
    return b if a is None else a if b is None else a + b


def minus(a, b):
    return a if b is None else -b if a is None else a - b


def cadd(x, y):
    return plus(x[0], y[0]), plus(x[1], y[1])


def csub(x, y):
    return minus(x[0], y[0]), minus(x[1], y[1])


def turn_back(x):
    return x[1], minus(None, x[0])


def four(x0, x1, x2, x3):
    s, d = cadd(x0, x2), csub(x0, x2)
    t, u = cadd(x1, x3), turn_back(csub(x1, x3))
    return cadd(s, t), cadd(d, u), csub(s, t), csub(d, u)


def sixteen(values):
    columns = [four(*values[low::4]) for low in range(4)]
    out = [None] * 16
    for k1 in range(4):
        terms = []
        for low in range(4):
            term = columns[low][k1]
            if low * k1 == 4:
                term = turn_back(term)
            elif low * k1:
                c, s = unit(np.float64(low * k1), 16)
                term = cmul(term, (F32(c), F32(s)))
            terms.append(term)
        for k2, value in enumerate(four(*terms)):
            out[k1 + 4 * k2] = value
    return out


def prepare_kernel(d_ref, within_ref, shift_ref, start_ref, count_ref, w_ref, s_ref, m_ref):
    me = d_ref[0]
    own_class = me // 2
    for r in range(1, w_ref.shape[1]):
        own = [shift_ref[me, part, r : r + 1, :] for part in range(2)]
        twiddle = cmul((within_ref[0, r], within_ref[1, r]), own)
        for part in range(2):
            w_ref[part, r] = twiddle[part]

    phi = lax.broadcasted_iota(jnp.int32, (SLOTS, COARSE), 1)
    slot = lax.broadcasted_iota(jnp.int32, (SLOTS, COARSE), 0)
    pairs = slot * SLOTS - jnp.where(slot < SUB, 0, SUB * SLOTS - SUB)
    mine = jnp.where(own_class == 0, pairs, own_class + SLOTS * slot)
    mirror = jnp.where(mine == 0, COARSE // 2, COARSE - mine)
    for index, (h, c) in enumerate(PIECES):
        for k, residue in enumerate((mine, mirror)):
            hit = jnp.where(h * phi - COARSE * c == residue, 1.0, 0.0)
            s_ref[pl.ds(index * PIECE + k * SLOTS, SLOTS), :] = hit.astype(BF16)

    bands, slots = start_ref.shape
    cell = [lax.broadcasted_iota(jnp.int32, (bands, bands), axis) for axis in range(2)]
    counts = jnp.where(cell[0] == cell[1], count_ref[...].astype(F32), 0.0)
    live = jnp.sum(counts, axis=1, keepdims=True).astype(jnp.int32)
    slot = lax.broadcasted_iota(jnp.int32, (bands, slots), 1)
    starts = jnp.where(slot < live, start_ref[...], -1).astype(F32)
    m_ref[...] = jnp.concatenate([starts] * (LANES // slots), axis=1)


def first_kernel(x_ref, w_ref, o_ref):
    shards = x_ref.shape[0]
    tiles = x_ref.shape[1] // 2
    flat = x_ref.reshape(shards * 2 * tiles, LANES)
    half = shards // 2
    for row in range(2):
        for k in range(tiles // SUB):
            inner = slice(k * SUB, (k + 1) * SUB)
            at = [(t * tiles + k * SUB) * 2 + row for t in range(shards)]
            classes = sixteen([(flat[pl.ds(x, SUB, stride=2), :], None) for x in at])
            for r in range(half):
                if r:
                    value = cmul(classes[r], [w_ref[part, r, inner, :] for part in range(2)])
                else:
                    value = classes[0][0], classes[half][0]
                for part in range(2):
                    to = part * tiles + k * SUB
                    o_ref[2 * r + row, to : to + SUB, :] = value[part]


def second_kernel(d_ref, x_ref, after_ref, middle_ref, between_ref, th_ref, tl_ref, s_ref, o_ref, v_scr, x_scr, t_scr, dh_scr, dl_scr, r_scr, l_scr, h_scr):
    shards = x_ref.shape[0]
    tiles = x_ref.shape[1] // 2
    half = LANES // 2
    own_class = d_ref[0] // 2
    is_first = own_class == 0
    sub = lax.broadcasted_iota(jnp.int32, (SUB, LANES), 0)
    lead = jnp.logical_and(sub == 0, is_first)

    for k in range(tiles // SUB):
        rows = slice(k * SUB, (k + 1) * SUB)
        main, middle = [], []
        for s in range(shards):
            re = x_ref[s, k * SUB : (k + 1) * SUB, :]
            im = x_ref[s, tiles + k * SUB : tiles + (k + 1) * SUB, :]
            main.append((re, jnp.where(is_first, 0.0, im)))
            c, sn = unit(np.float64(s), 2 * shards)
            middle.append((im * F32(c), im * F32(sn) if s else None))
        for slot, value in enumerate(sixteen(main)):
            value = cmul(value, (after_ref[0, slot, rows, :], after_ref[1, slot, rows, :]))
            for part in range(2):
                v_scr[pl.ds(part * tiles * shards + k * SUB * shards + slot, SUB, stride=shards), :] = value[part]
        for slot, value in enumerate(sixteen(middle)[: shards // 2]):
            value = cmul(value, (middle_ref[0, slot, rows, :], middle_ref[1, slot, rows, :]))
            for part in range(2):
                at = part * tiles * SUB + k * SUB * SUB + slot
                x_scr[pl.ds(at, SUB, stride=SUB), :] = value[part]

    groups = [[], [], []]
    for u in range(tiles):
        low, high, mid = [], [], []
        for part in range(2):
            at = part * tiles * shards + u * shards
            low.append(v_scr[at : at + SUB, :])
            high.append(v_scr[at + SUB : at + 2 * SUB, :])
            at = part * tiles * SUB + u * SUB
            mid.append(x_scr[at : at + SUB, :])
        groups[0].append(tuple(low))
        groups[1].append(tuple(jnp.where(is_first, mid[part], high[part]) for part in range(2)))
        groups[2].append(tuple(high))
    for group, values in enumerate(groups):
        for rho, value in enumerate(sixteen(values)):
            value = cmul(value, (between_ref[0, rho : rho + 1, :], between_ref[1, rho : rho + 1, :]))
            for part in range(2):
                t_scr[group, rho, part] = value[part]

    for rho in range(tiles):
        for part in range(2):
            back = tiles - 1 - rho
            low = jnp.concatenate([t_scr[0, rho, part], t_scr[1, rho, part]], axis=0)
            turned = jnp.where(lead, t_scr[2, rho, part], t_scr[0, back, part])
            high = jnp.concatenate([turned, t_scr[1, back, part]], axis=0)
            for k, tile in enumerate((low, high)):
                top, rest = halves(tile)
                rows = pl.ds(rho * PIECE + k * SLOTS, SLOTS)
                cols = pl.ds(part * LANES, LANES)
                dh_scr[rows, cols] = top
                dl_scr[rows, cols] = rest
    dims = (((1,), (1,)), ((), ()))
    dot_t = functools.partial(lax.dot_general, dimension_numbers=dims, preferred_element_type=F32)
    lane = lax.broadcasted_iota(jnp.int32, (half, 2 * LANES), 1)
    within = lane % PIECE
    from_low = jnp.logical_or(within < SLOTS, jnp.logical_and(within == SLOTS, is_first))
    scale = 1.0 / (shards * shards * tiles * LANES)
    powers = []
    for part in range(2):
        top = dh_scr[part * 256 : (part + 1) * 256, :]
        rest = dl_scr[part * 256 : (part + 1) * 256, :]
        z = dot_t(th_ref[...], top) + dot_t(th_ref[...], rest) + dot_t(tl_ref[...], top)
        z = z * z
        low = z[0:half] + z[half : 2 * half]
        high = z[2 * half : 3 * half] + z[3 * half :]
        powers.append(jnp.where(from_low, low, high) * scale)

    count = 2 * SLOTS * half * tiles

    def over_all(value):
        column = jnp.sum(value, axis=0, keepdims=True)
        return jnp.sum(column, axis=1, keepdims=True)

    mean = over_all(powers[0] + powers[1]) / count
    off0, off1 = powers[0] - mean, powers[1] - mean
    deviation = over_all(off0 * off0 + off1 * off1)
    stats = jnp.where(sub[0:1] + lax.broadcasted_iota(jnp.int32, (1, LANES), 1) < half, mean, deviation)
    for t in range(shards):
        o_ref[t * ROWS + 2 * SUB : (t + 1) * ROWS, :] = stats

    for group in range(4):
        value = powers[group // 2][:, (group % 2) * LANES : (group % 2 + 1) * LANES]
        for shift in range(4):
            at = (group * 4 + shift) * half
            r_scr[at : at + half, :] = pltpu.roll(value, shift * PIECE, 1) if shift else value
    lane8 = lax.broadcasted_iota(jnp.int32, (SUB, LANES), 1) // PIECE
    for chunk in range(CHUNKS):
        for g_pair in range(tiles // 2):
            parts = []
            for g0 in (2 * g_pair, 2 * g_pair + 1):
                tile = None
                for place in range(4):
                    h, c = PIECES[chunk * 4 + place]
                    rho, e = (h * g0 + c) % tiles, (h * g0 + c) // tiles
                    shift = (place - rho % 4) % 4
                    rows = pl.ds((rho // 4 * 4 + shift) * half + e, SUB, stride=h)
                    got = r_scr[rows, :]
                    tile = got if tile is None else jnp.where(lane8 == place, got, tile)
                parts.append(tile)
            top, rest = halves(jnp.concatenate(parts, axis=0))
            cols = pl.ds(chunk * LANES, LANES)
            l_scr[pl.ds(g_pair * 16, 16), cols] = top
            l_scr[pl.ds(LANES + g_pair * 16, 16), cols] = rest
    both = jnp.dot(l_scr[...], s_ref[...], preferred_element_type=F32)
    for tile in range(2):
        cols = slice(tile * LANES, (tile + 1) * LANES)
        h_scr[tile * LANES : (tile + 1) * LANES, :] = both[:LANES, cols] + both[LANES:, cols]
    for t in range(shards):
        for tile in range(2):
            rows = pl.ds(tile * LANES + (t % 2) * half + t // 2, SUB, stride=SUB)
            o_ref[t * ROWS + tile * SUB : t * ROWS + (tile + 1) * SUB, :] = h_scr[rows, :]


def third_kernel(m_ref, x_ref, hs_ref, msg_ref, level_ref):
    shards = x_ref.shape[0] // ROWS
    holders = shards // 2
    count = 2 * SLOTS * (LANES // 2) * SLOTS
    tiles = []
    for row in range(2):
        blocks = [(2 * r + row) * ROWS for r in range(holders)]
        sums = [x_ref[at : at + 2 * SUB, :] for at in blocks]
        stats = [x_ref[at + 2 * SUB : at + ROWS, :] for at in blocks]
        total, both = sums[0], stats[0]
        for r in range(1, holders):
            total, both = total + sums[r], both + stats[r]
        mean = both[:, 0:1] / holders
        spread = both[:, LANES // 2 : LANES // 2 + 1]
        for r in range(holders):
            off = stats[r][:, 0:1] - mean
            spread = spread + count * (off * off)
        scale = 1.0 / jnp.sqrt(spread / (count * holders) + EPSILON)
        tiles.append([(total[k * SUB : (k + 1) * SUB] - HARM * mean) * scale for k in range(2)])
    for row in range(2):
        for k in range(2):
            for g in range(SUB):
                hs_ref[row : row + 1, pl.ds(g * COARSE + k * LANES, LANES)] = tiles[row][k][g : g + 1]
    for k in range(2):
        level_ref[k * SUB : (k + 1) * SUB, :] = (tiles[0][k] + tiles[1][k]) / 2
    peak = jnp.concatenate([jnp.maximum(tiles[0][k], tiles[1][k]) for k in range(2)], axis=0)
    for e in range(m_ref.shape[0]):
        msg_ref[e * ROWS : e * ROWS + 2 * SUB, :] = peak
        msg_ref[e * ROWS + 2 * SUB : (e + 1) * ROWS, :] = m_ref[e : e + 1, :]


def sift_kernel(x_ref, level_ref, bins_ref, o_ref, hs_ref, out_scr, sems):
    steps = sems.shape[0] - 1
    bins_out = pltpu.make_async_copy(bins_ref, hs_ref, sems.at[steps])
    bins_out.start()
    bands, slots = o_ref.shape[:2]
    level = level_ref[...]
    rows = bands * slots
    diff = jnp.concatenate([x_ref[d * ROWS : d * ROWS + 2 * SUB, :] - level for d in range(bands)], axis=0)
    lane = lax.broadcasted_iota(jnp.int32, (rows, LANES), 1)
    line = lax.broadcasted_iota(jnp.int32, (rows, LANES), 0)
    listed = [x_ref[d * ROWS + 2 * SUB : (d + 1) * ROWS, :] for d in range(bands)]
    listed = jnp.concatenate([jnp.broadcast_to(x, (slots, LANES)) for x in listed], axis=0)
    start = jnp.sum(jnp.where(lane == line & (slots - 1), listed, 0.0), axis=1, keepdims=True)
    start = jnp.broadcast_to(start, (rows, LANES)).astype(jnp.int32)
    block = jnp.maximum(start, 0)
    tile_id, offset = block >> 7, block & (LANES - 1)
    band = line & -slots

    def pick(which):
        place = band + ((which & 1) << 3) + (which >> 1)
        return jnp.where(lane == place, 1.0, 0.0).astype(BF16)

    both = jnp.concatenate([pick(tile_id), pick(tile_id + 1)], axis=0)
    parts = jnp.dot(both, jnp.concatenate(halves(diff), axis=1), preferred_element_type=F32)
    parts = parts[:, :LANES] + parts[:, LANES:]
    copies = []
    for step in range(steps):
        part = slice(step * rows // steps, (step + 1) * rows // steps)
        joined = jnp.where(lane[part] >= offset[part], parts[:rows][part], parts[rows:][part])
        moved = jnp.take_along_axis(joined, (lane[part] + offset[part]) & (LANES - 1), axis=1)
        moved = jnp.where(start[part] >= 0, moved, 0.0)
        here = pl.ds(step * bands // steps, bands // steps)
        out_scr[here] = moved.reshape(bands // steps, slots, LANES)
        copies.append(pltpu.make_async_copy(out_scr.at[here], o_ref.at[here], sems.at[step]))
        copies[-1].start()
    for copy in copies:
        copy.wait()
    bins_out.wait()


PARAMS = pltpu.CompilerParams(vmem_limit_bytes=16 * 2**20)


def near(array):
    return pltpu.with_memory_space_constraint(array, pltpu.VMEM)


def shape(*dims):
    return pltpu.VMEM(dims, F32)


def spaces(*kinds):
    return [pl.BlockSpec(memory_space=pltpu.SMEM if kind == "s" else pltpu.VMEM) for kind in kinds]


def run_prepare(me, first, starts, counts):
    within, shift = map(jnp.asarray, first)
    return pl.pallas_call(
        prepare_kernel,
        out_shape=(
            shape(*within.shape),
            pltpu.VMEM((CHUNKS * LANES, COARSE), BF16),
            shape(starts.shape[0], LANES),
        ),
        in_specs=spaces("s", *"vvvv"),
        out_specs=spaces(*"vvv"),
        compiler_params=PARAMS,
    )(me, *[near(x) for x in (within, shift, starts, counts)])


def run_first(received, twiddles):
    return pl.pallas_call(
        first_kernel,
        out_shape=shape(*received.shape),
        in_specs=spaces(*"vv"),
        out_specs=spaces("v")[0],
        compiler_params=PARAMS,
    )(near(received), near(twiddles))


def run_second(me, received, second, mapping):
    shards = received.shape[0]
    inputs = [near(x) for x in (received, *map(jnp.asarray, second), mapping)]
    sent = pl.pallas_call(
        second_kernel,
        out_shape=shape(shards * ROWS, LANES),
        in_specs=spaces("s", *"vvvvvvv"),
        out_specs=spaces("v")[0],
        scratch_shapes=[
            pltpu.VMEM((2 * SLOTS * SLOTS, LANES), F32),
            pltpu.VMEM((2 * SLOTS * SUB, LANES), F32),
            pltpu.VMEM((3, SLOTS, 2, SUB, LANES), F32),
            pltpu.VMEM((SLOTS * PIECE, 2 * LANES), BF16),
            pltpu.VMEM((SLOTS * PIECE, 2 * LANES), BF16),
            pltpu.VMEM((16 * LANES // 2, LANES), F32),
            pltpu.VMEM((2 * LANES, CHUNKS * LANES), BF16),
            pltpu.VMEM((2 * LANES, LANES), F32),
        ],
        compiler_params=PARAMS,
    )(me, *inputs)
    return sent.reshape(shards, 1, ROWS * LANES)


def run_third(received, markers):
    bands = markers.shape[0]
    bins, message, level = pl.pallas_call(
        third_kernel,
        out_shape=(shape(2, SUB * COARSE), shape(bands * ROWS, LANES), shape(2 * SUB, LANES)),
        in_specs=spaces(*"vv"),
        out_specs=spaces(*"vvv"),
        compiler_params=PARAMS,
    )(near(markers), near(received.reshape(-1, LANES)))
    return bins, message.reshape(bands, 1, ROWS * LANES), level


def run_sift(received, level, bins):
    bands = received.shape[0]
    steps = bands // 2
    anywhere = pl.BlockSpec(memory_space=pl.ANY)
    return pl.pallas_call(
        sift_kernel,
        out_shape=(
            jax.ShapeDtypeStruct((bands, 2 * SUB, LANES), F32),
            jax.ShapeDtypeStruct(bins.shape, F32),
        ),
        in_specs=spaces(*"vvv"),
        out_specs=[anywhere, anywhere],
        scratch_shapes=[
            pltpu.VMEM((bands, 2 * SUB, LANES), F32),
            pltpu.SemaphoreType.DMA((steps + 1,)),
        ],
        compiler_params=PARAMS,
    )(near(received.reshape(-1, LANES)), near(level), near(bins))


def per_device(series, cand_start, cand_count):
    shards = lax.axis_size("tm")
    first, second = tables(shards, shards * series.shape[1])
    me = lax.axis_index("tm").astype(jnp.int32).reshape(1)
    swap = functools.partial(lax.all_to_all, split_axis=0, concat_axis=0, tiled=True)
    blocks = series.reshape(2, shards, -1, LANES).transpose(1, 2, 0, 3).reshape(shards, -1, LANES)
    samples = swap(blocks, "tm")
    twiddles, mapping, markers = run_prepare(me, first, cand_start[0, 0], cand_count[0])
    classes = swap(run_first(samples, twiddles), "tm")
    sums = swap(run_second(me, classes, second, mapping), "tm")
    bins, message, level = run_third(sums, markers)
    sifted, harmonic_sum = run_sift(swap(message, "dm"), level, bins)
    return harmonic_sum, sifted[None, None]


def solution(mesh):
    return jax.shard_map(
        per_device,
        mesh=mesh,
        in_specs=(
            P(("beam", "dm"), "tm"),
            P(("beam", "tm"), "dm", None, None),
            P(("beam", "tm"), "dm", None),
        ),
        out_specs=(P(("beam", "dm"), "tm"), P(("beam", "tm"), "dm", None, None, None)),
        check_vma=False,
    )
```

```python
import functools
import math

import jax
import jax.numpy as jnp
import numpy as np
from jax import lax
from jax.experimental import pallas as pl
from jax.experimental.pallas import tpu as pltpu
from jax.sharding import PartitionSpec as P

HARM = 8
BW = 128
EPSILON = 1e-06

LANES = 128
SUB = 8
COARSE = 256
SLOTS = 16
PIECE = 32
PIECES = [(h, c) for h in range(1, HARM + 1) for c in range(h)]
CHUNKS = len(PIECES) // 4
ROWS = 2 * SUB + 1

F32 = jnp.float32
BF16 = jnp.bfloat16


def halves(value):
    top = value.astype(BF16)
    return top, (value - top.astype(F32)).astype(BF16)


def np_halves(value):
    top = value.astype(np.float32).astype(BF16)
    rest = (value - top.astype(np.float64)).astype(np.float32).astype(BF16)
    return top, rest


def unit(turns, period):
    angle = -2.0 * math.pi * (turns % period) / period
    return np.cos(angle), np.sin(angle)


@functools.cache
def tables(shards, samples):
    part = samples // (shards * shards)
    tiles = part // LANES
    m = np.arange(part)
    v = np.arange(LANES)
    s = np.arange(shards)
    half = shards // 2
    r = np.arange(half)
    wide = np.arange(2 * part)
    within = np.stack(unit(r[:, None] * wide[None, :], samples)).reshape(2, half, 2 * tiles, LANES)
    shift = np.stack(unit(r[:, None] * r[None, :], samples // (2 * part)), axis=1)
    shift = np.broadcast_to(shift[..., None], (half, 2, half, LANES))
    after = np.stack(unit(s[:, None] * m[None, :], samples // shards)).reshape(2, shards, tiles, LANES)
    middle = (half + shards * r)[:, None] * m[None, :]
    middle = np.stack(unit(middle, samples)).reshape(2, half, tiles, LANES)
    between = np.stack(unit(s[:, None] * v[None, :], part))
    j = np.arange(LANES // 2)
    rows = []
    for q2 in (j, LANES - 1 - j):
        c2, s2 = unit(q2[:, None] * v[None, :], LANES)
        rows += [np.concatenate([c2, -s2], axis=1), np.concatenate([s2, c2], axis=1)]
    last = np_halves(np.concatenate(rows, axis=0))
    first = [x.astype(np.float32) for x in (within, shift)]
    second = [x.astype(np.float32) for x in (after, middle, between)] + list(last)
    return first, second


def cmul(x, y):
    if x[1] is None:
        return x[0] * y[0], x[0] * y[1]
    return x[0] * y[0] - x[1] * y[1], x[0] * y[1] + x[1] * y[0]


def plus(a, b):
    return b if a is None else a if b is None else a + b


def minus(a, b):
    return a if b is None else -b if a is None else a - b


def cadd(x, y):
    return plus(x[0], y[0]), plus(x[1], y[1])


def csub(x, y):
    return minus(x[0], y[0]), minus(x[1], y[1])


def turn_back(x):
    return x[1], minus(None, x[0])


def four(x0, x1, x2, x3):
    s, d = cadd(x0, x2), csub(x0, x2)
    t, u = cadd(x1, x3), turn_back(csub(x1, x3))
    return cadd(s, t), cadd(d, u), csub(s, t), csub(d, u)


def sixteen(values):
    columns = [four(*values[low::4]) for low in range(4)]
    out = [None] * 16
    for k1 in range(4):
        terms = []
        for low in range(4):
            term = columns[low][k1]
            if low * k1 == 4:
                term = turn_back(term)
            elif low * k1:
                c, s = unit(np.float64(low * k1), 16)
                term = cmul(term, (F32(c), F32(s)))
            terms.append(term)
        for k2, value in enumerate(four(*terms)):
            out[k1 + 4 * k2] = value
    return out


def prepare_kernel(d_ref, within_ref, shift_ref, start_ref, count_ref, w_ref, s_ref, m_ref):
    own_class = d_ref[0] % w_ref.shape[1]
    for r in range(1, w_ref.shape[1]):
        own = [shift_ref[own_class, part, r : r + 1, :] for part in range(2)]
        twiddle = cmul((within_ref[0, r], within_ref[1, r]), own)
        for part in range(2):
            w_ref[part, r] = twiddle[part]

    phi = lax.broadcasted_iota(jnp.int32, (SLOTS, COARSE), 1)
    slot = lax.broadcasted_iota(jnp.int32, (SLOTS, COARSE), 0)
    pairs = slot * SLOTS - jnp.where(slot < SUB, 0, SUB * SLOTS - SUB)
    mine = jnp.where(own_class == 0, pairs, own_class + SLOTS * slot)
    mirror = jnp.where(mine == 0, COARSE // 2, COARSE - mine)
    for index, (h, c) in enumerate(PIECES):
        for k, residue in enumerate((mine, mirror)):
            hit = jnp.where(h * phi - COARSE * c == residue, 1.0, 0.0)
            s_ref[pl.ds(index * PIECE + k * SLOTS, SLOTS), :] = hit.astype(BF16)

    bands, slots = start_ref.shape
    cell = [lax.broadcasted_iota(jnp.int32, (bands, bands), axis) for axis in range(2)]
    counts = jnp.where(cell[0] == cell[1], count_ref[...].astype(F32), 0.0)
    live = jnp.sum(counts, axis=1, keepdims=True).astype(jnp.int32)
    slot = lax.broadcasted_iota(jnp.int32, (bands, slots), 1)
    starts = jnp.where(slot < live, start_ref[...], -1).astype(F32)
    m_ref[...] = jnp.concatenate([starts] * (LANES // slots), axis=1)


def separate_kernel(x_ref, o_ref, sems):
    count = sems.shape[1]
    size = x_ref.shape[0] // count
    copies = []
    for row in range(2):
        for part in range(count):
            here = pl.ds(part * size, size)
            copies.append(pltpu.make_async_copy(x_ref.at[here, row], o_ref.at[row, here], sems.at[row, part]))
            copies[-1].start()
    for copy in copies:
        copy.wait()


def first_kernel(x_ref, w_ref, o_ref):
    shards, tiles = x_ref.shape[:2]
    half = shards // 2
    for k in range(tiles // SUB):
        inner = slice(k * SUB, (k + 1) * SUB)
        classes = sixteen([(x_ref[t, inner, :], None) for t in range(shards)])
        for r in range(half):
            if r:
                value = cmul(classes[r], [w_ref[part, r, inner, :] for part in range(2)])
            else:
                value = classes[0][0], classes[half][0]
            for part in range(2):
                to = part * tiles + k * SUB
                o_ref[r, to : to + SUB, :] = value[part]


def second_kernel(d_ref, x_ref, after_ref, middle_ref, between_ref, th_ref, tl_ref, s_ref, o_ref, v_scr, x_scr, t_scr, dh_scr, dl_scr, r_scr, l_scr, h_scr):
    shards = 2 * x_ref.shape[0]
    tiles = x_ref.shape[1] // 4
    half = LANES // 2
    own_class = d_ref[0] % x_ref.shape[0]
    is_first = own_class == 0
    sub = lax.broadcasted_iota(jnp.int32, (SUB, LANES), 0)
    lead = jnp.logical_and(sub == 0, is_first)

    for k in range(tiles // SUB):
        rows = slice(k * SUB, (k + 1) * SUB)
        main, middle = [], []
        for s in range(shards):
            at = s % 2 * tiles + k * SUB
            re = x_ref[s // 2, at : at + SUB, :]
            im = x_ref[s // 2, 2 * tiles + at : 2 * tiles + at + SUB, :]
            main.append((re, jnp.where(is_first, 0.0, im)))
            c, sn = unit(np.float64(s), 2 * shards)
            middle.append((im * F32(c), im * F32(sn) if s else None))
        for slot, value in enumerate(sixteen(main)):
            value = cmul(value, (after_ref[0, slot, rows, :], after_ref[1, slot, rows, :]))
            for part in range(2):
                v_scr[pl.ds(part * tiles * shards + k * SUB * shards + slot, SUB, stride=shards), :] = value[part]
        for slot, value in enumerate(sixteen(middle)[: shards // 2]):
            value = cmul(value, (middle_ref[0, slot, rows, :], middle_ref[1, slot, rows, :]))
            for part in range(2):
                at = part * tiles * SUB + k * SUB * SUB + slot
                x_scr[pl.ds(at, SUB, stride=SUB), :] = value[part]

    groups = [[], [], []]
    for u in range(tiles):
        low, high, mid = [], [], []
        for part in range(2):
            at = part * tiles * shards + u * shards
            low.append(v_scr[at : at + SUB, :])
            high.append(v_scr[at + SUB : at + 2 * SUB, :])
            at = part * tiles * SUB + u * SUB
            mid.append(x_scr[at : at + SUB, :])
        groups[0].append(tuple(low))
        groups[1].append(tuple(jnp.where(is_first, mid[part], high[part]) for part in range(2)))
        groups[2].append(tuple(high))
    for group, values in enumerate(groups):
        for rho, value in enumerate(sixteen(values)):
            value = cmul(value, (between_ref[0, rho : rho + 1, :], between_ref[1, rho : rho + 1, :]))
            for part in range(2):
                t_scr[group, rho, part] = value[part]

    for rho in range(tiles):
        for part in range(2):
            back = tiles - 1 - rho
            low = jnp.concatenate([t_scr[0, rho, part], t_scr[1, rho, part]], axis=0)
            turned = jnp.where(lead, t_scr[2, rho, part], t_scr[0, back, part])
            high = jnp.concatenate([turned, t_scr[1, back, part]], axis=0)
            for k, tile in enumerate((low, high)):
                top, rest = halves(tile)
                rows = pl.ds(rho * PIECE + k * SLOTS, SLOTS)
                cols = pl.ds(part * LANES, LANES)
                dh_scr[rows, cols] = top
                dl_scr[rows, cols] = rest
    dims = (((1,), (1,)), ((), ()))
    dot_t = functools.partial(lax.dot_general, dimension_numbers=dims, preferred_element_type=F32)
    lane = lax.broadcasted_iota(jnp.int32, (half, 2 * LANES), 1)
    within = lane % PIECE
    from_low = jnp.logical_or(within < SLOTS, jnp.logical_and(within == SLOTS, is_first))
    scale = 1.0 / (shards * shards * tiles * LANES)
    powers = []
    for part in range(2):
        top = dh_scr[part * 256 : (part + 1) * 256, :]
        rest = dl_scr[part * 256 : (part + 1) * 256, :]
        z = dot_t(th_ref[...], top) + dot_t(th_ref[...], rest) + dot_t(tl_ref[...], top)
        z = z * z
        low = z[0:half] + z[half : 2 * half]
        high = z[2 * half : 3 * half] + z[3 * half :]
        powers.append(jnp.where(from_low, low, high) * scale)

    count = 2 * SLOTS * half * tiles

    def over_all(value):
        column = jnp.sum(value, axis=0, keepdims=True)
        return jnp.sum(column, axis=1, keepdims=True)

    mean = over_all(powers[0] + powers[1]) / count
    off0, off1 = powers[0] - mean, powers[1] - mean
    deviation = over_all(off0 * off0 + off1 * off1)
    stats = jnp.where(sub[0:1] + lax.broadcasted_iota(jnp.int32, (1, LANES), 1) < half, mean, deviation)
    for t in range(shards):
        o_ref[t * ROWS + 2 * SUB : (t + 1) * ROWS, :] = stats

    for group in range(4):
        value = powers[group // 2][:, (group % 2) * LANES : (group % 2 + 1) * LANES]
        for shift in range(4):
            at = (group * 4 + shift) * half
            r_scr[at : at + half, :] = pltpu.roll(value, shift * PIECE, 1) if shift else value
    lane8 = lax.broadcasted_iota(jnp.int32, (SUB, LANES), 1) // PIECE
    for chunk in range(CHUNKS):
        for g_pair in range(tiles // 2):
            parts = []
            for g0 in (2 * g_pair, 2 * g_pair + 1):
                tile = None
                for place in range(4):
                    h, c = PIECES[chunk * 4 + place]
                    rho, e = (h * g0 + c) % tiles, (h * g0 + c) // tiles
                    shift = (place - rho % 4) % 4
                    rows = pl.ds((rho // 4 * 4 + shift) * half + e, SUB, stride=h)
                    got = r_scr[rows, :]
                    tile = got if tile is None else jnp.where(lane8 == place, got, tile)
                parts.append(tile)
            top, rest = halves(jnp.concatenate(parts, axis=0))
            cols = pl.ds(chunk * LANES, LANES)
            l_scr[pl.ds(g_pair * 16, 16), cols] = top
            l_scr[pl.ds(LANES + g_pair * 16, 16), cols] = rest
    both = jnp.dot(l_scr[...], s_ref[...], preferred_element_type=F32)
    for tile in range(2):
        cols = slice(tile * LANES, (tile + 1) * LANES)
        h_scr[tile * LANES : (tile + 1) * LANES, :] = both[:LANES, cols] + both[LANES:, cols]
    for t in range(shards):
        for tile in range(2):
            rows = pl.ds(tile * LANES + (t % 2) * half + t // 2, SUB, stride=SUB)
            o_ref[t * ROWS + tile * SUB : t * ROWS + (tile + 1) * SUB, :] = h_scr[rows, :]


def third_kernel(m_ref, x_ref, hs_ref, msg_ref, level_ref):
    shards = x_ref.shape[0] // ROWS
    holders = shards // 2
    count = 2 * SLOTS * (LANES // 2) * SLOTS
    tiles = []
    for row in range(2):
        blocks = [(row * holders + r) * ROWS for r in range(holders)]
        sums = [x_ref[at : at + 2 * SUB, :] for at in blocks]
        stats = [x_ref[at + 2 * SUB : at + ROWS, :] for at in blocks]
        total, both = sums[0], stats[0]
        for r in range(1, holders):
            total, both = total + sums[r], both + stats[r]
        mean = both[:, 0:1] / holders
        spread = both[:, LANES // 2 : LANES // 2 + 1]
        for r in range(holders):
            off = stats[r][:, 0:1] - mean
            spread = spread + count * (off * off)
        scale = 1.0 / jnp.sqrt(spread / (count * holders) + EPSILON)
        tiles.append([(total[k * SUB : (k + 1) * SUB] - HARM * mean) * scale for k in range(2)])
    for row in range(2):
        for k in range(2):
            for g in range(SUB):
                hs_ref[row : row + 1, pl.ds(g * COARSE + k * LANES, LANES)] = tiles[row][k][g : g + 1]
    for k in range(2):
        level_ref[k * SUB : (k + 1) * SUB, :] = (tiles[0][k] + tiles[1][k]) / 2
    peak = jnp.concatenate([jnp.maximum(tiles[0][k], tiles[1][k]) for k in range(2)], axis=0)
    for e in range(m_ref.shape[0]):
        msg_ref[e * ROWS : e * ROWS + 2 * SUB, :] = peak
        msg_ref[e * ROWS + 2 * SUB : (e + 1) * ROWS, :] = m_ref[e : e + 1, :]


def sift_kernel(x_ref, level_ref, bins_ref, o_ref, hs_ref, out_scr, sems):
    steps = sems.shape[0] - 1
    bins_out = pltpu.make_async_copy(bins_ref, hs_ref, sems.at[steps])
    bins_out.start()
    bands, slots = o_ref.shape[:2]
    level = level_ref[...]
    rows = bands * slots
    diff = jnp.concatenate([x_ref[d * ROWS : d * ROWS + 2 * SUB, :] - level for d in range(bands)], axis=0)
    lane = lax.broadcasted_iota(jnp.int32, (rows, LANES), 1)
    line = lax.broadcasted_iota(jnp.int32, (rows, LANES), 0)
    listed = [x_ref[d * ROWS + 2 * SUB : (d + 1) * ROWS, :] for d in range(bands)]
    listed = jnp.concatenate([jnp.broadcast_to(x, (slots, LANES)) for x in listed], axis=0)
    start = jnp.sum(jnp.where(lane == line & (slots - 1), listed, 0.0), axis=1, keepdims=True)
    start = jnp.broadcast_to(start, (rows, LANES)).astype(jnp.int32)
    block = jnp.maximum(start, 0)
    tile_id, offset = block >> 7, block & (LANES - 1)
    band = line & -slots

    def pick(which):
        place = band + ((which & 1) << 3) + (which >> 1)
        return jnp.where(lane == place, 1.0, 0.0).astype(BF16)

    both = jnp.concatenate([pick(tile_id), pick(tile_id + 1)], axis=0)
    parts = jnp.dot(both, jnp.concatenate(halves(diff), axis=1), preferred_element_type=F32)
    parts = parts[:, :LANES] + parts[:, LANES:]
    copies = []
    for step in range(steps):
        part = slice(step * rows // steps, (step + 1) * rows // steps)
        joined = jnp.where(lane[part] >= offset[part], parts[:rows][part], parts[rows:][part])
        moved = jnp.take_along_axis(joined, (lane[part] + offset[part]) & (LANES - 1), axis=1)
        moved = jnp.where(start[part] >= 0, moved, 0.0)
        here = pl.ds(step * bands // steps, bands // steps)
        out_scr[here] = moved.reshape(bands // steps, slots, LANES)
        copies.append(pltpu.make_async_copy(out_scr.at[here], o_ref.at[here], sems.at[step]))
        copies[-1].start()
    for copy in copies:
        copy.wait()
    bins_out.wait()


PARAMS = pltpu.CompilerParams(vmem_limit_bytes=16 * 2**20)


def near(array):
    return pltpu.with_memory_space_constraint(array, pltpu.VMEM)


def shape(*dims):
    return pltpu.VMEM(dims, F32)


def spaces(*kinds):
    return [pl.BlockSpec(memory_space=pltpu.SMEM if kind == "s" else pltpu.VMEM) for kind in kinds]


def run_prepare(me, first, starts, counts):
    within, shift = map(jnp.asarray, first)
    return pl.pallas_call(
        prepare_kernel,
        out_shape=(
            shape(*within.shape),
            pltpu.VMEM((CHUNKS * LANES, COARSE), BF16),
            shape(starts.shape[0], LANES),
        ),
        in_specs=spaces("s", *"vvvv"),
        out_specs=spaces(*"vvv"),
        compiler_params=PARAMS,
    )(me, *[near(x) for x in (within, shift, starts, counts)])


def run_separate(series, shards):
    tiles = series.shape[1] // LANES
    anywhere = pl.BlockSpec(memory_space=pl.ANY)
    rows = pl.pallas_call(
        separate_kernel,
        out_shape=jax.ShapeDtypeStruct((2, tiles, 1, LANES), F32),
        in_specs=[anywhere],
        out_specs=anywhere,
        scratch_shapes=[pltpu.SemaphoreType.DMA((2, SUB))],
    )(jnp.swapaxes(series.reshape(2, tiles, 1, LANES), 0, 1))
    return rows.reshape(shards, 1, -1)


def run_first(received, twiddles):
    shards = received.shape[0]
    received = received.reshape(shards, -1, LANES)
    return pl.pallas_call(
        first_kernel,
        out_shape=shape(received.shape[0] // 2, 2 * received.shape[1], LANES),
        in_specs=spaces(*"vv"),
        out_specs=spaces("v")[0],
        compiler_params=PARAMS,
    )(near(received), near(twiddles))


def run_second(me, received, second, mapping):
    shards = 2 * received.shape[0]
    inputs = [near(x) for x in (received, *map(jnp.asarray, second), mapping)]
    sent = pl.pallas_call(
        second_kernel,
        out_shape=shape(shards * ROWS, LANES),
        in_specs=spaces("s", *"vvvvvvv"),
        out_specs=spaces("v")[0],
        scratch_shapes=[
            pltpu.VMEM((2 * SLOTS * SLOTS, LANES), F32),
            pltpu.VMEM((2 * SLOTS * SUB, LANES), F32),
            pltpu.VMEM((3, SLOTS, 2, SUB, LANES), F32),
            pltpu.VMEM((SLOTS * PIECE, 2 * LANES), BF16),
            pltpu.VMEM((SLOTS * PIECE, 2 * LANES), BF16),
            pltpu.VMEM((16 * LANES // 2, LANES), F32),
            pltpu.VMEM((2 * LANES, CHUNKS * LANES), BF16),
            pltpu.VMEM((2 * LANES, LANES), F32),
        ],
        compiler_params=PARAMS,
    )(me, *inputs)
    return sent.reshape(shards, 1, ROWS * LANES)


def run_third(received, markers):
    bands = markers.shape[0]
    bins, message, level = pl.pallas_call(
        third_kernel,
        out_shape=(shape(2, SUB * COARSE), shape(bands * ROWS, LANES), shape(2 * SUB, LANES)),
        in_specs=spaces(*"vv"),
        out_specs=spaces(*"vvv"),
        compiler_params=PARAMS,
    )(near(markers), near(received.reshape(-1, LANES)))
    return bins, message.reshape(bands, 1, ROWS * LANES), level


def run_sift(received, level, bins):
    bands = received.shape[0]
    steps = bands // 2
    anywhere = pl.BlockSpec(memory_space=pl.ANY)
    return pl.pallas_call(
        sift_kernel,
        out_shape=(
            jax.ShapeDtypeStruct((bands, 2 * SUB, LANES), F32),
            jax.ShapeDtypeStruct(bins.shape, F32),
        ),
        in_specs=spaces(*"vvv"),
        out_specs=[anywhere, anywhere],
        scratch_shapes=[
            pltpu.VMEM((bands, 2 * SUB, LANES), F32),
            pltpu.SemaphoreType.DMA((steps + 1,)),
        ],
        compiler_params=PARAMS,
    )(near(received.reshape(-1, LANES)), near(level), near(bins))


def per_device(series, cand_start, cand_count):
    shards = lax.axis_size("tm")
    first, second = tables(shards, shards * series.shape[1])
    me = lax.axis_index("tm").astype(jnp.int32).reshape(1)
    swap = functools.partial(lax.all_to_all, split_axis=0, concat_axis=0, tiled=True)
    samples = swap(run_separate(series, shards), "tm")
    twiddles, mapping, markers = run_prepare(me, first, cand_start[0, 0], cand_count[0])
    half = shards // 2
    by_row = [list(range(half)), list(range(half, shards))]
    classes = swap(run_first(samples, twiddles), "tm", axis_index_groups=by_row)
    sums = swap(run_second(me, classes, second, mapping), "tm")
    bins, message, level = run_third(sums, markers)
    sifted, harmonic_sum = run_sift(swap(message, "dm"), level, bins)
    return harmonic_sum, sifted[None, None]


def solution(mesh):
    return jax.shard_map(
        per_device,
        mesh=mesh,
        in_specs=(
            P(("beam", "dm"), "tm"),
            P(("beam", "tm"), "dm", None, None),
            P(("beam", "tm"), "dm", None),
        ),
        out_specs=(P(("beam", "dm"), "tm"), P(("beam", "tm"), "dm", None, None, None)),
        check_vma=False,
    )
```

```python
import functools
import math

import jax
import jax.numpy as jnp
import numpy as np
from jax import lax
from jax.experimental import pallas as pl
from jax.experimental.pallas import tpu as pltpu
from jax.sharding import PartitionSpec as P

HARM = 8
BW = 128
EPSILON = 1e-06

LANES = 128
SUB = 8
COARSE = 256
SLOTS = 16
PIECE = 32
PIECES = [(h, c) for h in range(1, HARM + 1) for c in range(h)]
CHUNKS = len(PIECES) // 4
ROWS = 2 * SUB + 1

F32 = jnp.float32
BF16 = jnp.bfloat16


def halves(value):
    top = value.astype(BF16)
    return top, (value - top.astype(F32)).astype(BF16)


def np_halves(value):
    top = value.astype(np.float32).astype(BF16)
    rest = (value - top.astype(np.float64)).astype(np.float32).astype(BF16)
    return top, rest


def unit(turns, period):
    angle = -2.0 * math.pi * (turns % period) / period
    return np.cos(angle), np.sin(angle)


@functools.cache
def tables(shards, samples):
    part = samples // (shards * shards)
    tiles = part // LANES
    m = np.arange(part)
    v = np.arange(LANES)
    s = np.arange(shards)
    half = shards // 2
    r = np.arange(half)
    wide = np.arange(2 * part)
    within = np.stack(unit(r[:, None] * wide[None, :], samples)).reshape(2, half, 2 * tiles, LANES)
    shift = np.stack(unit(r[:, None] * r[None, :], samples // (2 * part)), axis=1)
    shift = np.broadcast_to(shift[..., None], (half, 2, half, LANES))
    after = np.stack(unit(s[:, None] * m[None, :], samples // shards)).reshape(2, shards, tiles, LANES)
    middle = (half + shards * r)[:, None] * m[None, :]
    middle = np.stack(unit(middle, samples)).reshape(2, half, tiles, LANES)
    between = np.stack(unit(s[:, None] * v[None, :], part))
    j = np.arange(LANES // 2)
    rows = []
    for q2 in (j, LANES - 1 - j):
        c2, s2 = unit(q2[:, None] * v[None, :], LANES)
        rows += [np.concatenate([c2, -s2], axis=1), np.concatenate([s2, c2], axis=1)]
    last = np_halves(np.concatenate(rows, axis=0))
    first = [x.astype(np.float32) for x in (within, shift)]
    second = [x.astype(np.float32) for x in (after, middle, between)] + list(last)
    return first, second


def cmul(x, y):
    if x[1] is None:
        return x[0] * y[0], x[0] * y[1]
    return x[0] * y[0] - x[1] * y[1], x[0] * y[1] + x[1] * y[0]


def plus(a, b):
    return b if a is None else a if b is None else a + b


def minus(a, b):
    return a if b is None else -b if a is None else a - b


def cadd(x, y):
    return plus(x[0], y[0]), plus(x[1], y[1])


def csub(x, y):
    return minus(x[0], y[0]), minus(x[1], y[1])


def turn_back(x):
    return x[1], minus(None, x[0])


def four(x0, x1, x2, x3):
    s, d = cadd(x0, x2), csub(x0, x2)
    t, u = cadd(x1, x3), turn_back(csub(x1, x3))
    return cadd(s, t), cadd(d, u), csub(s, t), csub(d, u)


def sixteen(values):
    columns = [four(*values[low::4]) for low in range(4)]
    out = [None] * 16
    for k1 in range(4):
        terms = []
        for low in range(4):
            term = columns[low][k1]
            if low * k1 == 4:
                term = turn_back(term)
            elif low * k1:
                c, s = unit(np.float64(low * k1), 16)
                term = cmul(term, (F32(c), F32(s)))
            terms.append(term)
        for k2, value in enumerate(four(*terms)):
            out[k1 + 4 * k2] = value
    return out


def prepare_kernel(d_ref, x_ref, start_ref, count_ref, o_ref, s_ref, m_ref, x_scr, start_scr, count_scr, sems):
    small = [
        pltpu.make_async_copy(start_ref, start_scr, sems.at[0]),
        pltpu.make_async_copy(count_ref, count_scr, sems.at[1]),
    ]
    pieces = sems.shape[0] - 2
    size = x_ref.shape[0] // pieces
    copies = []
    for piece in range(pieces):
        here = pl.ds(piece * size, size)
        copies.append(pltpu.make_async_copy(x_ref.at[here], x_scr.at[here], sems.at[2 + piece]))
    for copy in copies + small:
        copy.start()

    own_class = d_ref[0] % SUB
    phi = lax.broadcasted_iota(jnp.int32, (SLOTS, COARSE), 1)
    slot = lax.broadcasted_iota(jnp.int32, (SLOTS, COARSE), 0)
    pairs = slot * SLOTS - jnp.where(slot < SUB, 0, SUB * SLOTS - SUB)
    mine = jnp.where(own_class == 0, pairs, own_class + SLOTS * slot)
    mirror = jnp.where(mine == 0, COARSE // 2, COARSE - mine)
    for index, (h, c) in enumerate(PIECES):
        for k, residue in enumerate((mine, mirror)):
            hit = jnp.where(h * phi - COARSE * c == residue, 1.0, 0.0)
            s_ref[pl.ds(index * PIECE + k * SLOTS, SLOTS), :] = hit.astype(BF16)

    tiles = x_ref.shape[0] // 2
    for piece, copy in enumerate(copies):
        copy.wait()
        for at in range(piece * size // 2, (piece + 1) * size // 2, SUB):
            for row in range(2):
                o_ref[row * tiles + at : row * tiles + at + SUB, :] = x_scr[pl.ds(2 * at + row, SUB, stride=2), :]

    for copy in small:
        copy.wait()
    bands, slots = start_ref.shape
    cell = [lax.broadcasted_iota(jnp.int32, (bands, bands), axis) for axis in range(2)]
    counts = jnp.where(cell[0] == cell[1], count_scr[...].astype(F32), 0.0)
    live = jnp.sum(counts, axis=1, keepdims=True).astype(jnp.int32)
    slot = lax.broadcasted_iota(jnp.int32, (bands, slots), 1)
    starts = jnp.where(slot < live, start_scr[...], -1).astype(F32)
    m_ref[...] = jnp.concatenate([starts] * (LANES // slots), axis=1)


def first_kernel(d_ref, x_ref, within_ref, shift_ref, o_ref):
    shards, tiles = x_ref.shape[:2]
    half = shards // 2
    me = d_ref[0] % half
    for k in range(tiles // SUB):
        inner = slice(k * SUB, (k + 1) * SUB)
        classes = sixteen([(x_ref[t, inner, :], None) for t in range(shards)])
        for r in range(half):
            if r:
                own = [shift_ref[me, part, r : r + 1, :] for part in range(2)]
                value = cmul(classes[r], cmul([within_ref[part, r, inner, :] for part in range(2)], own))
            else:
                value = classes[0][0], classes[half][0]
            for part in range(2):
                to = part * tiles + k * SUB
                o_ref[r, to : to + SUB, :] = value[part]


def second_kernel(d_ref, x_ref, after_ref, middle_ref, between_ref, th_ref, tl_ref, s_ref, o_ref, v_scr, x_scr, t_scr, dh_scr, dl_scr, r_scr, l_scr, h_scr):
    shards = 2 * x_ref.shape[0]
    tiles = x_ref.shape[1] // 4
    half = LANES // 2
    own_class = d_ref[0] % x_ref.shape[0]
    is_first = own_class == 0
    sub = lax.broadcasted_iota(jnp.int32, (SUB, LANES), 0)
    lead = jnp.logical_and(sub == 0, is_first)

    for k in range(tiles // SUB):
        rows = slice(k * SUB, (k + 1) * SUB)
        main, middle = [], []
        for s in range(shards):
            at = s % 2 * tiles + k * SUB
            re = x_ref[s // 2, at : at + SUB, :]
            im = x_ref[s // 2, 2 * tiles + at : 2 * tiles + at + SUB, :]
            main.append((re, jnp.where(is_first, 0.0, im)))
            c, sn = unit(np.float64(s), 2 * shards)
            middle.append((im * F32(c), im * F32(sn) if s else None))
        for slot, value in enumerate(sixteen(main)):
            value = cmul(value, (after_ref[0, slot, rows, :], after_ref[1, slot, rows, :]))
            for part in range(2):
                v_scr[pl.ds(part * tiles * shards + k * SUB * shards + slot, SUB, stride=shards), :] = value[part]
        for slot, value in enumerate(sixteen(middle)[: shards // 2]):
            value = cmul(value, (middle_ref[0, slot, rows, :], middle_ref[1, slot, rows, :]))
            for part in range(2):
                at = part * tiles * SUB + k * SUB * SUB + slot
                x_scr[pl.ds(at, SUB, stride=SUB), :] = value[part]

    groups = [[], [], []]
    for u in range(tiles):
        low, high, mid = [], [], []
        for part in range(2):
            at = part * tiles * shards + u * shards
            low.append(v_scr[at : at + SUB, :])
            high.append(v_scr[at + SUB : at + 2 * SUB, :])
            at = part * tiles * SUB + u * SUB
            mid.append(x_scr[at : at + SUB, :])
        groups[0].append(tuple(low))
        groups[1].append(tuple(jnp.where(is_first, mid[part], high[part]) for part in range(2)))
        groups[2].append(tuple(high))
    for group, values in enumerate(groups):
        for rho, value in enumerate(sixteen(values)):
            value = cmul(value, (between_ref[0, rho : rho + 1, :], between_ref[1, rho : rho + 1, :]))
            for part in range(2):
                t_scr[group, rho, part] = value[part]

    for rho in range(tiles):
        for part in range(2):
            back = tiles - 1 - rho
            low = jnp.concatenate([t_scr[0, rho, part], t_scr[1, rho, part]], axis=0)
            turned = jnp.where(lead, t_scr[2, rho, part], t_scr[0, back, part])
            high = jnp.concatenate([turned, t_scr[1, back, part]], axis=0)
            for k, tile in enumerate((low, high)):
                top, rest = halves(tile)
                rows = pl.ds(rho * PIECE + k * SLOTS, SLOTS)
                cols = pl.ds(part * LANES, LANES)
                dh_scr[rows, cols] = top
                dl_scr[rows, cols] = rest
    dims = (((1,), (1,)), ((), ()))
    dot_t = functools.partial(lax.dot_general, dimension_numbers=dims, preferred_element_type=F32)
    lane = lax.broadcasted_iota(jnp.int32, (half, 2 * LANES), 1)
    within = lane % PIECE
    from_low = jnp.logical_or(within < SLOTS, jnp.logical_and(within == SLOTS, is_first))
    scale = 1.0 / (shards * shards * tiles * LANES)
    powers = []
    for part in range(2):
        top = dh_scr[part * 256 : (part + 1) * 256, :]
        rest = dl_scr[part * 256 : (part + 1) * 256, :]
        z = dot_t(th_ref[...], top) + dot_t(th_ref[...], rest) + dot_t(tl_ref[...], top)
        z = z * z
        low = z[0:half] + z[half : 2 * half]
        high = z[2 * half : 3 * half] + z[3 * half :]
        powers.append(jnp.where(from_low, low, high) * scale)

    count = 2 * SLOTS * half * tiles

    def over_all(value):
        column = jnp.sum(value, axis=0, keepdims=True)
        return jnp.sum(column, axis=1, keepdims=True)

    mean = over_all(powers[0] + powers[1]) / count
    off0, off1 = powers[0] - mean, powers[1] - mean
    deviation = over_all(off0 * off0 + off1 * off1)
    stats = jnp.where(sub[0:1] + lax.broadcasted_iota(jnp.int32, (1, LANES), 1) < half, mean, deviation)
    for t in range(shards):
        o_ref[t * ROWS + 2 * SUB : (t + 1) * ROWS, :] = stats

    for group in range(4):
        value = powers[group // 2][:, (group % 2) * LANES : (group % 2 + 1) * LANES]
        for shift in range(4):
            at = (group * 4 + shift) * half
            r_scr[at : at + half, :] = pltpu.roll(value, shift * PIECE, 1) if shift else value
    lane8 = lax.broadcasted_iota(jnp.int32, (SUB, LANES), 1) // PIECE
    for chunk in range(CHUNKS):
        for g_pair in range(tiles // 2):
            parts = []
            for g0 in (2 * g_pair, 2 * g_pair + 1):
                tile = None
                for place in range(4):
                    h, c = PIECES[chunk * 4 + place]
                    rho, e = (h * g0 + c) % tiles, (h * g0 + c) // tiles
                    shift = (place - rho % 4) % 4
                    rows = pl.ds((rho // 4 * 4 + shift) * half + e, SUB, stride=h)
                    got = r_scr[rows, :]
                    tile = got if tile is None else jnp.where(lane8 == place, got, tile)
                parts.append(tile)
            top, rest = halves(jnp.concatenate(parts, axis=0))
            cols = pl.ds(chunk * LANES, LANES)
            l_scr[pl.ds(g_pair * 16, 16), cols] = top
            l_scr[pl.ds(LANES + g_pair * 16, 16), cols] = rest
    both = jnp.dot(l_scr[...], s_ref[...], preferred_element_type=F32)
    for tile in range(2):
        cols = slice(tile * LANES, (tile + 1) * LANES)
        h_scr[tile * LANES : (tile + 1) * LANES, :] = both[:LANES, cols] + both[LANES:, cols]
    for t in range(shards):
        for tile in range(2):
            rows = pl.ds(tile * LANES + (t % 2) * half + t // 2, SUB, stride=SUB)
            o_ref[t * ROWS + tile * SUB : t * ROWS + (tile + 1) * SUB, :] = h_scr[rows, :]


def third_kernel(m_ref, x_ref, hs_ref, msg_ref, level_ref):
    shards = x_ref.shape[0] // ROWS
    holders = shards // 2
    count = 2 * SLOTS * (LANES // 2) * SLOTS
    tiles = []
    for row in range(2):
        blocks = [(row * holders + r) * ROWS for r in range(holders)]
        sums = [x_ref[at : at + 2 * SUB, :] for at in blocks]
        stats = [x_ref[at + 2 * SUB : at + ROWS, :] for at in blocks]
        total, both = sums[0], stats[0]
        for r in range(1, holders):
            total, both = total + sums[r], both + stats[r]
        mean = both[:, 0:1] / holders
        spread = both[:, LANES // 2 : LANES // 2 + 1]
        for r in range(holders):
            off = stats[r][:, 0:1] - mean
            spread = spread + count * (off * off)
        scale = 1.0 / jnp.sqrt(spread / (count * holders) + EPSILON)
        tiles.append([(total[k * SUB : (k + 1) * SUB] - HARM * mean) * scale for k in range(2)])
    for row in range(2):
        for k in range(2):
            for g in range(SUB):
                hs_ref[row : row + 1, pl.ds(g * COARSE + k * LANES, LANES)] = tiles[row][k][g : g + 1]
    for k in range(2):
        level_ref[k * SUB : (k + 1) * SUB, :] = (tiles[0][k] + tiles[1][k]) / 2
    peak = jnp.concatenate([jnp.maximum(tiles[0][k], tiles[1][k]) for k in range(2)], axis=0)
    for e in range(m_ref.shape[0]):
        msg_ref[e * ROWS : e * ROWS + 2 * SUB, :] = peak
        msg_ref[e * ROWS + 2 * SUB : (e + 1) * ROWS, :] = m_ref[e : e + 1, :]


def sift_kernel(x_ref, level_ref, bins_ref, o_ref, hs_ref, out_scr, sems):
    steps = sems.shape[0] - 1
    bins_out = pltpu.make_async_copy(bins_ref, hs_ref, sems.at[steps])
    bins_out.start()
    bands, slots = o_ref.shape[:2]
    level = level_ref[...]
    rows = bands * slots
    diff = jnp.concatenate([x_ref[d * ROWS : d * ROWS + 2 * SUB, :] - level for d in range(bands)], axis=0)
    lane = lax.broadcasted_iota(jnp.int32, (rows, LANES), 1)
    line = lax.broadcasted_iota(jnp.int32, (rows, LANES), 0)
    listed = [x_ref[d * ROWS + 2 * SUB : (d + 1) * ROWS, :] for d in range(bands)]
    listed = jnp.concatenate([jnp.broadcast_to(x, (slots, LANES)) for x in listed], axis=0)
    start = jnp.sum(jnp.where(lane == line & (slots - 1), listed, 0.0), axis=1, keepdims=True)
    start = jnp.broadcast_to(start, (rows, LANES)).astype(jnp.int32)
    block = jnp.maximum(start, 0)
    tile_id, offset = block >> 7, block & (LANES - 1)
    band = line & -slots

    def pick(which):
        place = band + ((which & 1) << 3) + (which >> 1)
        return jnp.where(lane == place, 1.0, 0.0).astype(BF16)

    both = jnp.concatenate([pick(tile_id), pick(tile_id + 1)], axis=0)
    parts = jnp.dot(both, jnp.concatenate(halves(diff), axis=1), preferred_element_type=F32)
    parts = parts[:, :LANES] + parts[:, LANES:]
    copies = []
    for step in range(steps):
        part = slice(step * rows // steps, (step + 1) * rows // steps)
        joined = jnp.where(lane[part] >= offset[part], parts[:rows][part], parts[rows:][part])
        moved = jnp.take_along_axis(joined, (lane[part] + offset[part]) & (LANES - 1), axis=1)
        moved = jnp.where(start[part] >= 0, moved, 0.0)
        here = pl.ds(step * bands // steps, bands // steps)
        out_scr[here] = moved.reshape(bands // steps, slots, LANES)
        copies.append(pltpu.make_async_copy(out_scr.at[here], o_ref.at[here], sems.at[step]))
        copies[-1].start()
    for copy in copies:
        copy.wait()
    bins_out.wait()


PARAMS = pltpu.CompilerParams(vmem_limit_bytes=16 * 2**20)


def near(array):
    return pltpu.with_memory_space_constraint(array, pltpu.VMEM)


def shape(*dims):
    return pltpu.VMEM(dims, F32)


def spaces(*kinds):
    return [pl.BlockSpec(memory_space=pltpu.SMEM if kind == "s" else pltpu.VMEM) for kind in kinds]


def run_prepare(me, series, starts, counts, shards):
    tiles = series.shape[1] // LANES
    lines = jnp.swapaxes(series.reshape(2, tiles, LANES), 0, 1).reshape(2 * tiles, LANES)
    rows, mapping, markers = pl.pallas_call(
        prepare_kernel,
        out_shape=(
            shape(2 * tiles, LANES),
            pltpu.VMEM((CHUNKS * LANES, COARSE), BF16),
            shape(starts.shape[0], LANES),
        ),
        in_specs=spaces("s") + [pl.BlockSpec(memory_space=pl.ANY)] * 3,
        out_specs=spaces(*"vvv"),
        scratch_shapes=[
            pltpu.VMEM((2 * tiles, LANES), F32),
            pltpu.VMEM(starts.shape, jnp.int32),
            pltpu.VMEM(counts.shape, jnp.int32),
            pltpu.SemaphoreType.DMA((6,)),
        ],
        compiler_params=PARAMS,
    )(me, *[pltpu.with_memory_space_constraint(x, pltpu.HBM) for x in (lines, starts, counts)])
    return rows.reshape(shards, -1, LANES), mapping, markers


def run_first(me, received, first):
    shards = received.shape[0]
    within, shift = map(jnp.asarray, first)
    return pl.pallas_call(
        first_kernel,
        out_shape=shape(shards // 2, 2 * received.shape[1], LANES),
        in_specs=spaces(*"svvv"),
        out_specs=spaces("v")[0],
        compiler_params=PARAMS,
    )(me, *[near(x) for x in (received, within, shift)])


def run_second(me, received, second, mapping):
    shards = 2 * received.shape[0]
    inputs = [near(x) for x in (received, *map(jnp.asarray, second), mapping)]
    sent = pl.pallas_call(
        second_kernel,
        out_shape=shape(shards * ROWS, LANES),
        in_specs=spaces("s", *"vvvvvvv"),
        out_specs=spaces("v")[0],
        scratch_shapes=[
            pltpu.VMEM((2 * SLOTS * SLOTS, LANES), F32),
            pltpu.VMEM((2 * SLOTS * SUB, LANES), F32),
            pltpu.VMEM((3, SLOTS, 2, SUB, LANES), F32),
            pltpu.VMEM((SLOTS * PIECE, 2 * LANES), BF16),
            pltpu.VMEM((SLOTS * PIECE, 2 * LANES), BF16),
            pltpu.VMEM((16 * LANES // 2, LANES), F32),
            pltpu.VMEM((2 * LANES, CHUNKS * LANES), BF16),
            pltpu.VMEM((2 * LANES, LANES), F32),
        ],
        compiler_params=PARAMS,
    )(me, *inputs)
    return sent.reshape(shards, 1, ROWS * LANES)


def run_third(received, markers):
    bands = markers.shape[0]
    bins, message, level = pl.pallas_call(
        third_kernel,
        out_shape=(shape(2, SUB * COARSE), shape(bands * ROWS, LANES), shape(2 * SUB, LANES)),
        in_specs=spaces(*"vv"),
        out_specs=spaces(*"vvv"),
        compiler_params=PARAMS,
    )(near(markers), near(received.reshape(-1, LANES)))
    return bins, message.reshape(bands, 1, ROWS * LANES), level


def run_sift(received, level, bins):
    bands = received.shape[0]
    steps = bands // 2
    anywhere = pl.BlockSpec(memory_space=pl.ANY)
    return pl.pallas_call(
        sift_kernel,
        out_shape=(
            jax.ShapeDtypeStruct((bands, 2 * SUB, LANES), F32),
            jax.ShapeDtypeStruct(bins.shape, F32),
        ),
        in_specs=spaces(*"vvv"),
        out_specs=[anywhere, anywhere],
        scratch_shapes=[
            pltpu.VMEM((bands, 2 * SUB, LANES), F32),
            pltpu.SemaphoreType.DMA((steps + 1,)),
        ],
        compiler_params=PARAMS,
    )(near(received.reshape(-1, LANES)), near(level), near(bins))


def per_device(series, cand_start, cand_count):
    shards = lax.axis_size("tm")
    first, second = tables(shards, shards * series.shape[1])
    me = lax.axis_index("tm").astype(jnp.int32).reshape(1)
    swap = functools.partial(lax.all_to_all, split_axis=0, concat_axis=0, tiled=True)
    rows, mapping, markers = run_prepare(me, series, cand_start[0, 0], cand_count[0], shards)
    half = shards // 2
    by_row = [list(range(half)), list(range(half, shards))]
    classes = swap(run_first(me, swap(rows, "tm"), first), "tm", axis_index_groups=by_row)
    sums = swap(run_second(me, classes, second, mapping), "tm")
    bins, message, level = run_third(sums, markers)
    sifted, harmonic_sum = run_sift(swap(message, "dm"), level, bins)
    return harmonic_sum, sifted[None, None]


def solution(mesh):
    return jax.shard_map(
        per_device,
        mesh=mesh,
        in_specs=(
            P(("beam", "dm"), "tm"),
            P(("beam", "tm"), "dm", None, None),
            P(("beam", "tm"), "dm", None),
        ),
        out_specs=(P(("beam", "dm"), "tm"), P(("beam", "tm"), "dm", None, None, None)),
        check_vma=False,
    )
```

```python
import functools
import math

import jax
import jax.numpy as jnp
import numpy as np
from jax import lax
from jax.experimental import pallas as pl
from jax.experimental.pallas import tpu as pltpu
from jax.sharding import PartitionSpec as P

HARM = 8
BW = 128
EPSILON = 1e-06

LANES = 128
SUB = 8
COARSE = 256
SLOTS = 16
PIECE = 32
PIECES = [(h, c) for h in range(1, HARM + 1) for c in range(h)]
CHUNKS = len(PIECES) // 4
ROWS = 2 * SUB + 1

F32 = jnp.float32
BF16 = jnp.bfloat16


def halves(value):
    top = value.astype(BF16)
    return top, (value - top.astype(F32)).astype(BF16)


def np_halves(value):
    top = value.astype(np.float32).astype(BF16)
    rest = (value - top.astype(np.float64)).astype(np.float32).astype(BF16)
    return top, rest


def unit(turns, period):
    angle = -2.0 * math.pi * (turns % period) / period
    return np.cos(angle), np.sin(angle)


@functools.cache
def tables(shards, samples):
    part = samples // (shards * shards)
    tiles = part // LANES
    m = np.arange(part)
    v = np.arange(LANES)
    s = np.arange(shards)
    half = shards // 2
    r = np.arange(half)
    wide = np.arange(2 * part)
    within = np.stack(unit(r[:, None] * wide[None, :], samples)).reshape(2, half, 2 * tiles, LANES)
    shift = np.stack(unit(r[:, None] * r[None, :], samples // (2 * part)), axis=1)
    shift = np.broadcast_to(shift[..., None], (half, 2, half, LANES))
    after = np.stack(unit(s[:, None] * m[None, :], samples // shards)).reshape(2, shards, tiles, LANES)
    middle = (half + shards * r)[:, None] * m[None, :]
    middle = np.stack(unit(middle, samples)).reshape(2, half, tiles, LANES)
    between = np.stack(unit(s[:, None] * v[None, :], part))
    j = np.arange(LANES // 2)
    rows = []
    for q2 in (j, LANES - 1 - j):
        c2, s2 = unit(q2[:, None] * v[None, :], LANES)
        rows += [np.concatenate([c2, -s2], axis=1), np.concatenate([s2, c2], axis=1)]
    last = np_halves(np.concatenate(rows, axis=0))
    first = [x.astype(np.float32) for x in (within, shift)]
    second = [x.astype(np.float32) for x in (after, middle, between)] + list(last)
    return first, second


def cmul(x, y):
    if x[1] is None:
        return x[0] * y[0], x[0] * y[1]
    return x[0] * y[0] - x[1] * y[1], x[0] * y[1] + x[1] * y[0]


def plus(a, b):
    return b if a is None else a if b is None else a + b


def minus(a, b):
    return a if b is None else -b if a is None else a - b


def cadd(x, y):
    return plus(x[0], y[0]), plus(x[1], y[1])


def csub(x, y):
    return minus(x[0], y[0]), minus(x[1], y[1])


def turn_back(x):
    return x[1], minus(None, x[0])


def four(x0, x1, x2, x3):
    s, d = cadd(x0, x2), csub(x0, x2)
    t, u = cadd(x1, x3), turn_back(csub(x1, x3))
    return cadd(s, t), cadd(d, u), csub(s, t), csub(d, u)


def sixteen(values):
    columns = [four(*values[low::4]) for low in range(4)]
    out = [None] * 16
    for k1 in range(4):
        terms = []
        for low in range(4):
            term = columns[low][k1]
            if low * k1 == 4:
                term = turn_back(term)
            elif low * k1:
                c, s = unit(np.float64(low * k1), 16)
                term = cmul(term, (F32(c), F32(s)))
            terms.append(term)
        for k2, value in enumerate(four(*terms)):
            out[k1 + 4 * k2] = value
    return out


def prepare_kernel(d_ref, x_ref, start_ref, count_ref, o_ref, s_ref, m_ref, x_scr, start_scr, count_scr, sems):
    small = [
        pltpu.make_async_copy(start_ref, start_scr, sems.at[0]),
        pltpu.make_async_copy(count_ref, count_scr, sems.at[1]),
    ]
    pieces = sems.shape[0] - 2
    size = x_ref.shape[0] // pieces
    copies = []
    for piece in range(pieces):
        here = pl.ds(piece * size, size)
        copies.append(pltpu.make_async_copy(x_ref.at[here], x_scr.at[here], sems.at[2 + piece]))
    for copy in small + copies:
        copy.start()

    own_class = d_ref[0] % SUB
    phi = lax.broadcasted_iota(jnp.int32, (SLOTS, COARSE), 1)
    slot = lax.broadcasted_iota(jnp.int32, (SLOTS, COARSE), 0)
    pairs = slot * SLOTS - jnp.where(slot < SUB, 0, SUB * SLOTS - SUB)
    mine = jnp.where(own_class == 0, pairs, own_class + SLOTS * slot)
    mirror = jnp.where(mine == 0, COARSE // 2, COARSE - mine)
    for index, (h, c) in enumerate(PIECES):
        for k, residue in enumerate((mine, mirror)):
            hit = jnp.where(h * phi - COARSE * c == residue, 1.0, 0.0)
            s_ref[pl.ds(index * PIECE + k * SLOTS, SLOTS), :] = hit.astype(BF16)

    for copy in small:
        copy.wait()
    bands, slots = start_ref.shape
    cell = [lax.broadcasted_iota(jnp.int32, (bands, bands), axis) for axis in range(2)]
    counts = jnp.where(cell[0] == cell[1], count_scr[...].astype(F32), 0.0)
    live = jnp.sum(counts, axis=1, keepdims=True).astype(jnp.int32)
    slot = lax.broadcasted_iota(jnp.int32, (bands, slots), 1)
    starts = jnp.where(slot < live, start_scr[...], -1).astype(F32)
    m_ref[...] = jnp.concatenate([starts] * (LANES // slots), axis=1)

    tiles = x_ref.shape[0] // 2
    for piece, copy in enumerate(copies):
        copy.wait()
        for at in range(piece * size // 2, (piece + 1) * size // 2, SUB):
            for row in range(2):
                o_ref[row * tiles + at : row * tiles + at + SUB, :] = x_scr[pl.ds(2 * at + row, SUB, stride=2), :]


def first_kernel(d_ref, x_ref, within_ref, shift_ref, o_ref):
    shards, tiles = x_ref.shape[:2]
    half = shards // 2
    me = d_ref[0] % half
    for k in range(tiles // SUB):
        inner = slice(k * SUB, (k + 1) * SUB)
        classes = sixteen([(x_ref[t, inner, :], None) for t in range(shards)])
        for r in range(half):
            if r:
                own = [shift_ref[me, part, r : r + 1, :] for part in range(2)]
                value = cmul(classes[r], cmul([within_ref[part, r, inner, :] for part in range(2)], own))
            else:
                value = classes[0][0], classes[half][0]
            for part in range(2):
                to = part * tiles + k * SUB
                o_ref[r, to : to + SUB, :] = value[part]


def second_kernel(d_ref, x_ref, after_ref, middle_ref, between_ref, th_ref, tl_ref, s_ref, o_ref, v_scr, x_scr, t_scr, dh_scr, dl_scr, r_scr, l_scr, h_scr):
    shards = 2 * x_ref.shape[0]
    tiles = x_ref.shape[1] // 4
    half = LANES // 2
    own_class = d_ref[0] % x_ref.shape[0]
    is_first = own_class == 0
    sub = lax.broadcasted_iota(jnp.int32, (SUB, LANES), 0)
    lead = jnp.logical_and(sub == 0, is_first)

    for k in range(tiles // SUB):
        rows = slice(k * SUB, (k + 1) * SUB)
        main, middle = [], []
        for s in range(shards):
            at = s % 2 * tiles + k * SUB
            re = x_ref[s // 2, at : at + SUB, :]
            im = x_ref[s // 2, 2 * tiles + at : 2 * tiles + at + SUB, :]
            main.append((re, jnp.where(is_first, 0.0, im)))
            c, sn = unit(np.float64(s), 2 * shards)
            middle.append((im * F32(c), im * F32(sn) if s else None))
        for slot, value in enumerate(sixteen(main)):
            value = cmul(value, (after_ref[0, slot, rows, :], after_ref[1, slot, rows, :]))
            for part in range(2):
                v_scr[pl.ds(part * tiles * shards + k * SUB * shards + slot, SUB, stride=shards), :] = value[part]
        for slot, value in enumerate(sixteen(middle)[: shards // 2]):
            value = cmul(value, (middle_ref[0, slot, rows, :], middle_ref[1, slot, rows, :]))
            for part in range(2):
                at = part * tiles * SUB + k * SUB * SUB + slot
                x_scr[pl.ds(at, SUB, stride=SUB), :] = value[part]

    groups = [[], [], []]
    for u in range(tiles):
        low, high, mid = [], [], []
        for part in range(2):
            at = part * tiles * shards + u * shards
            low.append(v_scr[at : at + SUB, :])
            high.append(v_scr[at + SUB : at + 2 * SUB, :])
            at = part * tiles * SUB + u * SUB
            mid.append(x_scr[at : at + SUB, :])
        groups[0].append(tuple(low))
        groups[1].append(tuple(jnp.where(is_first, mid[part], high[part]) for part in range(2)))
        groups[2].append(tuple(high))
    for group, values in enumerate(groups):
        for rho, value in enumerate(sixteen(values)):
            value = cmul(value, (between_ref[0, rho : rho + 1, :], between_ref[1, rho : rho + 1, :]))
            for part in range(2):
                t_scr[group, rho, part] = value[part]

    for rho in range(tiles):
        for part in range(2):
            back = tiles - 1 - rho
            low = jnp.concatenate([t_scr[0, rho, part], t_scr[1, rho, part]], axis=0)
            turned = jnp.where(lead, t_scr[2, rho, part], t_scr[0, back, part])
            high = jnp.concatenate([turned, t_scr[1, back, part]], axis=0)
            for k, tile in enumerate((low, high)):
                top, rest = halves(tile)
                rows = pl.ds(rho * PIECE + k * SLOTS, SLOTS)
                cols = pl.ds(part * LANES, LANES)
                dh_scr[rows, cols] = top
                dl_scr[rows, cols] = rest
    dims = (((1,), (1,)), ((), ()))
    dot_t = functools.partial(lax.dot_general, dimension_numbers=dims, preferred_element_type=F32)
    lane = lax.broadcasted_iota(jnp.int32, (half, 2 * LANES), 1)
    within = lane % PIECE
    from_low = jnp.logical_or(within < SLOTS, jnp.logical_and(within == SLOTS, is_first))
    scale = 1.0 / (shards * shards * tiles * LANES)
    powers = []
    for part in range(2):
        top = dh_scr[part * 256 : (part + 1) * 256, :]
        rest = dl_scr[part * 256 : (part + 1) * 256, :]
        z = dot_t(th_ref[...], top) + dot_t(th_ref[...], rest) + dot_t(tl_ref[...], top)
        z = z * z
        low = z[0:half] + z[half : 2 * half]
        high = z[2 * half : 3 * half] + z[3 * half :]
        powers.append(jnp.where(from_low, low, high) * scale)

    count = 2 * SLOTS * half * tiles

    def over_all(value):
        column = jnp.sum(value, axis=0, keepdims=True)
        return jnp.sum(column, axis=1, keepdims=True)

    mean = over_all(powers[0] + powers[1]) / count
    off0, off1 = powers[0] - mean, powers[1] - mean
    deviation = over_all(off0 * off0 + off1 * off1)
    stats = jnp.where(sub[0:1] + lax.broadcasted_iota(jnp.int32, (1, LANES), 1) < half, mean, deviation)
    for t in range(shards):
        o_ref[t * ROWS + 2 * SUB : (t + 1) * ROWS, :] = stats

    for group in range(4):
        value = powers[group // 2][:, (group % 2) * LANES : (group % 2 + 1) * LANES]
        for shift in range(4):
            at = (group * 4 + shift) * half
            r_scr[at : at + half, :] = pltpu.roll(value, shift * PIECE, 1) if shift else value
    lane8 = lax.broadcasted_iota(jnp.int32, (SUB, LANES), 1) // PIECE
    for chunk in range(CHUNKS):
        for g_pair in range(tiles // 2):
            parts = []
            for g0 in (2 * g_pair, 2 * g_pair + 1):
                tile = None
                for place in range(4):
                    h, c = PIECES[chunk * 4 + place]
                    rho, e = (h * g0 + c) % tiles, (h * g0 + c) // tiles
                    shift = (place - rho % 4) % 4
                    rows = pl.ds((rho // 4 * 4 + shift) * half + e, SUB, stride=h)
                    got = r_scr[rows, :]
                    tile = got if tile is None else jnp.where(lane8 == place, got, tile)
                parts.append(tile)
            top, rest = halves(jnp.concatenate(parts, axis=0))
            cols = pl.ds(chunk * LANES, LANES)
            l_scr[pl.ds(g_pair * 16, 16), cols] = top
            l_scr[pl.ds(LANES + g_pair * 16, 16), cols] = rest
    both = jnp.dot(l_scr[...], s_ref[...], preferred_element_type=F32)
    for tile in range(2):
        cols = slice(tile * LANES, (tile + 1) * LANES)
        h_scr[tile * LANES : (tile + 1) * LANES, :] = both[:LANES, cols] + both[LANES:, cols]
    for t in range(shards):
        for tile in range(2):
            rows = pl.ds(tile * LANES + (t % 2) * half + t // 2, SUB, stride=SUB)
            o_ref[t * ROWS + tile * SUB : t * ROWS + (tile + 1) * SUB, :] = h_scr[rows, :]


def third_kernel(m_ref, x_ref, hs_ref, msg_ref, level_ref):
    shards = x_ref.shape[0] // ROWS
    holders = shards // 2
    count = 2 * SLOTS * (LANES // 2) * SLOTS
    tiles = []
    for row in range(2):
        blocks = [(row * holders + r) * ROWS for r in range(holders)]
        sums = [x_ref[at : at + 2 * SUB, :] for at in blocks]
        stats = [x_ref[at + 2 * SUB : at + ROWS, :] for at in blocks]
        total, both = sums[0], stats[0]
        for r in range(1, holders):
            total, both = total + sums[r], both + stats[r]
        mean = both[:, 0:1] / holders
        spread = both[:, LANES // 2 : LANES // 2 + 1]
        for r in range(holders):
            off = stats[r][:, 0:1] - mean
            spread = spread + count * (off * off)
        scale = 1.0 / jnp.sqrt(spread / (count * holders) + EPSILON)
        tiles.append([(total[k * SUB : (k + 1) * SUB] - HARM * mean) * scale for k in range(2)])
    for row in range(2):
        for k in range(2):
            for g in range(SUB):
                hs_ref[row : row + 1, pl.ds(g * COARSE + k * LANES, LANES)] = tiles[row][k][g : g + 1]
    for k in range(2):
        level_ref[k * SUB : (k + 1) * SUB, :] = (tiles[0][k] + tiles[1][k]) / 2
    peak = jnp.concatenate([jnp.maximum(tiles[0][k], tiles[1][k]) for k in range(2)], axis=0)
    for e in range(m_ref.shape[0]):
        msg_ref[e * ROWS : e * ROWS + 2 * SUB, :] = peak
        msg_ref[e * ROWS + 2 * SUB : (e + 1) * ROWS, :] = m_ref[e : e + 1, :]


def sift_kernel(x_ref, level_ref, bins_ref, o_ref, hs_ref, out_scr, sems):
    steps = sems.shape[0] - 1
    bins_out = pltpu.make_async_copy(bins_ref, hs_ref, sems.at[steps])
    bins_out.start()
    bands, slots = o_ref.shape[:2]
    level = level_ref[...]
    rows = bands * slots
    diff = jnp.concatenate([x_ref[d * ROWS : d * ROWS + 2 * SUB, :] - level for d in range(bands)], axis=0)
    lane = lax.broadcasted_iota(jnp.int32, (rows, LANES), 1)
    line = lax.broadcasted_iota(jnp.int32, (rows, LANES), 0)
    listed = [x_ref[d * ROWS + 2 * SUB : (d + 1) * ROWS, :] for d in range(bands)]
    listed = jnp.concatenate([jnp.broadcast_to(x, (slots, LANES)) for x in listed], axis=0)
    start = jnp.sum(jnp.where(lane == line & (slots - 1), listed, 0.0), axis=1, keepdims=True)
    start = jnp.broadcast_to(start, (rows, LANES)).astype(jnp.int32)
    block = jnp.maximum(start, 0)
    tile_id, offset = block >> 7, block & (LANES - 1)
    band = line & -slots

    def pick(which):
        place = band + ((which & 1) << 3) + (which >> 1)
        return jnp.where(lane == place, 1.0, 0.0).astype(BF16)

    both = jnp.concatenate([pick(tile_id), pick(tile_id + 1)], axis=0)
    parts = jnp.dot(both, jnp.concatenate(halves(diff), axis=1), preferred_element_type=F32)
    parts = parts[:, :LANES] + parts[:, LANES:]
    copies = []
    for step in range(steps):
        part = slice(step * rows // steps, (step + 1) * rows // steps)
        joined = jnp.where(lane[part] >= offset[part], parts[:rows][part], parts[rows:][part])
        moved = jnp.take_along_axis(joined, (lane[part] + offset[part]) & (LANES - 1), axis=1)
        moved = jnp.where(start[part] >= 0, moved, 0.0)
        here = pl.ds(step * bands // steps, bands // steps)
        out_scr[here] = moved.reshape(bands // steps, slots, LANES)
        copies.append(pltpu.make_async_copy(out_scr.at[here], o_ref.at[here], sems.at[step]))
        copies[-1].start()
    for copy in copies:
        copy.wait()
    bins_out.wait()


PARAMS = pltpu.CompilerParams(vmem_limit_bytes=16 * 2**20)


def near(array):
    return pltpu.with_memory_space_constraint(array, pltpu.VMEM)


def shape(*dims):
    return pltpu.VMEM(dims, F32)


def spaces(*kinds):
    return [pl.BlockSpec(memory_space=pltpu.SMEM if kind == "s" else pltpu.VMEM) for kind in kinds]


def run_prepare(me, series, starts, counts, shards):
    tiles = series.shape[1] // LANES
    lines = jnp.swapaxes(series.reshape(2, tiles, LANES), 0, 1).reshape(2 * tiles, LANES)
    rows, mapping, markers = pl.pallas_call(
        prepare_kernel,
        out_shape=(
            shape(2 * tiles, LANES),
            pltpu.VMEM((CHUNKS * LANES, COARSE), BF16),
            shape(starts.shape[0], LANES),
        ),
        in_specs=spaces("s") + [pl.BlockSpec(memory_space=pl.ANY)] * 3,
        out_specs=spaces(*"vvv"),
        scratch_shapes=[
            pltpu.VMEM((2 * tiles, LANES), F32),
            pltpu.VMEM(starts.shape, jnp.int32),
            pltpu.VMEM(counts.shape, jnp.int32),
            pltpu.SemaphoreType.DMA((6,)),
        ],
        compiler_params=PARAMS,
    )(me, *[pltpu.with_memory_space_constraint(x, pltpu.HBM) for x in (lines, starts, counts)])
    return rows.reshape(shards, -1, LANES), mapping, markers


def run_first(me, received, first):
    shards = received.shape[0]
    within, shift = map(jnp.asarray, first)
    return pl.pallas_call(
        first_kernel,
        out_shape=shape(shards // 2, 2 * received.shape[1], LANES),
        in_specs=spaces(*"svvv"),
        out_specs=spaces("v")[0],
        compiler_params=PARAMS,
    )(me, *[near(x) for x in (received, within, shift)])


def run_second(me, received, second, mapping):
    shards = 2 * received.shape[0]
    inputs = [near(x) for x in (received, *map(jnp.asarray, second), mapping)]
    sent = pl.pallas_call(
        second_kernel,
        out_shape=shape(shards * ROWS, LANES),
        in_specs=spaces("s", *"vvvvvvv"),
        out_specs=spaces("v")[0],
        scratch_shapes=[
            pltpu.VMEM((2 * SLOTS * SLOTS, LANES), F32),
            pltpu.VMEM((2 * SLOTS * SUB, LANES), F32),
            pltpu.VMEM((3, SLOTS, 2, SUB, LANES), F32),
            pltpu.VMEM((SLOTS * PIECE, 2 * LANES), BF16),
            pltpu.VMEM((SLOTS * PIECE, 2 * LANES), BF16),
            pltpu.VMEM((16 * LANES // 2, LANES), F32),
            pltpu.VMEM((2 * LANES, CHUNKS * LANES), BF16),
            pltpu.VMEM((2 * LANES, LANES), F32),
        ],
        compiler_params=PARAMS,
    )(me, *inputs)
    return sent.reshape(shards, 1, ROWS * LANES)


def run_third(received, markers):
    bands = markers.shape[0]
    bins, message, level = pl.pallas_call(
        third_kernel,
        out_shape=(shape(2, SUB * COARSE), shape(bands * ROWS, LANES), shape(2 * SUB, LANES)),
        in_specs=spaces(*"vv"),
        out_specs=spaces(*"vvv"),
        compiler_params=PARAMS,
    )(near(markers), near(received.reshape(-1, LANES)))
    return bins, message.reshape(bands, 1, ROWS * LANES), level


def run_sift(received, level, bins):
    bands = received.shape[0]
    steps = 1
    anywhere = pl.BlockSpec(memory_space=pl.ANY)
    return pl.pallas_call(
        sift_kernel,
        out_shape=(
            jax.ShapeDtypeStruct((bands, 2 * SUB, LANES), F32),
            jax.ShapeDtypeStruct(bins.shape, F32),
        ),
        in_specs=spaces(*"vvv"),
        out_specs=[anywhere, anywhere],
        scratch_shapes=[
            pltpu.VMEM((bands, 2 * SUB, LANES), F32),
            pltpu.SemaphoreType.DMA((steps + 1,)),
        ],
        compiler_params=PARAMS,
    )(near(received.reshape(-1, LANES)), near(level), near(bins))


def per_device(series, cand_start, cand_count):
    shards = lax.axis_size("tm")
    first, second = tables(shards, shards * series.shape[1])
    me = lax.axis_index("tm").astype(jnp.int32).reshape(1)
    swap = functools.partial(lax.all_to_all, split_axis=0, concat_axis=0, tiled=True)
    rows, mapping, markers = run_prepare(me, series, cand_start[0, 0], cand_count[0], shards)
    half = shards // 2
    by_row = [list(range(half)), list(range(half, shards))]
    classes = swap(run_first(me, swap(rows, "tm"), first), "tm", axis_index_groups=by_row)
    sums = swap(run_second(me, classes, second, mapping), "tm")
    bins, message, level = run_third(sums, markers)
    sifted, harmonic_sum = run_sift(swap(message, "dm"), level, bins)
    return harmonic_sum, sifted[None, None]


def solution(mesh):
    return jax.shard_map(
        per_device,
        mesh=mesh,
        in_specs=(
            P(("beam", "dm"), "tm"),
            P(("beam", "tm"), "dm", None, None),
            P(("beam", "tm"), "dm", None),
        ),
        out_specs=(P(("beam", "dm"), "tm"), P(("beam", "tm"), "dm", None, None, None)),
        check_vma=False,
    )
```

```python
import functools
import math

import jax
import jax.numpy as jnp
import numpy as np
from jax import lax
from jax.experimental import pallas as pl
from jax.experimental.pallas import tpu as pltpu
from jax.sharding import PartitionSpec as P

HARM = 8
BW = 128
EPSILON = 1e-06

LANES = 128
SUB = 8
COARSE = 256
SLOTS = 16
PIECE = 32
ODD = {h: h // (h & -h) for h in range(1, HARM + 1)}
PIECES = [(h, range(c, c + ODD[h])) for h in range(1, HARM + 1) for c in range(0, h, ODD[h])]
CHUNKS = len(PIECES) // 4
ROWS = 2 * SUB + 1

F32 = jnp.float32
BF16 = jnp.bfloat16


def halves(value):
    top = value.astype(BF16)
    return top, (value - top.astype(F32)).astype(BF16)


def np_halves(value):
    top = value.astype(np.float32).astype(BF16)
    rest = (value - top.astype(np.float64)).astype(np.float32).astype(BF16)
    return top, rest


def unit(turns, period):
    angle = -2.0 * math.pi * (turns % period) / period
    return np.cos(angle), np.sin(angle)


@functools.cache
def tables(shards, samples):
    part = samples // (shards * shards)
    tiles = part // LANES
    m = np.arange(part)
    v = np.arange(LANES)
    s = np.arange(shards)
    half = shards // 2
    r = np.arange(half)
    wide = np.arange(2 * part)
    within = np.stack(unit(r[:, None] * wide[None, :], samples)).reshape(2, half, 2 * tiles, LANES)
    shift = np.stack(unit(r[:, None] * r[None, :], samples // (2 * part)), axis=1)
    shift = np.broadcast_to(shift[..., None], (half, 2, half, LANES))
    after = np.stack(unit(s[:, None] * m[None, :], samples // shards)).reshape(2, shards, tiles, LANES)
    middle = (half + shards * r)[:, None] * m[None, :]
    middle = np.stack(unit(middle, samples)).reshape(2, half, tiles, LANES)
    between = np.stack(unit(s[:, None] * v[None, :], part))
    j = np.arange(LANES // 2)
    rows = []
    for q2 in (j, LANES - 1 - j):
        c2, s2 = unit(q2[:, None] * v[None, :], LANES)
        rows += [np.concatenate([c2, -s2], axis=1), np.concatenate([s2, c2], axis=1)]
    last = np_halves(np.concatenate(rows, axis=0))
    fitting = np.zeros((half, SUB, LANES), np.float32)
    for own in range(half):
        for lane in range(LANES):
            slot = lane % SLOTS
            residue = own + SLOTS * slot if own else SLOTS * (slot % SUB) + SUB * (slot // SUB)
            if lane % PIECE >= SLOTS:
                residue = COARSE - residue if residue else COARSE // 2
            for odd in (3, 5, 7):
                fitting[own, odd, lane] = next(c for c in range(odd) if (residue + COARSE * c) % odd == 0)
    first = [x.astype(np.float32) for x in (within, shift)]
    second = [x.astype(np.float32) for x in (after, middle, between, fitting)] + [np.concatenate(last)]
    return first, second


def cmul(x, y):
    if x[1] is None:
        return x[0] * y[0], x[0] * y[1]
    return x[0] * y[0] - x[1] * y[1], x[0] * y[1] + x[1] * y[0]


def plus(a, b):
    return b if a is None else a if b is None else a + b


def minus(a, b):
    return a if b is None else -b if a is None else a - b


def cadd(x, y):
    return plus(x[0], y[0]), plus(x[1], y[1])


def csub(x, y):
    return minus(x[0], y[0]), minus(x[1], y[1])


def turn_back(x):
    return x[1], minus(None, x[0])


def four(x0, x1, x2, x3):
    s, d = cadd(x0, x2), csub(x0, x2)
    t, u = cadd(x1, x3), turn_back(csub(x1, x3))
    return cadd(s, t), cadd(d, u), csub(s, t), csub(d, u)


def sixteen(values):
    columns = [four(*values[low::4]) for low in range(4)]
    out = [None] * 16
    for k1 in range(4):
        terms = []
        for low in range(4):
            term = columns[low][k1]
            if low * k1 == 4:
                term = turn_back(term)
            elif low * k1:
                c, s = unit(np.float64(low * k1), 16)
                term = cmul(term, (F32(c), F32(s)))
            terms.append(term)
        for k2, value in enumerate(four(*terms)):
            out[k1 + 4 * k2] = value
    return out


def prepare_kernel(d_ref, x_ref, start_ref, count_ref, o_ref, s_ref, m_ref, x_scr, start_scr, count_scr, sems):
    small = [
        pltpu.make_async_copy(start_ref, start_scr, sems.at[0]),
        pltpu.make_async_copy(count_ref, count_scr, sems.at[1]),
    ]
    pieces = sems.shape[0] - 2
    size = x_ref.shape[0] // pieces
    copies = []
    for piece in range(pieces):
        here = pl.ds(piece * size, size)
        copies.append(pltpu.make_async_copy(x_ref.at[here], x_scr.at[here], sems.at[2 + piece]))
    for copy in small + copies:
        copy.start()

    own_class = d_ref[0] % SUB
    phi = lax.broadcasted_iota(jnp.int32, (SLOTS, COARSE), 1)
    slot = lax.broadcasted_iota(jnp.int32, (SLOTS, COARSE), 0)
    pairs = slot * SLOTS - jnp.where(slot < SUB, 0, SUB * SLOTS - SUB)
    mine = jnp.where(own_class == 0, pairs, own_class + SLOTS * slot)
    mirror = jnp.where(mine == 0, COARSE // 2, COARSE - mine)
    for index, (h, carries) in enumerate(PIECES):
        for k, residue in enumerate((mine, mirror)):
            gap = h * phi - residue
            hit = functools.reduce(jnp.logical_or, [gap == COARSE * c for c in carries])
            hit = jnp.where(hit, 1.0, 0.0)
            s_ref[pl.ds(index * PIECE + k * SLOTS, SLOTS), :] = hit.astype(BF16)

    for copy in small:
        copy.wait()
    bands, slots = start_ref.shape
    cell = [lax.broadcasted_iota(jnp.int32, (bands, bands), axis) for axis in range(2)]
    counts = jnp.where(cell[0] == cell[1], count_scr[...].astype(F32), 0.0)
    live = jnp.sum(counts, axis=1, keepdims=True).astype(jnp.int32)
    slot = lax.broadcasted_iota(jnp.int32, (bands, slots), 1)
    starts = jnp.where(slot < live, start_scr[...], -1).astype(F32)
    m_ref[...] = jnp.concatenate([starts] * (LANES // slots), axis=1)

    tiles = x_ref.shape[0] // 2
    for piece, copy in enumerate(copies):
        copy.wait()
        for at in range(piece * size // 2, (piece + 1) * size // 2, SUB):
            for row in range(2):
                o_ref[row * tiles + at : row * tiles + at + SUB, :] = x_scr[pl.ds(2 * at + row, SUB, stride=2), :]


def first_kernel(d_ref, x_ref, within_ref, shift_ref, o_ref):
    shards, tiles = x_ref.shape[:2]
    half = shards // 2
    me = d_ref[0] % half
    for k in range(tiles // SUB):
        inner = slice(k * SUB, (k + 1) * SUB)
        classes = sixteen([(x_ref[t, inner, :], None) for t in range(shards)])
        for r in range(half):
            if r:
                own = [shift_ref[me, part, r : r + 1, :] for part in range(2)]
                value = cmul(classes[r], cmul([within_ref[part, r, inner, :] for part in range(2)], own))
            else:
                value = classes[0][0], classes[half][0]
            for part in range(2):
                to = part * tiles + k * SUB
                o_ref[r, to : to + SUB, :] = value[part]


def second_kernel(d_ref, x_ref, after_ref, middle_ref, between_ref, fit_ref, table_ref, s_ref, o_ref, v_scr, x_scr, t_scr, dh_scr, dl_scr, r_scr, l_scr, h_scr):
    shards = 2 * x_ref.shape[0]
    tiles = x_ref.shape[1] // 4
    half = LANES // 2
    own_class = d_ref[0] % x_ref.shape[0]
    is_first = own_class == 0
    sub = lax.broadcasted_iota(jnp.int32, (SUB, LANES), 0)
    lead = jnp.logical_and(sub == 0, is_first)

    for k in range(tiles // SUB):
        rows = slice(k * SUB, (k + 1) * SUB)
        main, middle = [], []
        for s in range(shards):
            at = s % 2 * tiles + k * SUB
            re = x_ref[s // 2, at : at + SUB, :]
            im = x_ref[s // 2, 2 * tiles + at : 2 * tiles + at + SUB, :]
            main.append((re, jnp.where(is_first, 0.0, im)))
            c, sn = unit(np.float64(s), 2 * shards)
            middle.append((im * F32(c), im * F32(sn) if s else None))
        for slot, value in enumerate(sixteen(main)):
            value = cmul(value, (after_ref[0, slot, rows, :], after_ref[1, slot, rows, :]))
            for part in range(2):
                v_scr[pl.ds(part * tiles * shards + k * SUB * shards + slot, SUB, stride=shards), :] = value[part]
        for slot, value in enumerate(sixteen(middle)[: shards // 2]):
            value = cmul(value, (middle_ref[0, slot, rows, :], middle_ref[1, slot, rows, :]))
            for part in range(2):
                at = part * tiles * SUB + k * SUB * SUB + slot
                x_scr[pl.ds(at, SUB, stride=SUB), :] = value[part]

    groups = [[], [], []]
    for u in range(tiles):
        low, high, mid = [], [], []
        for part in range(2):
            at = part * tiles * shards + u * shards
            low.append(v_scr[at : at + SUB, :])
            high.append(v_scr[at + SUB : at + 2 * SUB, :])
            at = part * tiles * SUB + u * SUB
            mid.append(x_scr[at : at + SUB, :])
        groups[0].append(tuple(low))
        groups[1].append(tuple(jnp.where(is_first, mid[part], high[part]) for part in range(2)))
        groups[2].append(tuple(high))
    for group, values in enumerate(groups):
        for rho, value in enumerate(sixteen(values)):
            value = cmul(value, (between_ref[0, rho : rho + 1, :], between_ref[1, rho : rho + 1, :]))
            for part in range(2):
                t_scr[group, rho, part] = value[part]

    for rho in range(tiles):
        for part in range(2):
            back = tiles - 1 - rho
            low = jnp.concatenate([t_scr[0, rho, part], t_scr[1, rho, part]], axis=0)
            turned = jnp.where(lead, t_scr[2, rho, part], t_scr[0, back, part])
            high = jnp.concatenate([turned, t_scr[1, back, part]], axis=0)
            for k, tile in enumerate((low, high)):
                top, rest = halves(tile)
                rows = pl.ds(rho * PIECE + k * SLOTS, SLOTS)
                cols = pl.ds(part * LANES, LANES)
                dh_scr[rows, cols] = top
                dl_scr[rows, cols] = rest
    dims = (((1,), (1,)), ((), ()))
    dot_t = functools.partial(lax.dot_general, dimension_numbers=dims, preferred_element_type=F32)
    lane = lax.broadcasted_iota(jnp.int32, (half, 2 * LANES), 1)
    within = lane % PIECE
    from_low = jnp.logical_or(within < SLOTS, jnp.logical_and(within == SLOTS, is_first))
    scale = 1.0 / (shards * shards * tiles * LANES)
    powers = []
    for part in range(2):
        top = dh_scr[part * 256 : (part + 1) * 256, :]
        rest = dl_scr[part * 256 : (part + 1) * 256, :]
        z = dot_t(table_ref[...], top)
        z = z[:256] + z[256:] + dot_t(table_ref[:256, :], rest)
        z = z * z
        low = z[0:half] + z[half : 2 * half]
        high = z[2 * half : 3 * half] + z[3 * half :]
        powers.append(jnp.where(from_low, low, high) * scale)

    count = 2 * SLOTS * half * tiles

    def over_all(value):
        column = jnp.sum(value, axis=0, keepdims=True)
        return jnp.sum(column, axis=1, keepdims=True)

    mean = over_all(powers[0] + powers[1]) / count
    off0, off1 = powers[0] - mean, powers[1] - mean
    deviation = over_all(off0 * off0 + off1 * off1)
    stats = jnp.where(sub[0:1] + lax.broadcasted_iota(jnp.int32, (1, LANES), 1) < half, mean, deviation)
    for t in range(shards):
        o_ref[t * ROWS + 2 * SUB : (t + 1) * ROWS, :] = stats

    for group in range(4):
        value = powers[group // 2][:, (group % 2) * LANES : (group % 2 + 1) * LANES]
        for shift in range(4):
            at = (group * 4 + shift) * half
            r_scr[at : at + half, :] = pltpu.roll(value, shift * PIECE, 1) if shift else value
    lane8 = lax.broadcasted_iota(jnp.int32, (SUB, LANES), 1) // PIECE
    fits = {}
    for index, (h, _) in enumerate(PIECES):
        if ODD[h] > 1:
            fit = jnp.broadcast_to(fit_ref[own_class, ODD[h] : ODD[h] + 1, :], (SUB, LANES))
            fits[index % 4, ODD[h]] = jnp.where(lane8 == index % 4, fit, -1.0).astype(jnp.int32)
    for chunk in range(CHUNKS):
        for g_pair in range(tiles // 2):
            parts = []
            for g0 in (2 * g_pair, 2 * g_pair + 1):
                tile = None
                for place in range(4):
                    h, carries = PIECES[chunk * 4 + place]
                    for c in carries:
                        rho, e = (h * g0 + c) % tiles, (h * g0 + c) // tiles
                        shift = (place - rho % 4) % 4
                        rows = pl.ds((rho // 4 * 4 + shift) * half + e, SUB, stride=h)
                        got = r_scr[rows, :]
                        here = lane8 == place if c == carries[0] else fits[place, ODD[h]] == c % ODD[h]
                        tile = got if tile is None else jnp.where(here, got, tile)
                parts.append(tile)
            top, rest = halves(jnp.concatenate(parts, axis=0))
            cols = pl.ds(chunk * LANES, LANES)
            l_scr[pl.ds(g_pair * 16, 16), cols] = top
            l_scr[pl.ds(LANES + g_pair * 16, 16), cols] = rest
    both = jnp.dot(l_scr[...], s_ref[...], preferred_element_type=F32)
    for tile in range(2):
        cols = slice(tile * LANES, (tile + 1) * LANES)
        h_scr[tile * LANES : (tile + 1) * LANES, :] = both[:LANES, cols] + both[LANES:, cols]
    for t in range(shards):
        for tile in range(2):
            rows = pl.ds(tile * LANES + (t % 2) * half + t // 2, SUB, stride=SUB)
            o_ref[t * ROWS + tile * SUB : t * ROWS + (tile + 1) * SUB, :] = h_scr[rows, :]


def third_kernel(m_ref, x_ref, hs_ref, msg_ref, level_ref):
    shards = x_ref.shape[0] // ROWS
    holders = shards // 2
    count = 2 * SLOTS * (LANES // 2) * SLOTS
    tiles = []
    for row in range(2):
        blocks = [(row * holders + r) * ROWS for r in range(holders)]
        sums = [x_ref[at : at + 2 * SUB, :] for at in blocks]
        stats = [x_ref[at + 2 * SUB : at + ROWS, :] for at in blocks]
        total, both = sums[0], stats[0]
        for r in range(1, holders):
            total, both = total + sums[r], both + stats[r]
        mean = both[:, 0:1] / holders
        spread = both[:, LANES // 2 : LANES // 2 + 1]
        for r in range(holders):
            off = stats[r][:, 0:1] - mean
            spread = spread + count * (off * off)
        scale = 1.0 / jnp.sqrt(spread / (count * holders) + EPSILON)
        tiles.append([(total[k * SUB : (k + 1) * SUB] - HARM * mean) * scale for k in range(2)])
    for row in range(2):
        for k in range(2):
            for g in range(SUB):
                hs_ref[row : row + 1, pl.ds(g * COARSE + k * LANES, LANES)] = tiles[row][k][g : g + 1]
    for k in range(2):
        level_ref[k * SUB : (k + 1) * SUB, :] = (tiles[0][k] + tiles[1][k]) / 2
    peak = jnp.concatenate([jnp.maximum(tiles[0][k], tiles[1][k]) for k in range(2)], axis=0)
    for e in range(m_ref.shape[0]):
        msg_ref[e * ROWS : e * ROWS + 2 * SUB, :] = peak
        msg_ref[e * ROWS + 2 * SUB : (e + 1) * ROWS, :] = m_ref[e : e + 1, :]


def sift_kernel(x_ref, level_ref, bins_ref, o_ref, hs_ref, out_scr, sems):
    steps = sems.shape[0] - 1
    bins_out = pltpu.make_async_copy(bins_ref, hs_ref, sems.at[steps])
    bins_out.start()
    bands, slots = o_ref.shape[:2]
    level = level_ref[...]
    rows = bands * slots
    diff = jnp.concatenate([x_ref[d * ROWS : d * ROWS + 2 * SUB, :] - level for d in range(bands)], axis=0)
    lane = lax.broadcasted_iota(jnp.int32, (rows, LANES), 1)
    line = lax.broadcasted_iota(jnp.int32, (rows, LANES), 0)
    listed = [x_ref[d * ROWS + 2 * SUB : (d + 1) * ROWS, :] for d in range(bands)]
    listed = jnp.concatenate([jnp.broadcast_to(x, (slots, LANES)) for x in listed], axis=0)
    start = jnp.sum(jnp.where(lane == line & (slots - 1), listed, 0.0), axis=1, keepdims=True)
    start = jnp.broadcast_to(start, (rows, LANES)).astype(jnp.int32)
    block = jnp.maximum(start, 0)
    tile_id, offset = block >> 7, block & (LANES - 1)
    band = line & -slots

    def pick(which):
        place = band + ((which & 1) << 3) + (which >> 1)
        return jnp.where(lane == place, 1.0, 0.0).astype(BF16)

    both = jnp.concatenate([pick(tile_id), pick(tile_id + 1)], axis=0)
    parts = jnp.dot(both, jnp.concatenate(halves(diff), axis=1), preferred_element_type=F32)
    parts = parts[:, :LANES] + parts[:, LANES:]
    copies = []
    for step in range(steps):
        part = slice(step * rows // steps, (step + 1) * rows // steps)
        joined = jnp.where(lane[part] >= offset[part], parts[:rows][part], parts[rows:][part])
        moved = jnp.take_along_axis(joined, (lane[part] + offset[part]) & (LANES - 1), axis=1)
        moved = jnp.where(start[part] >= 0, moved, 0.0)
        here = pl.ds(step * bands // steps, bands // steps)
        out_scr[here] = moved.reshape(bands // steps, slots, LANES)
        copies.append(pltpu.make_async_copy(out_scr.at[here], o_ref.at[here], sems.at[step]))
        copies[-1].start()
    for copy in copies:
        copy.wait()
    bins_out.wait()


PARAMS = pltpu.CompilerParams(vmem_limit_bytes=16 * 2**20)


def near(array):
    return pltpu.with_memory_space_constraint(array, pltpu.VMEM)


def shape(*dims):
    return pltpu.VMEM(dims, F32)


def spaces(*kinds):
    return [pl.BlockSpec(memory_space=pltpu.SMEM if kind == "s" else pltpu.VMEM) for kind in kinds]


def run_prepare(me, series, starts, counts, shards):
    tiles = series.shape[1] // LANES
    lines = jnp.swapaxes(series.reshape(2, tiles, LANES), 0, 1).reshape(2 * tiles, LANES)
    rows, mapping, markers = pl.pallas_call(
        prepare_kernel,
        out_shape=(
            shape(2 * tiles, LANES),
            pltpu.VMEM((CHUNKS * LANES, COARSE), BF16),
            shape(starts.shape[0], LANES),
        ),
        in_specs=spaces("s") + [pl.BlockSpec(memory_space=pl.ANY)] * 3,
        out_specs=spaces(*"vvv"),
        scratch_shapes=[
            pltpu.VMEM((2 * tiles, LANES), F32),
            pltpu.VMEM(starts.shape, jnp.int32),
            pltpu.VMEM(counts.shape, jnp.int32),
            pltpu.SemaphoreType.DMA((6,)),
        ],
        compiler_params=PARAMS,
    )(me, *[pltpu.with_memory_space_constraint(x, pltpu.HBM) for x in (lines, starts, counts)])
    return rows.reshape(shards, -1, LANES), mapping, markers


def run_first(me, received, first):
    shards = received.shape[0]
    within, shift = map(jnp.asarray, first)
    return pl.pallas_call(
        first_kernel,
        out_shape=shape(shards // 2, 2 * received.shape[1], LANES),
        in_specs=spaces(*"svvv"),
        out_specs=spaces("v")[0],
        compiler_params=PARAMS,
    )(me, *[near(x) for x in (received, within, shift)])


def run_second(me, received, second, mapping):
    shards = 2 * received.shape[0]
    inputs = [near(x) for x in (received, *map(jnp.asarray, second), mapping)]
    sent = pl.pallas_call(
        second_kernel,
        out_shape=shape(shards * ROWS, LANES),
        in_specs=spaces("s", *"vvvvvvv"),
        out_specs=spaces("v")[0],
        scratch_shapes=[
            pltpu.VMEM((2 * SLOTS * SLOTS, LANES), F32),
            pltpu.VMEM((2 * SLOTS * SUB, LANES), F32),
            pltpu.VMEM((3, SLOTS, 2, SUB, LANES), F32),
            pltpu.VMEM((SLOTS * PIECE, 2 * LANES), BF16),
            pltpu.VMEM((SLOTS * PIECE, 2 * LANES), BF16),
            pltpu.VMEM((16 * LANES // 2, LANES), F32),
            pltpu.VMEM((2 * LANES, CHUNKS * LANES), BF16),
            pltpu.VMEM((2 * LANES, LANES), F32),
        ],
        compiler_params=PARAMS,
    )(me, *inputs)
    return sent.reshape(shards, 1, ROWS * LANES)


def run_third(received, markers):
    bands = markers.shape[0]
    bins, message, level = pl.pallas_call(
        third_kernel,
        out_shape=(shape(2, SUB * COARSE), shape(bands * ROWS, LANES), shape(2 * SUB, LANES)),
        in_specs=spaces(*"vv"),
        out_specs=spaces(*"vvv"),
        compiler_params=PARAMS,
    )(near(markers), near(received.reshape(-1, LANES)))
    return bins, message.reshape(bands, 1, ROWS * LANES), level


def run_sift(received, level, bins):
    bands = received.shape[0]
    steps = 1
    anywhere = pl.BlockSpec(memory_space=pl.ANY)
    return pl.pallas_call(
        sift_kernel,
        out_shape=(
            jax.ShapeDtypeStruct((bands, 2 * SUB, LANES), F32),
            jax.ShapeDtypeStruct(bins.shape, F32),
        ),
        in_specs=spaces(*"vvv"),
        out_specs=[anywhere, anywhere],
        scratch_shapes=[
            pltpu.VMEM((bands, 2 * SUB, LANES), F32),
            pltpu.SemaphoreType.DMA((steps + 1,)),
        ],
        compiler_params=PARAMS,
    )(near(received.reshape(-1, LANES)), near(level), near(bins))


def per_device(series, cand_start, cand_count):
    shards = lax.axis_size("tm")
    first, second = tables(shards, shards * series.shape[1])
    me = lax.axis_index("tm").astype(jnp.int32).reshape(1)
    swap = functools.partial(lax.all_to_all, split_axis=0, concat_axis=0, tiled=True)
    rows, mapping, markers = run_prepare(me, series, cand_start[0, 0], cand_count[0], shards)
    half = shards // 2
    by_row = [list(range(half)), list(range(half, shards))]
    classes = swap(run_first(me, swap(rows, "tm"), first), "tm", axis_index_groups=by_row)
    sums = swap(run_second(me, classes, second, mapping), "tm")
    bins, message, level = run_third(sums, markers)
    sifted, harmonic_sum = run_sift(swap(message, "dm"), level, bins)
    return harmonic_sum, sifted[None, None]


def solution(mesh):
    return jax.shard_map(
        per_device,
        mesh=mesh,
        in_specs=(
            P(("beam", "dm"), "tm"),
            P(("beam", "tm"), "dm", None, None),
            P(("beam", "tm"), "dm", None),
        ),
        out_specs=(P(("beam", "dm"), "tm"), P(("beam", "tm"), "dm", None, None, None)),
        check_vma=False,
    )
```

```python
import functools
import math

import jax
import jax.numpy as jnp
import numpy as np
from jax import lax
from jax.experimental import pallas as pl
from jax.experimental.pallas import tpu as pltpu
from jax.sharding import PartitionSpec as P

HARM = 8
BW = 128
EPSILON = 1e-06

LANES = 128
SUB = 8
COARSE = 256
SLOTS = 16
PIECE = 32
ODD = {h: h // (h & -h) for h in range(1, HARM + 1)}
PIECES = [(h, range(c, c + ODD[h])) for h in range(1, HARM + 1) for c in range(0, h, ODD[h])]
CHUNKS = len(PIECES) // 4
ROWS = 2 * SUB + 1

F32 = jnp.float32
BF16 = jnp.bfloat16


def halves(value):
    top = value.astype(BF16)
    return top, (value - top.astype(F32)).astype(BF16)


def np_halves(value):
    top = value.astype(np.float32).astype(BF16)
    rest = (value - top.astype(np.float64)).astype(np.float32).astype(BF16)
    return top, rest


def unit(turns, period):
    angle = -2.0 * math.pi * (turns % period) / period
    return np.cos(angle), np.sin(angle)


@functools.cache
def tables(shards, samples):
    part = samples // (shards * shards)
    tiles = part // LANES
    m = np.arange(part)
    v = np.arange(LANES)
    s = np.arange(shards)
    half = shards // 2
    r = np.arange(half)
    wide = np.arange(2 * part)
    within = np.stack(unit(r[:, None] * wide[None, :], samples)).reshape(2, half, 2 * tiles, LANES)
    shift = np.stack(unit(r[:, None] * r[None, :], samples // (2 * part)), axis=1)
    shift = np.broadcast_to(shift[..., None], (half, 2, half, LANES))
    after = np.stack(unit(s[:, None] * m[None, :], samples // shards)).reshape(2, shards, tiles, LANES)
    middle = (half + shards * r)[:, None] * m[None, :]
    middle = np.stack(unit(middle, samples)).reshape(2, half, tiles, LANES)
    between = np.stack(unit(s[:, None] * v[None, :], part))
    j = np.arange(LANES // 2)
    rows = []
    for q2 in (j, LANES - 1 - j):
        c2, s2 = unit(q2[:, None] * v[None, :], LANES)
        rows += [np.concatenate([c2, -s2], axis=1), np.concatenate([s2, c2], axis=1)]
    last = np_halves(np.concatenate(rows, axis=0))
    fitting = np.zeros((half, SUB, LANES), np.float32)
    for own in range(half):
        for lane in range(LANES):
            slot = lane % SLOTS
            residue = own + SLOTS * slot if own else SLOTS * (slot % SUB) + SUB * (slot // SUB)
            if lane % PIECE >= SLOTS:
                residue = COARSE - residue if residue else COARSE // 2
            for odd in (3, 5, 7):
                fitting[own, odd, lane] = next(c for c in range(odd) if (residue + COARSE * c) % odd == 0)
    first = [x.astype(np.float32) for x in (within, shift)]
    second = [x.astype(np.float32) for x in (after, middle, between, fitting)] + [np.concatenate(last)]
    return first, second


def cmul(x, y):
    if x[1] is None:
        return x[0] * y[0], x[0] * y[1]
    return x[0] * y[0] - x[1] * y[1], x[0] * y[1] + x[1] * y[0]


def plus(a, b):
    return b if a is None else a if b is None else a + b


def minus(a, b):
    return a if b is None else -b if a is None else a - b


def cadd(x, y):
    return plus(x[0], y[0]), plus(x[1], y[1])


def csub(x, y):
    return minus(x[0], y[0]), minus(x[1], y[1])


def turn_back(x):
    return x[1], minus(None, x[0])


def four(x0, x1, x2, x3):
    s, d = cadd(x0, x2), csub(x0, x2)
    t, u = cadd(x1, x3), turn_back(csub(x1, x3))
    return cadd(s, t), cadd(d, u), csub(s, t), csub(d, u)


def sixteen(values):
    columns = [four(*values[low::4]) for low in range(4)]
    out = [None] * 16
    for k1 in range(4):
        terms = []
        for low in range(4):
            term = columns[low][k1]
            if low * k1 == 4:
                term = turn_back(term)
            elif low * k1:
                c, s = unit(np.float64(low * k1), 16)
                term = cmul(term, (F32(c), F32(s)))
            terms.append(term)
        for k2, value in enumerate(four(*terms)):
            out[k1 + 4 * k2] = value
    return out


def prepare_kernel(d_ref, x_ref, start_ref, count_ref, o_ref, s_ref, m_ref, x_scr, start_scr, count_scr, sems):
    small = [
        pltpu.make_async_copy(start_ref, start_scr, sems.at[0]),
        pltpu.make_async_copy(count_ref, count_scr, sems.at[1]),
    ]
    pieces = sems.shape[0] - 2
    size = x_ref.shape[0] // pieces
    copies = []
    for piece in range(pieces):
        here = pl.ds(piece * size, size)
        copies.append(pltpu.make_async_copy(x_ref.at[here], x_scr.at[here], sems.at[2 + piece]))
    for copy in small + copies:
        copy.start()

    own_class = d_ref[0] % SUB
    phi = lax.broadcasted_iota(jnp.int32, (SLOTS, COARSE), 1)
    slot = lax.broadcasted_iota(jnp.int32, (SLOTS, COARSE), 0)
    pairs = slot * SLOTS - jnp.where(slot < SUB, 0, SUB * SLOTS - SUB)
    mine = jnp.where(own_class == 0, pairs, own_class + SLOTS * slot)
    mirror = jnp.where(mine == 0, COARSE // 2, COARSE - mine)
    for index, (h, carries) in enumerate(PIECES):
        for k, residue in enumerate((mine, mirror)):
            gap = h * phi - residue
            hit = functools.reduce(jnp.logical_or, [gap == COARSE * c for c in carries])
            hit = jnp.where(hit, 1.0, 0.0)
            s_ref[pl.ds(index * PIECE + k * SLOTS, SLOTS), :] = hit.astype(BF16)

    for copy in small:
        copy.wait()
    bands, slots = start_ref.shape
    cell = [lax.broadcasted_iota(jnp.int32, (bands, bands), axis) for axis in range(2)]
    counts = jnp.where(cell[0] == cell[1], count_scr[...].astype(F32), 0.0)
    live = jnp.sum(counts, axis=1, keepdims=True).astype(jnp.int32)
    slot = lax.broadcasted_iota(jnp.int32, (bands, slots), 1)
    starts = jnp.where(slot < live, start_scr[...], -1).astype(F32)
    m_ref[...] = jnp.concatenate([starts] * (LANES // slots), axis=1)

    tiles = x_ref.shape[0] // 2
    for piece, copy in enumerate(copies):
        copy.wait()
        for at in range(piece * size // 2, (piece + 1) * size // 2, SUB):
            for row in range(2):
                o_ref[row * tiles + at : row * tiles + at + SUB, :] = x_scr[pl.ds(2 * at + row, SUB, stride=2), :]


def first_kernel(d_ref, x_ref, within_ref, shift_ref, o_ref):
    shards, tiles = x_ref.shape[:2]
    half = shards // 2
    me = d_ref[0] % half
    for k in range(tiles // SUB):
        inner = slice(k * SUB, (k + 1) * SUB)
        classes = sixteen([(x_ref[t, inner, :], None) for t in range(shards)])
        for r in range(half):
            if r:
                own = [shift_ref[me, part, r : r + 1, :] for part in range(2)]
                value = cmul(classes[r], cmul([within_ref[part, r, inner, :] for part in range(2)], own))
            else:
                value = classes[0][0], classes[half][0]
            for part in range(2):
                to = part * tiles + k * SUB
                o_ref[r, to : to + SUB, :] = value[part]


def second_kernel(d_ref, x_ref, after_ref, middle_ref, between_ref, fit_ref, table_ref, s_ref, o_ref, v_scr, x_scr, t_scr, dh_scr, dl_scr, r_scr, l_scr, h_scr):
    shards = 2 * x_ref.shape[0]
    tiles = x_ref.shape[1] // 4
    half = LANES // 2
    own_class = d_ref[0] % x_ref.shape[0]
    is_first = own_class == 0
    sub = lax.broadcasted_iota(jnp.int32, (SUB, LANES), 0)
    lead = jnp.logical_and(sub == 0, is_first)

    for k in range(tiles // SUB):
        rows = slice(k * SUB, (k + 1) * SUB)
        main, middle = [], []
        for s in range(shards):
            at = s % 2 * tiles + k * SUB
            re = x_ref[s // 2, at : at + SUB, :]
            im = x_ref[s // 2, 2 * tiles + at : 2 * tiles + at + SUB, :]
            main.append((re, jnp.where(is_first, 0.0, im)))
            c, sn = unit(np.float64(s), 2 * shards)
            middle.append((im * F32(c), im * F32(sn) if s else None))
        for slot, value in enumerate(sixteen(main)):
            value = cmul(value, (after_ref[0, slot, rows, :], after_ref[1, slot, rows, :]))
            for part in range(2):
                v_scr[pl.ds(part * tiles * shards + k * SUB * shards + slot, SUB, stride=shards), :] = value[part]
        for slot, value in enumerate(sixteen(middle)[: shards // 2]):
            value = cmul(value, (middle_ref[0, slot, rows, :], middle_ref[1, slot, rows, :]))
            for part in range(2):
                at = part * tiles * SUB + k * SUB * SUB + slot
                x_scr[pl.ds(at, SUB, stride=SUB), :] = value[part]

    groups = [[], [], []]
    for u in range(tiles):
        low, high, mid = [], [], []
        for part in range(2):
            at = part * tiles * shards + u * shards
            low.append(v_scr[at : at + SUB, :])
            high.append(v_scr[at + SUB : at + 2 * SUB, :])
            at = part * tiles * SUB + u * SUB
            mid.append(x_scr[at : at + SUB, :])
        groups[0].append(tuple(low))
        groups[1].append(tuple(jnp.where(is_first, mid[part], high[part]) for part in range(2)))
        groups[2].append(tuple(high))
    for group, values in enumerate(groups):
        for rho, value in enumerate(sixteen(values)):
            value = cmul(value, (between_ref[0, rho : rho + 1, :], between_ref[1, rho : rho + 1, :]))
            for part in range(2):
                t_scr[group, rho, part] = value[part]

    for rho in range(tiles):
        for part in range(2):
            back = tiles - 1 - rho
            low = jnp.concatenate([t_scr[0, rho, part], t_scr[1, rho, part]], axis=0)
            turned = jnp.where(lead, t_scr[2, rho, part], t_scr[0, back, part])
            high = jnp.concatenate([turned, t_scr[1, back, part]], axis=0)
            for k, tile in enumerate((low, high)):
                top, rest = halves(tile)
                rows = pl.ds(rho * PIECE + k * SLOTS, SLOTS)
                cols = pl.ds(part * LANES, LANES)
                dh_scr[rows, cols] = top
                dl_scr[rows, cols] = rest
    dims = (((1,), (1,)), ((), ()))
    dot_t = functools.partial(lax.dot_general, dimension_numbers=dims, preferred_element_type=F32)
    lane = lax.broadcasted_iota(jnp.int32, (half, 2 * LANES), 1)
    within = lane % PIECE
    from_low = jnp.logical_or(within < SLOTS, jnp.logical_and(within == SLOTS, is_first))
    scale = 1.0 / (shards * shards * tiles * LANES)
    powers = []
    for part in range(2):
        top = dh_scr[part * 256 : (part + 1) * 256, :]
        rest = dl_scr[part * 256 : (part + 1) * 256, :]
        z = dot_t(table_ref[...], top)
        z = z[:256] + z[256:] + dot_t(table_ref[:256, :], rest)
        z = z * z
        low = z[0:half] + z[half : 2 * half]
        high = z[2 * half : 3 * half] + z[3 * half :]
        powers.append(jnp.where(from_low, low, high) * scale)

    count = 2 * SLOTS * half * tiles

    def over_all(value):
        column = jnp.sum(value, axis=0, keepdims=True)
        return jnp.sum(column, axis=1, keepdims=True)

    mean = over_all(powers[0] + powers[1]) / count
    off0, off1 = powers[0] - mean, powers[1] - mean
    deviation = over_all(off0 * off0 + off1 * off1)
    stats = jnp.where(sub[0:1] + lax.broadcasted_iota(jnp.int32, (1, LANES), 1) < half, mean, deviation)
    for t in range(shards):
        o_ref[t * ROWS + 2 * SUB : (t + 1) * ROWS, :] = stats

    for group in range(4):
        value = powers[group // 2][:, (group % 2) * LANES : (group % 2 + 1) * LANES]
        for shift in range(4):
            at = (group * 4 + shift) * half
            r_scr[at : at + half, :] = pltpu.roll(value, shift * PIECE, 1) if shift else value
    lane8 = lax.broadcasted_iota(jnp.int32, (SUB, LANES), 1) // PIECE
    fits = {}
    for index, (h, _) in enumerate(PIECES):
        if ODD[h] > 1:
            fit = jnp.broadcast_to(fit_ref[own_class, ODD[h] : ODD[h] + 1, :], (SUB, LANES))
            fits[index % 4, ODD[h]] = jnp.where(lane8 == index % 4, fit, -1.0).astype(jnp.int32)
    for chunk in range(CHUNKS):
        for g_pair in range(tiles // 2):
            parts = []
            for g0 in (2 * g_pair, 2 * g_pair + 1):
                tile = None
                for place in range(4):
                    h, carries = PIECES[chunk * 4 + place]
                    for c in carries:
                        rho, e = (h * g0 + c) % tiles, (h * g0 + c) // tiles
                        shift = (place - rho % 4) % 4
                        rows = pl.ds((rho // 4 * 4 + shift) * half + e, SUB, stride=h)
                        got = r_scr[rows, :]
                        here = lane8 == place if c == carries[0] else fits[place, ODD[h]] == c % ODD[h]
                        tile = got if tile is None else jnp.where(here, got, tile)
                parts.append(tile)
            top, rest = halves(jnp.concatenate(parts, axis=0))
            cols = pl.ds(chunk * LANES, LANES)
            l_scr[pl.ds(g_pair * 16, 16), cols] = top
            l_scr[pl.ds(LANES + g_pair * 16, 16), cols] = rest
    both = jnp.dot(l_scr[...], s_ref[...], preferred_element_type=F32)
    for tile in range(2):
        cols = slice(tile * LANES, (tile + 1) * LANES)
        h_scr[tile * LANES : (tile + 1) * LANES, :] = both[:LANES, cols] + both[LANES:, cols]
    for t in range(shards):
        for tile in range(2):
            rows = pl.ds(tile * LANES + (t % 2) * half + t // 2, SUB, stride=SUB)
            o_ref[t * ROWS + tile * SUB : t * ROWS + (tile + 1) * SUB, :] = h_scr[rows, :]


def third_kernel(m_ref, x_ref, hs_ref, msg_ref, level_ref):
    shards = x_ref.shape[0] // ROWS
    holders = shards // 2
    count = 2 * SLOTS * (LANES // 2) * SLOTS
    tiles = []
    for row in range(2):
        blocks = [(row * holders + r) * ROWS for r in range(holders)]
        sums = [x_ref[at : at + 2 * SUB, :] for at in blocks]
        stats = [x_ref[at + 2 * SUB : at + ROWS, :] for at in blocks]
        total, both = sums[0], stats[0]
        for r in range(1, holders):
            total, both = total + sums[r], both + stats[r]
        mean = both[:, 0:1] / holders
        spread = both[:, LANES // 2 : LANES // 2 + 1]
        for r in range(holders):
            off = stats[r][:, 0:1] - mean
            spread = spread + count * (off * off)
        scale = 1.0 / jnp.sqrt(spread / (count * holders) + EPSILON)
        tiles.append([(total[k * SUB : (k + 1) * SUB] - HARM * mean) * scale for k in range(2)])
    for row in range(2):
        for k in range(2):
            for g in range(SUB):
                hs_ref[row : row + 1, pl.ds(g * COARSE + k * LANES, LANES)] = tiles[row][k][g : g + 1]
    for k in range(2):
        level_ref[k * SUB : (k + 1) * SUB, :] = (tiles[0][k] + tiles[1][k]) / 2
    peak = jnp.concatenate([jnp.maximum(tiles[0][k], tiles[1][k]) for k in range(2)], axis=0)
    for e in range(m_ref.shape[0]):
        msg_ref[e * ROWS : e * ROWS + 2 * SUB, :] = peak
        msg_ref[e * ROWS + 2 * SUB : (e + 1) * ROWS, :] = m_ref[e : e + 1, :]


def sift_kernel(x_ref, level_ref, bins_ref, o_ref, hs_ref):
    hs_ref[...] = bins_ref[...]
    bands, slots = o_ref.shape[:2]
    level = level_ref[...]
    rows = bands * slots
    diff = jnp.concatenate([x_ref[d * ROWS : d * ROWS + 2 * SUB, :] - level for d in range(bands)], axis=0)
    lane = lax.broadcasted_iota(jnp.int32, (rows, LANES), 1)
    line = lax.broadcasted_iota(jnp.int32, (rows, LANES), 0)
    listed = [x_ref[d * ROWS + 2 * SUB : (d + 1) * ROWS, :] for d in range(bands)]
    listed = jnp.concatenate([jnp.broadcast_to(x, (slots, LANES)) for x in listed], axis=0)
    start = jnp.sum(jnp.where(lane == line & (slots - 1), listed, 0.0), axis=1, keepdims=True)
    start = jnp.broadcast_to(start, (rows, LANES)).astype(jnp.int32)
    block = jnp.maximum(start, 0)
    tile_id, offset = block >> 7, block & (LANES - 1)
    band = line & -slots

    def pick(which):
        place = band + ((which & 1) << 3) + (which >> 1)
        return jnp.where(lane == place, 1.0, 0.0).astype(BF16)

    both = jnp.concatenate([pick(tile_id), pick(tile_id + 1)], axis=0)
    parts = jnp.dot(both, jnp.concatenate(halves(diff), axis=1), preferred_element_type=F32)
    parts = parts[:, :LANES] + parts[:, LANES:]
    joined = jnp.where(lane >= offset, parts[:rows], parts[rows:])
    moved = jnp.take_along_axis(joined, (lane + offset) & (LANES - 1), axis=1)
    o_ref[...] = jnp.where(start >= 0, moved, 0.0).reshape(bands, slots, LANES)


PARAMS = pltpu.CompilerParams(vmem_limit_bytes=16 * 2**20)


def near(array):
    return pltpu.with_memory_space_constraint(array, pltpu.VMEM)


def shape(*dims):
    return pltpu.VMEM(dims, F32)


def spaces(*kinds):
    return [pl.BlockSpec(memory_space=pltpu.SMEM if kind == "s" else pltpu.VMEM) for kind in kinds]


def run_prepare(me, series, starts, counts, shards):
    tiles = series.shape[1] // LANES
    lines = jnp.swapaxes(series.reshape(2, tiles, LANES), 0, 1).reshape(2 * tiles, LANES)
    rows, mapping, markers = pl.pallas_call(
        prepare_kernel,
        out_shape=(
            shape(2 * tiles, LANES),
            pltpu.VMEM((CHUNKS * LANES, COARSE), BF16),
            shape(starts.shape[0], LANES),
        ),
        in_specs=spaces("s") + [pl.BlockSpec(memory_space=pl.ANY)] * 3,
        out_specs=spaces(*"vvv"),
        scratch_shapes=[
            pltpu.VMEM((2 * tiles, LANES), F32),
            pltpu.VMEM(starts.shape, jnp.int32),
            pltpu.VMEM(counts.shape, jnp.int32),
            pltpu.SemaphoreType.DMA((6,)),
        ],
        compiler_params=PARAMS,
    )(me, *[pltpu.with_memory_space_constraint(x, pltpu.HBM) for x in (lines, starts, counts)])
    return rows.reshape(shards, -1, LANES), mapping, markers


def run_first(me, received, first):
    shards = received.shape[0]
    within, shift = map(jnp.asarray, first)
    return pl.pallas_call(
        first_kernel,
        out_shape=shape(shards // 2, 2 * received.shape[1], LANES),
        in_specs=spaces(*"svvv"),
        out_specs=spaces("v")[0],
        compiler_params=PARAMS,
    )(me, *[near(x) for x in (received, within, shift)])


def run_second(me, received, second, mapping):
    shards = 2 * received.shape[0]
    inputs = [near(x) for x in (received, *map(jnp.asarray, second), mapping)]
    sent = pl.pallas_call(
        second_kernel,
        out_shape=shape(shards * ROWS, LANES),
        in_specs=spaces("s", *"vvvvvvv"),
        out_specs=spaces("v")[0],
        scratch_shapes=[
            pltpu.VMEM((2 * SLOTS * SLOTS, LANES), F32),
            pltpu.VMEM((2 * SLOTS * SUB, LANES), F32),
            pltpu.VMEM((3, SLOTS, 2, SUB, LANES), F32),
            pltpu.VMEM((SLOTS * PIECE, 2 * LANES), BF16),
            pltpu.VMEM((SLOTS * PIECE, 2 * LANES), BF16),
            pltpu.VMEM((16 * LANES // 2, LANES), F32),
            pltpu.VMEM((2 * LANES, CHUNKS * LANES), BF16),
            pltpu.VMEM((2 * LANES, LANES), F32),
        ],
        compiler_params=PARAMS,
    )(me, *inputs)
    return sent.reshape(shards, 1, ROWS * LANES)


def run_third(received, markers):
    bands = markers.shape[0]
    bins, message, level = pl.pallas_call(
        third_kernel,
        out_shape=(shape(2, SUB * COARSE), shape(bands * ROWS, LANES), shape(2 * SUB, LANES)),
        in_specs=spaces(*"vv"),
        out_specs=spaces(*"vvv"),
        compiler_params=PARAMS,
    )(near(markers), near(received.reshape(-1, LANES)))
    return bins, message.reshape(bands, 1, ROWS * LANES), level


def run_sift(received, level, bins):
    bands = received.shape[0]
    return pl.pallas_call(
        sift_kernel,
        out_shape=(
            jax.ShapeDtypeStruct((bands, 2 * SUB, LANES), F32),
            jax.ShapeDtypeStruct(bins.shape, F32),
        ),
        in_specs=spaces(*"vvv"),
        out_specs=spaces(*"vv"),
        compiler_params=PARAMS,
    )(near(received.reshape(-1, LANES)), near(level), near(bins))


def per_device(series, cand_start, cand_count):
    shards = lax.axis_size("tm")
    first, second = tables(shards, shards * series.shape[1])
    me = lax.axis_index("tm").astype(jnp.int32).reshape(1)
    swap = functools.partial(lax.all_to_all, split_axis=0, concat_axis=0, tiled=True)
    rows, mapping, markers = run_prepare(me, series, cand_start[0, 0], cand_count[0], shards)
    half = shards // 2
    by_row = [list(range(half)), list(range(half, shards))]
    classes = swap(run_first(me, swap(rows, "tm"), first), "tm", axis_index_groups=by_row)
    sums = swap(run_second(me, classes, second, mapping), "tm")
    bins, message, level = run_third(sums, markers)
    sifted, harmonic_sum = run_sift(swap(message, "dm"), level, bins)
    return harmonic_sum, sifted[None, None]


def solution(mesh):
    return jax.shard_map(
        per_device,
        mesh=mesh,
        in_specs=(
            P(("beam", "dm"), "tm"),
            P(("beam", "tm"), "dm", None, None),
            P(("beam", "tm"), "dm", None),
        ),
        out_specs=(P(("beam", "dm"), "tm"), P(("beam", "tm"), "dm", None, None, None)),
        check_vma=False,
    )
```

```python
import functools
import math

import jax
import jax.numpy as jnp
import numpy as np
from jax import lax
from jax.experimental import pallas as pl
from jax.experimental.pallas import tpu as pltpu
from jax.sharding import PartitionSpec as P

HARM = 8
BW = 128
EPSILON = 1e-06

LANES = 128
SUB = 8
COARSE = 256
SLOTS = 16
PIECE = 32
ODD = {h: h // (h & -h) for h in range(1, HARM + 1)}
PIECES = [(h, range(c, c + ODD[h])) for h in range(1, HARM + 1) for c in range(0, h, ODD[h])]
CHUNKS = len(PIECES) // 4
ROWS = 2 * SUB + 1

F32 = jnp.float32
BF16 = jnp.bfloat16


def halves(value):
    top = value.astype(BF16)
    return top, (value - top.astype(F32)).astype(BF16)


def np_halves(value):
    top = value.astype(np.float32).astype(BF16)
    rest = (value - top.astype(np.float64)).astype(np.float32).astype(BF16)
    return top, rest


def unit(turns, period):
    angle = -2.0 * math.pi * (turns % period) / period
    return np.cos(angle), np.sin(angle)


@functools.cache
def tables(shards, samples):
    part = samples // (shards * shards)
    tiles = part // LANES
    m = np.arange(part)
    v = np.arange(LANES)
    s = np.arange(shards)
    half = shards // 2
    r = np.arange(half)
    wide = np.arange(2 * part)
    within = np.stack(unit(r[:, None] * wide[None, :], samples)).reshape(2, half, 2 * tiles, LANES)
    shift = np.stack(unit(r[:, None] * r[None, :], samples // (2 * part)), axis=1)
    shift = np.broadcast_to(shift[..., None], (half, 2, half, LANES))
    after = np.stack(unit(s[:, None] * m[None, :], samples // shards)).reshape(2, shards, tiles, LANES)
    middle = (half + shards * r)[:, None] * m[None, :]
    middle = np.stack(unit(middle, samples)).reshape(2, half, tiles, LANES)
    between = np.stack(unit(s[:, None] * v[None, :], part))
    j = np.arange(LANES // 2)
    rows = []
    for q2 in (j, LANES - 1 - j):
        c2, s2 = unit(q2[:, None] * v[None, :], LANES)
        rows += [np.concatenate([c2, -s2], axis=1), np.concatenate([s2, c2], axis=1)]
    last = np_halves(np.concatenate(rows, axis=0))
    fitting = np.zeros((half, SUB, LANES), np.float32)
    for own in range(half):
        for lane in range(LANES):
            slot = lane % SLOTS
            residue = own + SLOTS * slot if own else SLOTS * (slot % SUB) + SUB * (slot // SUB)
            if lane % PIECE >= SLOTS:
                residue = COARSE - residue if residue else COARSE // 2
            for odd in (3, 5, 7):
                fitting[own, odd, lane] = next(c for c in range(odd) if (residue + COARSE * c) % odd == 0)
    first = [x.astype(np.float32) for x in (within, shift)]
    second = [x.astype(np.float32) for x in (after, middle, between, fitting)] + [np.concatenate(last)]
    return first, second


def cmul(x, y):
    if x[1] is None:
        return x[0] * y[0], x[0] * y[1]
    return x[0] * y[0] - x[1] * y[1], x[0] * y[1] + x[1] * y[0]


def plus(a, b):
    return b if a is None else a if b is None else a + b


def minus(a, b):
    return a if b is None else -b if a is None else a - b


def cadd(x, y):
    return plus(x[0], y[0]), plus(x[1], y[1])


def csub(x, y):
    return minus(x[0], y[0]), minus(x[1], y[1])


def turn_back(x):
    return x[1], minus(None, x[0])


def four(x0, x1, x2, x3):
    s, d = cadd(x0, x2), csub(x0, x2)
    t, u = cadd(x1, x3), turn_back(csub(x1, x3))
    return cadd(s, t), cadd(d, u), csub(s, t), csub(d, u)


def sixteen(values):
    columns = [four(*values[low::4]) for low in range(4)]
    out = [None] * 16
    for k1 in range(4):
        terms = []
        for low in range(4):
            term = columns[low][k1]
            if low * k1 == 4:
                term = turn_back(term)
            elif low * k1:
                c, s = unit(np.float64(low * k1), 16)
                term = cmul(term, (F32(c), F32(s)))
            terms.append(term)
        for k2, value in enumerate(four(*terms)):
            out[k1 + 4 * k2] = value
    return out


def prepare_kernel(d_ref, x_ref, start_ref, count_ref, o_ref, s_ref, m_ref, x_scr, start_scr, count_scr, sems):
    small = [
        pltpu.make_async_copy(start_ref, start_scr, sems.at[0]),
        pltpu.make_async_copy(count_ref, count_scr, sems.at[1]),
    ]
    pieces = sems.shape[0] - 2
    size = x_ref.shape[0] // pieces
    copies = []
    for piece in range(pieces):
        here = pl.ds(piece * size, size)
        copies.append(pltpu.make_async_copy(x_ref.at[here], x_scr.at[here], sems.at[2 + piece]))
    for copy in small + copies:
        copy.start()

    own_class = d_ref[0] % SUB
    phi = lax.broadcasted_iota(jnp.int32, (SLOTS, COARSE), 1)
    slot = lax.broadcasted_iota(jnp.int32, (SLOTS, COARSE), 0)
    pairs = slot * SLOTS - jnp.where(slot < SUB, 0, SUB * SLOTS - SUB)
    mine = jnp.where(own_class == 0, pairs, own_class + SLOTS * slot)
    mirror = jnp.where(mine == 0, COARSE // 2, COARSE - mine)
    for index, (h, carries) in enumerate(PIECES):
        for k, residue in enumerate((mine, mirror)):
            gap = h * phi - residue
            hit = functools.reduce(jnp.logical_or, [gap == COARSE * c for c in carries])
            hit = jnp.where(hit, 1.0, 0.0)
            s_ref[pl.ds(index * PIECE + k * SLOTS, SLOTS), :] = hit.astype(BF16)

    for copy in small:
        copy.wait()
    bands, slots = start_ref.shape
    cell = [lax.broadcasted_iota(jnp.int32, (bands, bands), axis) for axis in range(2)]
    counts = jnp.where(cell[0] == cell[1], count_scr[...].astype(F32), 0.0)
    live = jnp.sum(counts, axis=1, keepdims=True).astype(jnp.int32)
    slot = lax.broadcasted_iota(jnp.int32, (bands, slots), 1)
    starts = jnp.where(slot < live, start_scr[...], -1).astype(F32)
    m_ref[...] = jnp.concatenate([starts] * (LANES // slots), axis=1)

    tiles = x_ref.shape[0] // 2
    for piece, copy in enumerate(copies):
        copy.wait()
        for at in range(piece * size // 2, (piece + 1) * size // 2, SUB):
            for row in range(2):
                o_ref[row * tiles + at : row * tiles + at + SUB, :] = x_scr[pl.ds(2 * at + row, SUB, stride=2), :]


def first_kernel(d_ref, x_ref, within_ref, shift_ref, o_ref):
    shards, tiles = x_ref.shape[:2]
    half = shards // 2
    me = d_ref[0] % half
    for k in range(tiles // SUB):
        inner = slice(k * SUB, (k + 1) * SUB)
        classes = sixteen([(x_ref[t, inner, :], None) for t in range(shards)])
        for r in range(half):
            if r:
                own = [shift_ref[me, part, r : r + 1, :] for part in range(2)]
                value = cmul(classes[r], cmul([within_ref[part, r, inner, :] for part in range(2)], own))
            else:
                value = classes[0][0], classes[half][0]
            for part in range(2):
                to = part * tiles + k * SUB
                o_ref[r, to : to + SUB, :] = value[part]


def second_kernel(d_ref, x_ref, after_ref, middle_ref, between_ref, fit_ref, table_ref, s_ref, o_ref, v_scr, x_scr, t_scr, dh_scr, dl_scr, r_scr, l_scr, h_scr):
    shards = 2 * x_ref.shape[0]
    tiles = x_ref.shape[1] // 4
    half = LANES // 2
    own_class = d_ref[0] % x_ref.shape[0]
    is_first = own_class == 0
    sub = lax.broadcasted_iota(jnp.int32, (SUB, LANES), 0)
    lead = jnp.logical_and(sub == 0, is_first)

    for k in range(tiles // SUB):
        rows = slice(k * SUB, (k + 1) * SUB)
        main, middle = [], []
        for s in range(shards):
            at = s % 2 * tiles + k * SUB
            re = x_ref[s // 2, at : at + SUB, :]
            im = x_ref[s // 2, 2 * tiles + at : 2 * tiles + at + SUB, :]
            main.append((re, jnp.where(is_first, 0.0, im)))
            c, sn = unit(np.float64(s), 2 * shards)
            middle.append((im * F32(c), im * F32(sn) if s else None))
        for slot, value in enumerate(sixteen(main)):
            value = cmul(value, (after_ref[0, slot, rows, :], after_ref[1, slot, rows, :]))
            for part in range(2):
                v_scr[pl.ds(part * tiles * shards + k * SUB * shards + slot, SUB, stride=shards), :] = value[part]
        for slot, value in enumerate(sixteen(middle)[: shards // 2]):
            value = cmul(value, (middle_ref[0, slot, rows, :], middle_ref[1, slot, rows, :]))
            for part in range(2):
                at = part * tiles * SUB + k * SUB * SUB + slot
                x_scr[pl.ds(at, SUB, stride=SUB), :] = value[part]

    groups = [[], [], []]
    for u in range(tiles):
        low, high, mid = [], [], []
        for part in range(2):
            at = part * tiles * shards + u * shards
            low.append(v_scr[at : at + SUB, :])
            high.append(v_scr[at + SUB : at + 2 * SUB, :])
            at = part * tiles * SUB + u * SUB
            mid.append(x_scr[at : at + SUB, :])
        groups[0].append(tuple(low))
        groups[1].append(tuple(jnp.where(is_first, mid[part], high[part]) for part in range(2)))
        groups[2].append(tuple(high))
    for group, values in enumerate(groups):
        for rho, value in enumerate(sixteen(values)):
            value = cmul(value, (between_ref[0, rho : rho + 1, :], between_ref[1, rho : rho + 1, :]))
            for part in range(2):
                t_scr[group, rho, part] = value[part]

    for rho in range(tiles):
        for part in range(2):
            back = tiles - 1 - rho
            low = jnp.concatenate([t_scr[0, rho, part], t_scr[1, rho, part]], axis=0)
            turned = jnp.where(lead, t_scr[2, rho, part], t_scr[0, back, part])
            high = jnp.concatenate([turned, t_scr[1, back, part]], axis=0)
            for k, tile in enumerate((low, high)):
                top, rest = halves(tile)
                rows = pl.ds(rho * PIECE + k * SLOTS, SLOTS)
                cols = pl.ds(part * LANES, LANES)
                dh_scr[rows, cols] = top
                dl_scr[rows, cols] = rest
    dims = (((1,), (1,)), ((), ()))
    dot_t = functools.partial(lax.dot_general, dimension_numbers=dims, preferred_element_type=F32)
    lane = lax.broadcasted_iota(jnp.int32, (half, 2 * LANES), 1)
    within = lane % PIECE
    from_low = jnp.logical_or(within < SLOTS, jnp.logical_and(within == SLOTS, is_first))
    scale = 1.0 / (shards * shards * tiles * LANES)
    powers = []
    for part in range(2):
        top = dh_scr[part * 256 : (part + 1) * 256, :]
        rest = dl_scr[part * 256 : (part + 1) * 256, :]
        z = dot_t(table_ref[...], top)
        z = z[:256] + z[256:] + dot_t(table_ref[:256, :], rest)
        z = z * z
        low = z[0:half] + z[half : 2 * half]
        high = z[2 * half : 3 * half] + z[3 * half :]
        powers.append(jnp.where(from_low, low, high) * scale)

    count = 2 * SLOTS * half * tiles

    def over_all(value):
        column = jnp.sum(value, axis=0, keepdims=True)
        return jnp.sum(column, axis=1, keepdims=True)

    mean = over_all(powers[0] + powers[1]) / count
    off0, off1 = powers[0] - mean, powers[1] - mean
    deviation = over_all(off0 * off0 + off1 * off1)
    stats = jnp.where(sub[0:1] + lax.broadcasted_iota(jnp.int32, (1, LANES), 1) < half, mean, deviation)
    for t in range(shards):
        o_ref[t * ROWS + 2 * SUB : (t + 1) * ROWS, :] = stats

    for group in range(4):
        value = powers[group // 2][:, (group % 2) * LANES : (group % 2 + 1) * LANES]
        for shift in range(4):
            at = (group * 4 + shift) * half
            r_scr[at : at + half, :] = pltpu.roll(value, shift * PIECE, 1) if shift else value
    lane8 = lax.broadcasted_iota(jnp.int32, (SUB, LANES), 1) // PIECE
    fits = {}
    for index, (h, _) in enumerate(PIECES):
        if ODD[h] > 1:
            fit = jnp.broadcast_to(fit_ref[own_class, ODD[h] : ODD[h] + 1, :], (SUB, LANES))
            fits[index % 4, ODD[h]] = jnp.where(lane8 == index % 4, fit, -1.0).astype(jnp.int32)
    for chunk in range(CHUNKS):
        for g_pair in range(tiles // 2):
            parts = []
            for g0 in (2 * g_pair, 2 * g_pair + 1):
                tile = None
                for place in range(4):
                    h, carries = PIECES[chunk * 4 + place]
                    for c in carries:
                        rho, e = (h * g0 + c) % tiles, (h * g0 + c) // tiles
                        shift = (place - rho % 4) % 4
                        rows = pl.ds((rho // 4 * 4 + shift) * half + e, SUB, stride=h)
                        got = r_scr[rows, :]
                        here = lane8 == place if c == carries[0] else fits[place, ODD[h]] == c % ODD[h]
                        tile = got if tile is None else jnp.where(here, got, tile)
                parts.append(tile)
            top, rest = halves(jnp.concatenate(parts, axis=0))
            cols = pl.ds(chunk * LANES, LANES)
            l_scr[pl.ds(g_pair * 16, 16), cols] = top
            l_scr[pl.ds(LANES + g_pair * 16, 16), cols] = rest
    both = jnp.dot(l_scr[...], s_ref[...], preferred_element_type=F32)
    for tile in range(2):
        cols = slice(tile * LANES, (tile + 1) * LANES)
        h_scr[tile * LANES : (tile + 1) * LANES, :] = both[:LANES, cols] + both[LANES:, cols]
    for t in range(shards):
        for tile in range(2):
            rows = pl.ds(tile * LANES + (t % 2) * half + t // 2, SUB, stride=SUB)
            o_ref[t * ROWS + tile * SUB : t * ROWS + (tile + 1) * SUB, :] = h_scr[rows, :]


def third_kernel(m_ref, x_ref, hs_ref, msg_ref, level_ref):
    shards = x_ref.shape[0] // ROWS
    holders = shards // 2
    count = 2 * SLOTS * (LANES // 2) * SLOTS
    tiles = []
    for row in range(2):
        blocks = [(row * holders + r) * ROWS for r in range(holders)]
        sums = [x_ref[at : at + 2 * SUB, :] for at in blocks]
        stats = [x_ref[at + 2 * SUB : at + ROWS, :] for at in blocks]
        total, both = sums[0], stats[0]
        for r in range(1, holders):
            total, both = total + sums[r], both + stats[r]
        mean = both[:, 0:1] / holders
        spread = both[:, LANES // 2 : LANES // 2 + 1]
        for r in range(holders):
            off = stats[r][:, 0:1] - mean
            spread = spread + count * (off * off)
        scale = 1.0 / jnp.sqrt(spread / (count * holders) + EPSILON)
        tiles.append([(total[k * SUB : (k + 1) * SUB] - HARM * mean) * scale for k in range(2)])
    for row in range(2):
        for k in range(2):
            for g in range(SUB):
                hs_ref[row : row + 1, pl.ds(g * COARSE + k * LANES, LANES)] = tiles[row][k][g : g + 1]
    for k in range(2):
        level_ref[k * SUB : (k + 1) * SUB, :] = (tiles[0][k] + tiles[1][k]) / 2
    peak = jnp.concatenate([jnp.maximum(tiles[0][k], tiles[1][k]) for k in range(2)], axis=0)
    for e in range(m_ref.shape[0]):
        msg_ref[e * ROWS : e * ROWS + 2 * SUB, :] = peak
        msg_ref[e * ROWS + 2 * SUB : (e + 1) * ROWS, :] = m_ref[e : e + 1, :]


def sift_kernel(x_ref, level_ref, bins_ref, o_ref, hs_ref):
    hs_ref[...] = bins_ref[...]
    bands, slots = o_ref.shape[:2]
    level = level_ref[...]
    rows = bands * slots
    diff = jnp.concatenate([x_ref[d * ROWS : d * ROWS + 2 * SUB, :] - level for d in range(bands)], axis=0)
    lane = lax.broadcasted_iota(jnp.int32, (rows, LANES), 1)
    line = lax.broadcasted_iota(jnp.int32, (rows, LANES), 0)
    listed = [x_ref[d * ROWS + 2 * SUB : (d + 1) * ROWS, :] for d in range(bands)]
    listed = jnp.concatenate([jnp.broadcast_to(x, (slots, LANES)) for x in listed], axis=0)
    start = jnp.sum(jnp.where(lane == line & (slots - 1), listed, 0.0), axis=1, keepdims=True)
    start = jnp.broadcast_to(start, (rows, LANES)).astype(jnp.int32)
    block = jnp.maximum(start, 0)
    tile_id, offset = block >> 7, block & (LANES - 1)
    band = line & -slots

    def pick(which):
        place = band + ((which & 1) << 3) + (which >> 1)
        return jnp.where(lane == place, 1.0, 0.0).astype(BF16)

    both = jnp.concatenate([pick(tile_id), pick(tile_id + 1)], axis=0)
    parts = jnp.dot(both, jnp.concatenate(halves(diff), axis=1), preferred_element_type=F32)
    parts = parts[:, :LANES] + parts[:, LANES:]
    joined = jnp.where(lane >= offset, parts[:rows], parts[rows:])
    moved = jnp.take_along_axis(joined, (lane + offset) & (LANES - 1), axis=1)
    o_ref[...] = jnp.where(start >= 0, moved, 0.0).reshape(bands, slots, LANES)


PARAMS = pltpu.CompilerParams(vmem_limit_bytes=16 * 2**20)


def near(array):
    return pltpu.with_memory_space_constraint(array, pltpu.VMEM)


def shape(*dims):
    return pltpu.VMEM(dims, F32)


def spaces(*kinds):
    return [pl.BlockSpec(memory_space=pltpu.SMEM if kind == "s" else pltpu.VMEM) for kind in kinds]


def run_prepare(me, series, starts, counts, shards):
    tiles = series.shape[1] // LANES
    lines = jnp.swapaxes(series.reshape(2, tiles, LANES), 0, 1).reshape(2 * tiles, LANES)
    rows, mapping, markers = pl.pallas_call(
        prepare_kernel,
        out_shape=(
            shape(2 * tiles, LANES),
            pltpu.VMEM((CHUNKS * LANES, COARSE), BF16),
            shape(starts.shape[0], LANES),
        ),
        in_specs=spaces("s") + [pl.BlockSpec(memory_space=pl.ANY)] * 3,
        out_specs=spaces(*"vvv"),
        scratch_shapes=[
            pltpu.VMEM((2 * tiles, LANES), F32),
            pltpu.VMEM(starts.shape, jnp.int32),
            pltpu.VMEM(counts.shape, jnp.int32),
            pltpu.SemaphoreType.DMA((4,)),
        ],
        compiler_params=PARAMS,
    )(me, *[pltpu.with_memory_space_constraint(x, pltpu.HBM) for x in (lines, starts, counts)])
    return rows.reshape(shards, -1, LANES), mapping, markers


def run_first(me, received, first):
    shards = received.shape[0]
    within, shift = map(jnp.asarray, first)
    return pl.pallas_call(
        first_kernel,
        out_shape=shape(shards // 2, 2 * received.shape[1], LANES),
        in_specs=spaces(*"svvv"),
        out_specs=spaces("v")[0],
        compiler_params=PARAMS,
    )(me, *[near(x) for x in (received, within, shift)])


def run_second(me, received, second, mapping):
    shards = 2 * received.shape[0]
    inputs = [near(x) for x in (received, *map(jnp.asarray, second), mapping)]
    sent = pl.pallas_call(
        second_kernel,
        out_shape=shape(shards * ROWS, LANES),
        in_specs=spaces("s", *"vvvvvvv"),
        out_specs=spaces("v")[0],
        scratch_shapes=[
            pltpu.VMEM((2 * SLOTS * SLOTS, LANES), F32),
            pltpu.VMEM((2 * SLOTS * SUB, LANES), F32),
            pltpu.VMEM((3, SLOTS, 2, SUB, LANES), F32),
            pltpu.VMEM((SLOTS * PIECE, 2 * LANES), BF16),
            pltpu.VMEM((SLOTS * PIECE, 2 * LANES), BF16),
            pltpu.VMEM((16 * LANES // 2, LANES), F32),
            pltpu.VMEM((2 * LANES, CHUNKS * LANES), BF16),
            pltpu.VMEM((2 * LANES, LANES), F32),
        ],
        compiler_params=PARAMS,
    )(me, *inputs)
    return sent.reshape(shards, 1, ROWS * LANES)


def run_third(received, markers):
    bands = markers.shape[0]
    bins, message, level = pl.pallas_call(
        third_kernel,
        out_shape=(shape(2, SUB * COARSE), shape(bands * ROWS, LANES), shape(2 * SUB, LANES)),
        in_specs=spaces(*"vv"),
        out_specs=spaces(*"vvv"),
        compiler_params=PARAMS,
    )(near(markers), near(received.reshape(-1, LANES)))
    return bins, message.reshape(bands, 1, ROWS * LANES), level


def run_sift(received, level, bins):
    bands = received.shape[0]
    return pl.pallas_call(
        sift_kernel,
        out_shape=(
            jax.ShapeDtypeStruct((bands, 2 * SUB, LANES), F32),
            jax.ShapeDtypeStruct(bins.shape, F32),
        ),
        in_specs=spaces(*"vvv"),
        out_specs=spaces(*"vv"),
        compiler_params=PARAMS,
    )(near(received.reshape(-1, LANES)), near(level), near(bins))


def per_device(series, cand_start, cand_count):
    shards = lax.axis_size("tm")
    first, second = tables(shards, shards * series.shape[1])
    me = lax.axis_index("tm").astype(jnp.int32).reshape(1)
    swap = functools.partial(lax.all_to_all, split_axis=0, concat_axis=0, tiled=True)
    rows, mapping, markers = run_prepare(me, series, cand_start[0, 0], cand_count[0], shards)
    half = shards // 2
    by_row = [list(range(half)), list(range(half, shards))]
    classes = swap(run_first(me, swap(rows, "tm"), first), "tm", axis_index_groups=by_row)
    sums = swap(run_second(me, classes, second, mapping), "tm")
    bins, message, level = run_third(sums, markers)
    sifted, harmonic_sum = run_sift(swap(message, "dm"), level, bins)
    return harmonic_sum, sifted[None, None]


def solution(mesh):
    return jax.shard_map(
        per_device,
        mesh=mesh,
        in_specs=(
            P(("beam", "dm"), "tm"),
            P(("beam", "tm"), "dm", None, None),
            P(("beam", "tm"), "dm", None),
        ),
        out_specs=(P(("beam", "dm"), "tm"), P(("beam", "tm"), "dm", None, None, None)),
        check_vma=False,
    )
```

```python
import functools
import math

import jax
import jax.numpy as jnp
import numpy as np
from jax import lax
from jax.experimental import pallas as pl
from jax.experimental.pallas import tpu as pltpu
from jax.sharding import PartitionSpec as P

HARM = 8
BW = 128
EPSILON = 1e-06

LANES = 128
SUB = 8
COARSE = 256
SLOTS = 16
PIECE = 32
ODD = {h: h // (h & -h) for h in range(1, HARM + 1)}
PIECES = [(h, range(c, c + ODD[h])) for h in range(1, HARM + 1) for c in range(0, h, ODD[h])]
CHUNKS = len(PIECES) // 4
ROWS = 2 * SUB + 1

F32 = jnp.float32
BF16 = jnp.bfloat16


def halves(value):
    top = value.astype(BF16)
    return top, (value - top.astype(F32)).astype(BF16)


def np_halves(value):
    top = value.astype(np.float32).astype(BF16)
    rest = (value - top.astype(np.float64)).astype(np.float32).astype(BF16)
    return top, rest


def unit(turns, period):
    angle = -2.0 * math.pi * (turns % period) / period
    return np.cos(angle), np.sin(angle)


@functools.cache
def tables(shards, samples):
    part = samples // (shards * shards)
    tiles = part // LANES
    m = np.arange(part)
    v = np.arange(LANES)
    s = np.arange(shards)
    half = shards // 2
    r = np.arange(half)
    wide = np.arange(2 * part)
    within = np.stack(unit(r[:, None] * wide[None, :], samples)).reshape(2, half, 2 * tiles, LANES)
    shift = np.stack(unit(r[:, None] * r[None, :], samples // (2 * part)), axis=1)
    shift = np.broadcast_to(shift[..., None], (half, 2, half, LANES))
    after = np.stack(unit(s[:, None] * m[None, :], samples // shards)).reshape(2, shards, tiles, LANES)
    middle = (half + shards * r)[:, None] * m[None, :]
    middle = np.stack(unit(middle, samples)).reshape(2, half, tiles, LANES)
    between = np.stack(unit(s[:, None] * v[None, :], part))
    j = np.arange(LANES // 2)
    rows = []
    for q2 in (j, LANES - 1 - j):
        c2, s2 = unit(q2[:, None] * v[None, :], LANES)
        rows += [np.concatenate([c2, -s2], axis=1), np.concatenate([s2, c2], axis=1)]
    last = np_halves(np.concatenate(rows, axis=0))
    fitting = np.zeros((half, SUB, LANES), np.float32)
    for own in range(half):
        for lane in range(LANES):
            slot = lane % SLOTS
            residue = own + SLOTS * slot if own else SLOTS * (slot % SUB) + SUB * (slot // SUB)
            if lane % PIECE >= SLOTS:
                residue = COARSE - residue if residue else COARSE // 2
            for odd in (3, 5, 7):
                fitting[own, odd, lane] = next(c for c in range(odd) if (residue + COARSE * c) % odd == 0)
    first = [x.astype(np.float32) for x in (within, shift)]
    second = [x.astype(np.float32) for x in (after, middle, between, fitting)] + [np.concatenate(last)]
    return first, second


def cmul(x, y):
    if x[1] is None:
        return x[0] * y[0], x[0] * y[1]
    return x[0] * y[0] - x[1] * y[1], x[0] * y[1] + x[1] * y[0]


def plus(a, b):
    return b if a is None else a if b is None else a + b


def minus(a, b):
    return a if b is None else -b if a is None else a - b


def cadd(x, y):
    return plus(x[0], y[0]), plus(x[1], y[1])


def csub(x, y):
    return minus(x[0], y[0]), minus(x[1], y[1])


def turn_back(x):
    return x[1], minus(None, x[0])


def four(x0, x1, x2, x3):
    s, d = cadd(x0, x2), csub(x0, x2)
    t, u = cadd(x1, x3), turn_back(csub(x1, x3))
    return cadd(s, t), cadd(d, u), csub(s, t), csub(d, u)


def sixteen(values):
    columns = [four(*values[low::4]) for low in range(4)]
    out = [None] * 16
    for k1 in range(4):
        terms = []
        for low in range(4):
            term = columns[low][k1]
            if low * k1 == 4:
                term = turn_back(term)
            elif low * k1:
                c, s = unit(np.float64(low * k1), 16)
                term = cmul(term, (F32(c), F32(s)))
            terms.append(term)
        for k2, value in enumerate(four(*terms)):
            out[k1 + 4 * k2] = value
    return out


def prepare_kernel(d_ref, x_ref, start_ref, count_ref, o_ref, s_ref, m_ref, x_scr, start_scr, count_scr, sems):
    small = [
        pltpu.make_async_copy(start_ref, start_scr, sems.at[0]),
        pltpu.make_async_copy(count_ref, count_scr, sems.at[1]),
    ]
    pieces = sems.shape[0] - 2
    size = x_ref.shape[0] // pieces
    copies = []
    for piece in range(pieces):
        here = pl.ds(piece * size, size)
        copies.append(pltpu.make_async_copy(x_ref.at[here], x_scr.at[here], sems.at[2 + piece]))
    for copy in small + copies:
        copy.start()

    own_class = d_ref[0] % SUB
    phi = lax.broadcasted_iota(jnp.int32, (SLOTS, COARSE), 1)
    slot = lax.broadcasted_iota(jnp.int32, (SLOTS, COARSE), 0)
    pairs = slot * SLOTS - jnp.where(slot < SUB, 0, SUB * SLOTS - SUB)
    mine = jnp.where(own_class == 0, pairs, own_class + SLOTS * slot)
    mirror = jnp.where(mine == 0, COARSE // 2, COARSE - mine)
    for index, (h, carries) in enumerate(PIECES):
        for k, residue in enumerate((mine, mirror)):
            gap = h * phi - residue
            hit = functools.reduce(jnp.logical_or, [gap == COARSE * c for c in carries])
            hit = jnp.where(hit, 1.0, 0.0)
            s_ref[pl.ds(index * PIECE + k * SLOTS, SLOTS), :] = hit.astype(BF16)

    for copy in small:
        copy.wait()
    bands, slots = start_ref.shape
    cell = [lax.broadcasted_iota(jnp.int32, (bands, bands), axis) for axis in range(2)]
    counts = jnp.where(cell[0] == cell[1], count_scr[...].astype(F32), 0.0)
    live = jnp.sum(counts, axis=1, keepdims=True).astype(jnp.int32)
    slot = lax.broadcasted_iota(jnp.int32, (bands, slots), 1)
    starts = jnp.where(slot < live, start_scr[...], -1).astype(F32)
    m_ref[...] = jnp.concatenate([starts] * (LANES // slots), axis=1)

    tiles = x_ref.shape[0] // 2
    for piece, copy in enumerate(copies):
        copy.wait()
        for at in range(piece * size // 2, (piece + 1) * size // 2, SUB):
            for row in range(2):
                o_ref[row * tiles + at : row * tiles + at + SUB, :] = x_scr[pl.ds(2 * at + row, SUB, stride=2), :]


def first_kernel(d_ref, x_ref, within_ref, shift_ref, o_ref):
    shards, tiles = x_ref.shape[:2]
    half = shards // 2
    me = d_ref[0] % half
    for k in range(tiles // SUB):
        inner = slice(k * SUB, (k + 1) * SUB)
        classes = sixteen([(x_ref[t, inner, :], None) for t in range(shards)])
        for r in range(half):
            if r:
                own = [shift_ref[me, part, r : r + 1, :] for part in range(2)]
                value = cmul(classes[r], cmul([within_ref[part, r, inner, :] for part in range(2)], own))
            else:
                value = classes[0][0], classes[half][0]
            for part in range(2):
                to = part * tiles + k * SUB
                o_ref[r, to : to + SUB, :] = value[part]


def second_kernel(d_ref, x_ref, after_ref, middle_ref, between_ref, fit_ref, table_ref, s_ref, o_ref, v_scr, x_scr, t_scr, dh_scr, dl_scr, r_scr, l_scr, h_scr):
    shards = 2 * x_ref.shape[0]
    tiles = x_ref.shape[1] // 4
    half = LANES // 2
    own_class = d_ref[0] % x_ref.shape[0]
    is_first = own_class == 0
    sub = lax.broadcasted_iota(jnp.int32, (SUB, LANES), 0)
    lead = jnp.logical_and(sub == 0, is_first)

    for k in range(tiles // SUB):
        rows = slice(k * SUB, (k + 1) * SUB)
        main, middle = [], []
        for s in range(shards):
            at = s % 2 * tiles + k * SUB
            re = x_ref[s // 2, at : at + SUB, :]
            im = x_ref[s // 2, 2 * tiles + at : 2 * tiles + at + SUB, :]
            main.append((re, jnp.where(is_first, 0.0, im)))
            c, sn = unit(np.float64(s), 2 * shards)
            middle.append((im * F32(c), im * F32(sn) if s else None))
        for slot, value in enumerate(sixteen(main)):
            value = cmul(value, (after_ref[0, slot, rows, :], after_ref[1, slot, rows, :]))
            for part in range(2):
                v_scr[pl.ds(part * tiles * shards + k * SUB * shards + slot, SUB, stride=shards), :] = value[part]
        for slot, value in enumerate(sixteen(middle)[: shards // 2]):
            value = cmul(value, (middle_ref[0, slot, rows, :], middle_ref[1, slot, rows, :]))
            for part in range(2):
                at = part * tiles * SUB + k * SUB * SUB + slot
                x_scr[pl.ds(at, SUB, stride=SUB), :] = value[part]

    groups = [[], [], []]
    for u in range(tiles):
        low, high, mid = [], [], []
        for part in range(2):
            at = part * tiles * shards + u * shards
            low.append(v_scr[at : at + SUB, :])
            high.append(v_scr[at + SUB : at + 2 * SUB, :])
            at = part * tiles * SUB + u * SUB
            mid.append(x_scr[at : at + SUB, :])
        groups[0].append(tuple(low))
        groups[1].append(tuple(jnp.where(is_first, mid[part], high[part]) for part in range(2)))
        groups[2].append(tuple(high))
    for group, values in enumerate(groups):
        for rho, value in enumerate(sixteen(values)):
            value = cmul(value, (between_ref[0, rho : rho + 1, :], between_ref[1, rho : rho + 1, :]))
            for part in range(2):
                t_scr[group, rho, part] = value[part]

    for rho in range(tiles):
        for part in range(2):
            back = tiles - 1 - rho
            low = jnp.concatenate([t_scr[0, rho, part], t_scr[1, rho, part]], axis=0)
            turned = jnp.where(lead, t_scr[2, rho, part], t_scr[0, back, part])
            high = jnp.concatenate([turned, t_scr[1, back, part]], axis=0)
            for k, tile in enumerate((low, high)):
                top, rest = halves(tile)
                rows = pl.ds(rho * PIECE + k * SLOTS, SLOTS)
                cols = pl.ds(part * LANES, LANES)
                dh_scr[rows, cols] = top
                dl_scr[rows, cols] = rest
    dims = (((1,), (1,)), ((), ()))
    dot_t = functools.partial(lax.dot_general, dimension_numbers=dims, preferred_element_type=F32)
    lane = lax.broadcasted_iota(jnp.int32, (half, 2 * LANES), 1)
    within = lane % PIECE
    from_low = jnp.logical_or(within < SLOTS, jnp.logical_and(within == SLOTS, is_first))
    scale = 1.0 / (shards * shards * tiles * LANES)
    powers = []
    for part in range(2):
        top = dh_scr[part * 256 : (part + 1) * 256, :]
        rest = dl_scr[part * 256 : (part + 1) * 256, :]
        z = dot_t(table_ref[...], top)
        z = z[:256] + z[256:] + dot_t(table_ref[:256, :], rest)
        z = z * z
        low = z[0:half] + z[half : 2 * half]
        high = z[2 * half : 3 * half] + z[3 * half :]
        powers.append(jnp.where(from_low, low, high) * scale)

    count = 2 * SLOTS * half * tiles

    def over_all(value):
        column = jnp.sum(value, axis=0, keepdims=True)
        return jnp.sum(column, axis=1, keepdims=True)

    mean = over_all(powers[0] + powers[1]) / count
    off0, off1 = powers[0] - mean, powers[1] - mean
    deviation = over_all(off0 * off0 + off1 * off1)
    stats = jnp.where(sub[0:1] + lax.broadcasted_iota(jnp.int32, (1, LANES), 1) < half, mean, deviation)
    for t in range(shards):
        o_ref[t * ROWS + 2 * SUB : (t + 1) * ROWS, :] = stats

    for group in range(4):
        value = powers[group // 2][:, (group % 2) * LANES : (group % 2 + 1) * LANES]
        for shift in range(4):
            at = (group * 4 + shift) * half
            r_scr[at : at + half, :] = pltpu.roll(value, shift * PIECE, 1) if shift else value
    lane8 = lax.broadcasted_iota(jnp.int32, (SUB, LANES), 1) // PIECE
    fits = {}
    for index, (h, _) in enumerate(PIECES):
        if ODD[h] > 1:
            fit = jnp.broadcast_to(fit_ref[own_class, ODD[h] : ODD[h] + 1, :], (SUB, LANES))
            fits[index % 4, ODD[h]] = jnp.where(lane8 == index % 4, fit, -1.0).astype(jnp.int32)
    for chunk in range(CHUNKS):
        for g_pair in range(tiles // 2):
            parts = []
            for g0 in (2 * g_pair, 2 * g_pair + 1):
                tile = None
                for place in range(4):
                    h, carries = PIECES[chunk * 4 + place]
                    for c in carries:
                        rho, e = (h * g0 + c) % tiles, (h * g0 + c) // tiles
                        shift = (place - rho % 4) % 4
                        rows = pl.ds((rho // 4 * 4 + shift) * half + e, SUB, stride=h)
                        got = r_scr[rows, :]
                        here = lane8 == place if c == carries[0] else fits[place, ODD[h]] == c % ODD[h]
                        tile = got if tile is None else jnp.where(here, got, tile)
                parts.append(tile)
            top, rest = halves(jnp.concatenate(parts, axis=0))
            cols = pl.ds(chunk * LANES, LANES)
            l_scr[pl.ds(g_pair * 16, 16), cols] = top
            l_scr[pl.ds(LANES + g_pair * 16, 16), cols] = rest
    both = jnp.dot(l_scr[...], s_ref[...], preferred_element_type=F32)
    for tile in range(2):
        cols = slice(tile * LANES, (tile + 1) * LANES)
        h_scr[tile * LANES : (tile + 1) * LANES, :] = both[:LANES, cols] + both[LANES:, cols]
    for t in range(shards):
        for tile in range(2):
            rows = pl.ds(tile * LANES + (t % 2) * half + t // 2, SUB, stride=SUB)
            o_ref[t * ROWS + tile * SUB : t * ROWS + (tile + 1) * SUB, :] = h_scr[rows, :]


def third_kernel(m_ref, x_ref, hs_ref, msg_ref, level_ref):
    shards = x_ref.shape[0] // ROWS
    holders = shards // 2
    count = 2 * SLOTS * (LANES // 2) * SLOTS
    tiles = []
    for row in range(2):
        blocks = [(row * holders + r) * ROWS for r in range(holders)]
        sums = [x_ref[at : at + 2 * SUB, :] for at in blocks]
        stats = [x_ref[at + 2 * SUB : at + ROWS, :] for at in blocks]
        total, both = sums[0], stats[0]
        for r in range(1, holders):
            total, both = total + sums[r], both + stats[r]
        mean = both[:, 0:1] / holders
        spread = both[:, LANES // 2 : LANES // 2 + 1]
        for r in range(holders):
            off = stats[r][:, 0:1] - mean
            spread = spread + count * (off * off)
        scale = 1.0 / jnp.sqrt(spread / (count * holders) + EPSILON)
        tiles.append([(total[k * SUB : (k + 1) * SUB] - HARM * mean) * scale for k in range(2)])
    for row in range(2):
        for k in range(2):
            for g in range(SUB):
                hs_ref[row : row + 1, pl.ds(g * COARSE + k * LANES, LANES)] = tiles[row][k][g : g + 1]
    for k in range(2):
        level_ref[k * SUB : (k + 1) * SUB, :] = (tiles[0][k] + tiles[1][k]) / 2
    peak = jnp.concatenate([jnp.maximum(tiles[0][k], tiles[1][k]) for k in range(2)], axis=0)
    for e in range(m_ref.shape[0]):
        msg_ref[e * ROWS : e * ROWS + 2 * SUB, :] = peak
        msg_ref[e * ROWS + 2 * SUB : (e + 1) * ROWS, :] = m_ref[e : e + 1, :]


def sift_kernel(x_ref, level_ref, bins_ref, o_ref, hs_ref):
    hs_ref[...] = bins_ref[...]
    bands, slots = o_ref.shape[:2]
    level = level_ref[...]
    rows = bands * slots
    diff = jnp.concatenate([x_ref[d * ROWS : d * ROWS + 2 * SUB, :] - level for d in range(bands)], axis=0)
    lane = lax.broadcasted_iota(jnp.int32, (rows, LANES), 1)
    line = lax.broadcasted_iota(jnp.int32, (rows, LANES), 0)
    listed = [x_ref[d * ROWS + 2 * SUB : (d + 1) * ROWS, :] for d in range(bands)]
    listed = jnp.concatenate([jnp.broadcast_to(x, (slots, LANES)) for x in listed], axis=0)
    start = jnp.sum(jnp.where(lane == line & (slots - 1), listed, 0.0), axis=1, keepdims=True)
    start = jnp.broadcast_to(start, (rows, LANES)).astype(jnp.int32)
    block = jnp.maximum(start, 0)
    tile_id, offset = block >> 7, block & (LANES - 1)
    band = line & -slots

    def pick(which):
        place = band + ((which & 1) << 3) + (which >> 1)
        return jnp.where(lane == place, 1.0, 0.0).astype(BF16)

    both = jnp.concatenate([pick(tile_id), pick(tile_id + 1)], axis=0)
    parts = jnp.dot(both, jnp.concatenate(halves(diff), axis=1), preferred_element_type=F32)
    parts = parts[:, :LANES] + parts[:, LANES:]
    joined = jnp.where(lane >= offset, parts[:rows], parts[rows:])
    moved = jnp.take_along_axis(joined, (lane + offset) & (LANES - 1), axis=1)
    o_ref[...] = jnp.where(start >= 0, moved, 0.0).reshape(bands, slots, LANES)


PARAMS = pltpu.CompilerParams(vmem_limit_bytes=16 * 2**20)


def near(array):
    return pltpu.with_memory_space_constraint(array, pltpu.VMEM)


def shape(*dims):
    return pltpu.VMEM(dims, F32)


def spaces(*kinds):
    return [pl.BlockSpec(memory_space=pltpu.SMEM if kind == "s" else pltpu.VMEM) for kind in kinds]


def run_prepare(me, series, starts, counts, shards):
    tiles = series.shape[1] // LANES
    lines = jnp.swapaxes(series.reshape(2, tiles, LANES), 0, 1).reshape(2 * tiles, LANES)
    rows, mapping, markers = pl.pallas_call(
        prepare_kernel,
        out_shape=(
            shape(2 * tiles, LANES),
            pltpu.VMEM((CHUNKS * LANES, COARSE), BF16),
            shape(starts.shape[0], LANES),
        ),
        in_specs=spaces("s") + [pl.BlockSpec(memory_space=pl.ANY)] * 3,
        out_specs=spaces(*"vvv"),
        scratch_shapes=[
            pltpu.VMEM((2 * tiles, LANES), F32),
            pltpu.VMEM(starts.shape, jnp.int32),
            pltpu.VMEM(counts.shape, jnp.int32),
            pltpu.SemaphoreType.DMA((3,)),
        ],
        compiler_params=PARAMS,
    )(me, *[pltpu.with_memory_space_constraint(x, pltpu.HBM) for x in (lines, starts, counts)])
    return rows.reshape(shards, -1, LANES), mapping, markers


def run_first(me, received, first):
    shards = received.shape[0]
    within, shift = map(jnp.asarray, first)
    return pl.pallas_call(
        first_kernel,
        out_shape=shape(shards // 2, 2 * received.shape[1], LANES),
        in_specs=spaces(*"svvv"),
        out_specs=spaces("v")[0],
        compiler_params=PARAMS,
    )(me, *[near(x) for x in (received, within, shift)])


def run_second(me, received, second, mapping):
    shards = 2 * received.shape[0]
    inputs = [near(x) for x in (received, *map(jnp.asarray, second), mapping)]
    sent = pl.pallas_call(
        second_kernel,
        out_shape=shape(shards * ROWS, LANES),
        in_specs=spaces("s", *"vvvvvvv"),
        out_specs=spaces("v")[0],
        scratch_shapes=[
            pltpu.VMEM((2 * SLOTS * SLOTS, LANES), F32),
            pltpu.VMEM((2 * SLOTS * SUB, LANES), F32),
            pltpu.VMEM((3, SLOTS, 2, SUB, LANES), F32),
            pltpu.VMEM((SLOTS * PIECE, 2 * LANES), BF16),
            pltpu.VMEM((SLOTS * PIECE, 2 * LANES), BF16),
            pltpu.VMEM((16 * LANES // 2, LANES), F32),
            pltpu.VMEM((2 * LANES, CHUNKS * LANES), BF16),
            pltpu.VMEM((2 * LANES, LANES), F32),
        ],
        compiler_params=PARAMS,
    )(me, *inputs)
    return sent.reshape(shards, 1, ROWS * LANES)


def run_third(received, markers):
    bands = markers.shape[0]
    bins, message, level = pl.pallas_call(
        third_kernel,
        out_shape=(shape(2, SUB * COARSE), shape(bands * ROWS, LANES), shape(2 * SUB, LANES)),
        in_specs=spaces(*"vv"),
        out_specs=spaces(*"vvv"),
        compiler_params=PARAMS,
    )(near(markers), near(received.reshape(-1, LANES)))
    return bins, message.reshape(bands, 1, ROWS * LANES), level


def run_sift(received, level, bins):
    bands = received.shape[0]
    return pl.pallas_call(
        sift_kernel,
        out_shape=(
            jax.ShapeDtypeStruct((bands, 2 * SUB, LANES), F32),
            jax.ShapeDtypeStruct(bins.shape, F32),
        ),
        in_specs=spaces(*"vvv"),
        out_specs=spaces(*"vv"),
        compiler_params=PARAMS,
    )(near(received.reshape(-1, LANES)), near(level), near(bins))


def per_device(series, cand_start, cand_count):
    shards = lax.axis_size("tm")
    first, second = tables(shards, shards * series.shape[1])
    me = lax.axis_index("tm").astype(jnp.int32).reshape(1)
    swap = functools.partial(lax.all_to_all, split_axis=0, concat_axis=0, tiled=True)
    rows, mapping, markers = run_prepare(me, series, cand_start[0, 0], cand_count[0], shards)
    half = shards // 2
    by_row = [list(range(half)), list(range(half, shards))]
    classes = swap(run_first(me, swap(rows, "tm"), first), "tm", axis_index_groups=by_row)
    sums = swap(run_second(me, classes, second, mapping), "tm")
    bins, message, level = run_third(sums, markers)
    sifted, harmonic_sum = run_sift(swap(message, "dm"), level, bins)
    return harmonic_sum, sifted[None, None]


def solution(mesh):
    return jax.shard_map(
        per_device,
        mesh=mesh,
        in_specs=(
            P(("beam", "dm"), "tm"),
            P(("beam", "tm"), "dm", None, None),
            P(("beam", "tm"), "dm", None),
        ),
        out_specs=(P(("beam", "dm"), "tm"), P(("beam", "tm"), "dm", None, None, None)),
        check_vma=False,
    )
```
